32 devices in a mesh: rep: 8 (over z, x), tp: 4 (over y, core).
Axes of the slice: x: 2, y: 2, z: 4, core: 2. Of those that a mesh axis runs over, the one named last changes fastest.
Arguments:
- prompt_queries: bfloat16 [3968, 4096], P('rep', 'tp'), parts along dimension 0, may hold values from -240 to 240
- prompt_entries: bfloat16 [16, 496, 512], P('rep', 'tp'), parts along dimension 0, may hold values from -6 to 6
- history_cache: bfloat16 [16, 1024, 512], P('rep', 'tp'), parts along dimension 0, may hold values from -6 to 6
- decode_queries: bfloat16 [128, 4096], P('rep', 'tp'), parts along dimension 0, may hold values from -240 to 240
- decode_entries: bfloat16 [16, 16, 512], P('rep'), parts along dimension 0, may hold values from -6 to 6
- decode_cache: bfloat16 [16, 16, 768, 512], P('rep', None, 'tp'), parts along dimension 0, may hold values from -6 to 6
- decode_lengths: int32 [128], P('rep'), parts along dimension 0, may hold values from 1 to 768
- prompt_start: int32 [8], P('rep'), parts along dimension 0, may hold values from 512 to 1024
- out_weight: bfloat16 [4096, 4096], P('tp'), may hold values from -0.09375 to 0.09375
- residual: bfloat16 [512, 32768], P('tp', 'rep'), parts along dimension 1, may hold values from -4 to 4
- norm_gain: float32 [4096], replicated, may hold values from 0.5 to 1.5
Outputs:
- new_residual: bfloat16 [512, 32768], P('tp', 'rep'), parts along dimension 1
- normed: bfloat16 [512, 32768], P('tp', 'rep'), parts along dimension 1
The draws below stay inside these ranges and needn't reach their ends.
There are 8 independent parts, one for each index of `rep`. The reference program is written for one: setup_inputs(seed, part) draws one part's arguments, and reference() takes and returns one part's arrays. A program takes and returns all parts, laid end to end along the dimension named above; an argument that names none is the same for every part. Nothing has to cross between parts.
Inputs may be any that keep to these rules, and one draw needn't show every extreme that they name: The rows of history_cache at and past prompt_start are not read. `decode_lengths`: rows of decode_cache at and past a request's length are not read.
All inputs are finite; a program needn't handle non-finite values.
Results may differ from the reference program's by a relative error of at most 0.017.
Values may be sent and summed in bfloat16 or wider, within the bound.
No kernel may reach another device: no remote copies, remote signals or barrier semaphores. Data moves between devices by JAX's collectives and lax.ppermute only.
A program may use at most 64 MiB of HBM per device.

```python
import jax
import jax.numpy as jnp
from jax import lax

D = 4096
HEADS = 32
KV_HEADS = 4
HEAD_DIM = 128
PROMPT = 496
DECODE = 16
HISTORY = 1024
CACHE = 768
TOKENS = 512
N_TP = 4


def spread_queries(key, row_count):
    values = jnp.clip(2.0 * jax.random.normal(key, (row_count, HEADS * HEAD_DIM), jnp.float32), -12.0, 12.0)
    return values.astype(jnp.bfloat16)


def draw_prompt_queries(key, part):
    return spread_queries(jax.random.fold_in(key, 3), PROMPT)


def draw_decode_queries(key, part):
    return spread_queries(jax.random.fold_in(key, 5), DECODE)


def place_ends(entries, key, least, high):
    shape = entries.shape
    spot = [jax.random.randint(jax.random.fold_in(key, axis), (), 0, shape[axis]) for axis in range(len(shape))]
    entries = entries.at[tuple(spot)].set(least)
    longest = shape.index(max(shape))
    spot[longest] = (spot[longest] + 1) % shape[longest]
    return entries.at[tuple(spot)].set(high)


def shard_levels(stream_key, shape, split, least, top_value):
    gain = 1.0
    for dim, shards_of in split:
        heights = jax.random.uniform(jax.random.fold_in(jax.random.fold_in(stream_key, 6), dim), (shards_of,), jnp.float32, least / len(split), top_value / len(split))
        gain = gain * jnp.repeat(jnp.exp(heights), shape[dim] // shards_of).reshape((-1,) + (1,) * (len(shape) - 1 - dim))
    return gain


def bell_draw(own_key, extent, deviation, limit, cuts=(), kind=jnp.bfloat16):
    values = jax.random.normal(own_key, extent, jnp.float32) * deviation
    if len(cuts) > 0:
        values = shard_levels(own_key, extent, cuts, -0.22, 0.18) * values
    return jnp.clip(values, min=-limit, max=limit).astype(kind)


def setup_inputs(seed: int = 0, part: int = 0) -> dict:
    key_list = jax.random.split(jax.random.key(seed), 12)
    part_splits = jax.random.split(jax.random.fold_in(key_list[11], part), 12)
    return {
        "prompt_queries": draw_prompt_queries(jax.random.fold_in(jax.random.fold_in(key_list[11], part), 71), part),
        "prompt_entries": bell_draw(part_splits[1], (2, PROMPT, KV_HEADS * HEAD_DIM), 1.0, 6.0, ((1, 4),)),
        "history_cache": bell_draw(part_splits[2], (2, HISTORY, KV_HEADS * HEAD_DIM), 1.0, 6.0, ((1, 4),)),
        "decode_queries": draw_decode_queries(jax.random.fold_in(jax.random.fold_in(key_list[11], part), 71), part),
        "decode_entries": bell_draw(part_splits[4], (2, DECODE, KV_HEADS * HEAD_DIM), 1.0, 6.0),
        "decode_cache": bell_draw(part_splits[5], (2, DECODE, CACHE, KV_HEADS * HEAD_DIM), 1.0, 6.0, ((2, 4),)),
        "decode_lengths": place_ends(jax.random.randint(part_splits[6], (DECODE,), 1, CACHE + 1), jax.random.fold_in(part_splits[6], 1), 1, CACHE).astype(jnp.int32),
        "prompt_start": jax.random.randint(part_splits[7], (1,), HISTORY // 2, HISTORY + 1).astype(jnp.int32),
        "out_weight": bell_draw(key_list[8], (HEADS * HEAD_DIM, D), (HEADS * HEAD_DIM) ** -0.5, 0.09375, ((0, 4),)),
        "residual": bell_draw(part_splits[9], (TOKENS, D), 0.3, 4.0, ((0, 4),)),
        "norm_gain": jnp.clip(1.0 + 0.1 * jax.random.normal(key_list[10], (D,), jnp.float32), 0.5, 1.5),
    }


def weighted(scores, valid):
    masked = jnp.where(valid, scores, -jnp.inf)
    highest = lax.optimization_barrier(jnp.max(masked, axis=-1, keepdims=True))
    weights = jnp.where(valid, jnp.exp(scores - highest), 0.0)
    totals = lax.optimization_barrier(jnp.sum(weights, axis=-1))
    rounded = lax.optimization_barrier(weights.astype(jnp.bfloat16)).astype(jnp.float32)
    return (rounded, totals)

def prompt_attention(prompt_queries, prompt_entries, history_cache, start):
    group = HEADS // KV_HEADS
    scale = HEAD_DIM ** (-0.5)
    keys = jnp.concatenate([history_cache[0], prompt_entries[0]], axis=0).reshape(HISTORY + PROMPT, KV_HEADS, HEAD_DIM)
    values = jnp.concatenate([history_cache[1], prompt_entries[1]], axis=0).reshape(HISTORY + PROMPT, KV_HEADS, HEAD_DIM)
    queries = prompt_queries.reshape(PROMPT, KV_HEADS, group, HEAD_DIM)
    slots = jnp.arange(HISTORY + PROMPT, dtype=jnp.int32)[None, :]
    places = jnp.arange(PROMPT, dtype=jnp.int32)[:, None]
    valid = jnp.where(slots < HISTORY, slots < start, slots - HISTORY <= places)

    def one_head(inputs):
        query_block, key_block, value_block = inputs
        scores = jnp.einsum('tgd,pd->tgp', query_block.astype(jnp.float32), key_block.astype(jnp.float32)) * scale
        weights, totals = weighted(scores, valid[:, None, :])
        summed = jnp.einsum('tgp,pd->tgd', weights, value_block.astype(jnp.float32))
        return (summed / totals[..., None]).astype(jnp.bfloat16)
    outputs = lax.map(one_head, (queries.transpose(1, 0, 2, 3), keys.transpose(1, 0, 2), values.transpose(1, 0, 2)))
    return outputs.transpose(1, 0, 2, 3).reshape(PROMPT, HEADS * HEAD_DIM)

def decode_attention(decode_queries, decode_entries, decode_cache, lengths):
    group = HEADS // KV_HEADS
    scale = HEAD_DIM ** (-0.5)
    keys = jnp.concatenate([decode_cache[0].reshape(DECODE, CACHE, KV_HEADS, HEAD_DIM), decode_entries[0].reshape(DECODE, 1, KV_HEADS, HEAD_DIM)], axis=1)
    values = jnp.concatenate([decode_cache[1].reshape(DECODE, CACHE, KV_HEADS, HEAD_DIM), decode_entries[1].reshape(DECODE, 1, KV_HEADS, HEAD_DIM)], axis=1)
    slots = jnp.arange(CACHE + 1, dtype=jnp.int32)[None, :]
    valid = (slots < lengths[:, None]) | (slots == CACHE)
    queries = decode_queries.reshape(DECODE, KV_HEADS, group, HEAD_DIM)
    scores = jnp.einsum('bkgd,bpkd->bkgp', queries.astype(jnp.float32), keys.astype(jnp.float32)) * scale
    weights, totals = weighted(scores, valid[:, None, None, :])
    summed = jnp.einsum('bkgp,bpkd->bkgd', weights, values.astype(jnp.float32))
    return (summed / totals[..., None]).astype(jnp.bfloat16).reshape(DECODE, HEADS * HEAD_DIM)

def reference(prompt_queries, prompt_entries, history_cache, decode_queries, decode_entries, decode_cache, decode_lengths, prompt_start, out_weight, residual, norm_gain):
    prompt_out = prompt_attention(prompt_queries, prompt_entries, history_cache, prompt_start[0])
    decode_out = decode_attention(decode_queries, decode_entries, decode_cache, decode_lengths)
    attended = jnp.concatenate([prompt_out, decode_out], axis=0)
    width = HEADS * HEAD_DIM // N_TP
    projected = jnp.zeros((TOKENS, D), jnp.float32)
    for block in range(N_TP):
        partial_value = jnp.dot(attended[:, block * width:(block + 1) * width], out_weight[block * width:(block + 1) * width], preferred_element_type=jnp.float32)
        projected = projected + lax.optimization_barrier(partial_value.astype(jnp.bfloat16)).astype(jnp.float32)
    hidden = residual.astype(jnp.float32) + projected
    mean_square = lax.optimization_barrier(jnp.mean(hidden * hidden, axis=-1, keepdims=True))
    normed = (hidden * lax.rsqrt(mean_square + 1e-05) * norm_gain).astype(jnp.bfloat16)
    return (hidden.astype(jnp.bfloat16), normed)
```

```python
import jax
import jax.numpy as jnp
import numpy as np
from jax import lax
from jax.experimental import pallas as pl
from jax.experimental.pallas import tpu as pltpu
from jax.sharding import PartitionSpec as P

HEAD_DIM = 128
MASKED = -1e30
EPS = 1e-05
CHUNKS = (64, 64)
COLUMNS = 512

F32 = jnp.float32
BF16 = jnp.bfloat16


def round_up(value, unit):
    return -(-value // unit) * unit


def smem():
    return pl.BlockSpec(memory_space=pltpu.SMEM)


def hbm():
    return pl.BlockSpec(memory_space=pl.ANY)


def params(mib, **kwargs):
    return pltpu.CompilerParams(vmem_limit_bytes=mib << 20, **kwargs)


def pack(history, prompt, meta, devices, local_heads, group):
    h_rows, p_rows = history.shape[1], prompt.shape[1]
    p_pad = round_up(p_rows, 16)
    span = h_rows + p_pad

    def head_of(k):
        return lambda i, m: (0, 0, (m[0] ^ k) * local_heads // group)

    def body(m, *refs):
        for k in range(devices):
            h_ref, p_ref, o_ref = refs[k], refs[devices + k], refs[2 * devices + k]
            for part in range(2):
                o_ref[part, 0:h_rows, :] = h_ref[part]
                if p_pad > p_rows:
                    rows = jnp.concatenate(
                        [p_ref[part].astype(F32), jnp.zeros((p_pad - p_rows, HEAD_DIM), F32)], axis=0
                    )
                    o_ref[part, h_rows:span, :] = rows.astype(BF16)
                else:
                    o_ref[part, h_rows:span, :] = p_ref[part]

    return pl.pallas_call(
        body,
        grid_spec=pltpu.PrefetchScalarGridSpec(
            num_scalar_prefetch=1,
            grid=(1,),
            in_specs=[pl.BlockSpec((2, h_rows, HEAD_DIM), head_of(k)) for k in range(devices)]
            + [pl.BlockSpec((2, p_rows, HEAD_DIM), head_of(k)) for k in range(devices)],
            out_specs=[pl.BlockSpec((2, span, HEAD_DIM), lambda i, m: (0, 0, 0))] * devices,
        ),
        out_shape=[jax.ShapeDtypeStruct((2, span, HEAD_DIM), BF16)] * devices,
        compiler_params=params(16),
        name="pack",
    )(meta, *([history] * devices), *([prompt] * devices))


def decode_partials(queries, cache, lengths, meta, local_heads, group):
    devices = len(queries)
    rows, span, width = cache.shape[1], cache.shape[2], cache.shape[3]
    kv_heads = width // HEAD_DIM
    heads = devices * local_heads
    scale = HEAD_DIM ** (-0.5)
    step = 4
    part_rows = rows * local_heads
    stat_rows = round_up(local_heads, 8)

    def body(m, lens, *refs):
        q_refs, cache_ref = refs[:devices], refs[devices]
        o_refs = refs[devices + 1 : 2 * devices + 1]
        q_all, stats = refs[2 * devices + 1 :]
        me = m[0]

        @pl.when(pl.program_id(0) == 0)
        def _():
            for k in range(devices):
                for h in range(local_heads):
                    q_all[k, pl.ds(h, rows, stride=local_heads), :] = q_refs[k][
                        :, h * HEAD_DIM : (h + 1) * HEAD_DIM
                    ].astype(F32)
            stats[...] = jnp.zeros_like(stats)

        slot = lax.broadcasted_iota(jnp.int32, (heads, 1), 0) // local_heads
        reads = ((slot ^ me) * local_heads) // group
        lane = lax.broadcasted_iota(jnp.int32, (heads, HEAD_DIM), 1)
        place = me * span + lax.broadcasted_iota(jnp.int32, (1, span), 1)
        for r in range(step):
            b = pl.program_id(0) * step + r
            start = pl.multiple_of(b * local_heads, local_heads)
            q = jnp.concatenate([q_all[k, pl.ds(start, local_heads), :] for k in range(devices)], axis=0)
            spread = jnp.concatenate(
                [jnp.where(reads == g, q, 0.0) for g in range(kv_heads)], axis=1
            ).astype(BF16)
            scores = lax.dot_general(
                spread, cache_ref[0, r], (((1,), (1,)), ((), ())), preferred_element_type=F32
            )
            scores = scores * scale
            valid = place < lens[b]
            top = jnp.max(jnp.where(valid, scores, MASKED), axis=-1, keepdims=True)
            weights = jnp.where(valid, jnp.exp(scores - top), 0.0)
            total = jnp.sum(weights, axis=-1, keepdims=True)
            summed = jnp.dot(weights.astype(BF16), cache_ref[1, r], preferred_element_type=F32)
            own = jnp.zeros((heads, HEAD_DIM), F32)
            for g in range(kv_heads):
                own = own + jnp.where(reads == g, summed[:, g * HEAD_DIM : (g + 1) * HEAD_DIM], 0.0)
            for k in range(devices):
                o_refs[k][pl.ds(start, local_heads), :] = own[k * local_heads : (k + 1) * local_heads]
            stats[...] = jnp.where(lane == b, top, jnp.where(lane == rows + b, total, stats[...]))

        @pl.when(pl.program_id(0) == pl.num_programs(0) - 1)
        def _():
            for k in range(devices):
                o_refs[k][part_rows : part_rows + local_heads, :] = stats[
                    k * local_heads : (k + 1) * local_heads, :
                ]

    full = lambda i, m, n: (0, 0)
    return pl.pallas_call(
        body,
        grid_spec=pltpu.PrefetchScalarGridSpec(
            num_scalar_prefetch=2,
            grid=(rows // step,),
            in_specs=[pl.BlockSpec(queries[0].shape, full)] * devices
            + [pl.BlockSpec((2, step, span, width), lambda i, m, n: (0, i, 0, 0))],
            out_specs=[pl.BlockSpec((part_rows + stat_rows, HEAD_DIM), full)] * devices,
            scratch_shapes=[
                pltpu.VMEM((devices, part_rows, HEAD_DIM), F32),
                pltpu.VMEM((heads, HEAD_DIM), F32),
            ],
        ),
        out_shape=[jax.ShapeDtypeStruct((part_rows + stat_rows, HEAD_DIM), F32)] * devices,
        compiler_params=params(24),
        name="decode",
    )(meta, lengths, *queries, cache)


def decode_join(parts, queries, entries, meta, local_heads, group):
    devices = len(parts)
    rows = queries.shape[0]
    scale = HEAD_DIM ** (-0.5)
    part_rows = rows * local_heads

    def body(m, *refs):
        p_refs = refs[:devices]
        q_ref, e_ref, o_ref, q_all, out = refs[devices:]
        for h in range(local_heads):
            q_all[pl.ds(h, rows, stride=local_heads), :] = q_ref[:, h * HEAD_DIM : (h + 1) * HEAD_DIM].astype(F32)
        stats = [p[part_rows : part_rows + local_heads, :] for p in p_refs]
        keys, values = e_ref[0].astype(F32), e_ref[1].astype(F32)
        for b in range(rows):
            here = slice(b * local_heads, (b + 1) * local_heads)
            own = jnp.sum(q_all[here, :] * keys[b : b + 1, :], axis=-1, keepdims=True) * scale
            tops = [s[:, b : b + 1] for s in stats]
            top = own
            for t in tops:
                top = jnp.maximum(top, t)
            weight = jnp.exp(own - top)
            total = weight
            summed = weight.astype(BF16).astype(F32) * values[b : b + 1, :]
            for s, t, p in zip(stats, tops, p_refs):
                factor = jnp.exp(t - top)
                total = total + factor * s[:, rows + b : rows + b + 1]
                summed = summed + factor * p[here, :]
            out[here, :] = summed / total
        for h in range(local_heads):
            o_ref[:, h * HEAD_DIM : (h + 1) * HEAD_DIM] = out[pl.ds(h, rows, stride=local_heads), :].astype(BF16)

    full = lambda i, m: (0, 0)
    return pl.pallas_call(
        body,
        grid_spec=pltpu.PrefetchScalarGridSpec(
            num_scalar_prefetch=1,
            grid=(1,),
            in_specs=[pl.BlockSpec(parts[0].shape, full)] * devices
            + [
                pl.BlockSpec(queries.shape, full),
                pl.BlockSpec((2, rows, HEAD_DIM), lambda i, m: (0, 0, m[0] * local_heads // group)),
            ],
            out_specs=pl.BlockSpec((rows, local_heads * HEAD_DIM), full),
            scratch_shapes=[pltpu.VMEM((part_rows, HEAD_DIM), F32)] * 2,
        ),
        out_shape=jax.ShapeDtypeStruct((rows, local_heads * HEAD_DIM), BF16),
        compiler_params=params(16),
        name="join",
    )(meta, *parts, queries, entries)


def attend(slots, first, count, block, queries, decode_queries, kv, decoded, weight, meta, h_rows, p_rows):
    devices = len(kv)
    span = kv[0].shape[1]
    prompt_rows, local_width = queries.shape
    decode_rows = decode_queries.shape[0]
    local_heads = local_width // HEAD_DIM
    model = weight.shape[1]
    keys = devices * span
    order = [s for s in slots if s % 2 == 0] + [s for s in slots if s % 2 == 1]
    half = len(order) // 2 * count
    factor = HEAD_DIM ** (-0.5) * float(np.log2(np.e))
    pieces = model // COLUMNS
    has_decode = first + count == block

    def body(m, q_hbm, dq_hbm, *refs):
        kv_hbm = refs[:devices]
        dec_ref, w_hbm, keep_ref, give_ref = refs[devices : devices + 4]
        q, k_all, v_all, w, att, q_sem, kv_sem, w_sem = refs[devices + 4 :]
        me, valid_rows = m[0], m[1]
        q_copies = [
            pltpu.make_async_copy(q_hbm, q.at[0:prompt_rows, :], q_sem.at[0]),
            pltpu.make_async_copy(dq_hbm, q.at[prompt_rows : prompt_rows + decode_rows, :], q_sem.at[1]),
        ]
        kv_copies = []
        for k in range(devices):
            for part, dst in ((0, k_all), (1, v_all)):
                kv_copies.append(
                    pltpu.make_async_copy(
                        kv_hbm[k].at[part], dst.at[k * span : (k + 1) * span, :], kv_sem.at[2 * k + part]
                    )
                )
        w_copies = [
            pltpu.make_async_copy(w_hbm.at[:, c * COLUMNS : (c + 1) * COLUMNS], w.at[c], w_sem.at[c])
            for c in range(pieces)
        ]
        for copy in q_copies + kv_copies + w_copies:
            copy.start()

        column = lax.broadcasted_iota(jnp.int32, (1, keys), 1)
        source = (column // span) ^ me
        inner = column % span
        history = jnp.where(source * h_rows + inner < valid_rows, -1, 1 << 20)
        fresh = jnp.where(inner - h_rows < p_rows, source * p_rows + inner - h_rows, 1 << 20)
        seen_from = jnp.where(inner < h_rows, history, fresh)
        for copy in q_copies + kv_copies:
            copy.wait()
        for i, slot in enumerate(order):
            target = slot ^ me
            row0 = pl.multiple_of(target * block + first, 16)
            rows = row0 + lax.broadcasted_iota(jnp.int32, (count, 1), 0)
            bias = jnp.where(seen_from <= rows, 0.0, MASKED)
            for h in range(local_heads):
                here = slice(h * HEAD_DIM, (h + 1) * HEAD_DIM)
                scores = lax.dot_general(
                    q[pl.ds(row0, count), here], k_all[...], (((1,), (1,)), ((), ())), preferred_element_type=F32
                )
                scores = scores + bias
                top = jnp.max(scores, axis=-1, keepdims=True)
                weights = jnp.exp2((scores - top) * factor)
                total = jnp.sum(weights, axis=-1, keepdims=True)
                summed = jnp.dot(weights.astype(BF16), v_all[...], preferred_element_type=F32)
                att[i * count : (i + 1) * count, here] = (summed / total).astype(BF16)
            if has_decode:

                @pl.when(target == devices - 1)
                def _():
                    att[(i + 1) * count - decode_rows : (i + 1) * count, :] = dec_ref[...]

        for c in range(pieces):
            w_copies[c].wait()
            out = jnp.dot(att[...], w[c], preferred_element_type=F32).astype(BF16)
            keep_ref[:, c * COLUMNS : (c + 1) * COLUMNS] = out[:half]
            give_ref[:, c * COLUMNS : (c + 1) * COLUMNS] = out[half:]

    vmem = pl.BlockSpec(memory_space=pltpu.VMEM)
    flops = 2 * len(order) * count * (2 * local_width * keys + local_width * model)
    return pl.pallas_call(
        body,
        in_specs=[smem(), hbm(), hbm()] + [hbm()] * devices + [vmem, hbm()],
        out_specs=[vmem, vmem],
        out_shape=[jax.ShapeDtypeStruct((half, model), BF16)] * 2,
        scratch_shapes=[
            pltpu.VMEM((prompt_rows + decode_rows, local_width), BF16),
            pltpu.VMEM((keys, HEAD_DIM), BF16),
            pltpu.VMEM((keys, HEAD_DIM), BF16),
            pltpu.VMEM((pieces, local_width, COLUMNS), BF16),
            pltpu.VMEM((2 * half, local_width), BF16),
            pltpu.SemaphoreType.DMA((2,)),
            pltpu.SemaphoreType.DMA((2 * devices,)),
            pltpu.SemaphoreType.DMA((pieces,)),
        ],
        compiler_params=params(40),
        cost_estimate=pl.CostEstimate(flops=flops, transcendentals=0, bytes_accessed=weight.size * 2),
        name=f"attend_{slots[0]}_{first}",
    )(meta, queries, decode_queries, *kv, decoded, weight)


def finish(first, residual, own, given, crossed, gain, previous):
    block, model = residual.shape
    count = crossed[0].shape[0]
    tile = 16
    n_cross = len(crossed)

    def body(res_ref, own_ref, given_ref, *refs):
        cross = refs[:n_cross]
        gain_ref = refs[n_cross]
        hidden_ref, normed_ref = refs[-2:]
        hidden = res_ref[...].astype(F32) + own_ref[...].astype(F32) + given_ref[...].astype(F32)
        for c in cross:
            hidden = hidden + c[...].astype(F32)
        mean = jnp.mean(hidden * hidden, axis=-1, keepdims=True)
        hidden_ref[...] = hidden.astype(BF16)
        normed_ref[...] = (hidden * lax.rsqrt(mean + EPS) * gain_ref[...]).astype(BF16)

    here = pl.BlockSpec((tile, model), lambda i: (first // tile + i, 0))
    local = pl.BlockSpec((tile, model), lambda i: (i, 0))
    n_in = 3 + n_cross + 1
    return pl.pallas_call(
        body,
        grid=(count // tile,),
        in_specs=[here, here, here]
        + [local] * n_cross
        + [pl.BlockSpec((1, model), lambda i: (0, 0))]
        + [hbm()] * len(previous),
        out_specs=[here, here],
        out_shape=[jax.ShapeDtypeStruct((block, model), BF16)] * 2,
        input_output_aliases={n_in + i: i for i in range(len(previous))},
        compiler_params=params(16),
        name=f"finish_{first}",
    )(residual, own, given, *crossed, gain, *previous)


def per_device(
    prompt_queries,
    prompt_entries,
    history_cache,
    decode_queries,
    decode_entries,
    decode_cache,
    decode_lengths,
    prompt_start,
    out_weight,
    residual,
    norm_gain,
):
    devices = lax.axis_size("tp")
    local_heads = prompt_queries.shape[1] // HEAD_DIM
    kv_heads = history_cache.shape[2] // HEAD_DIM
    group = devices * local_heads // kv_heads
    block = residual.shape[0]
    h_rows, p_rows = history_cache.shape[1], prompt_entries.shape[1]
    assert group % local_heads == 0 and devices & (devices - 1) == 0
    assert block >= decode_queries.shape[0]
    meta = jnp.concatenate([lax.axis_index("tp").astype(jnp.int32)[None], prompt_start])

    def swap(value, k):
        return lax.ppermute(value, "tp", [(i, i ^ k) for i in range(devices)])

    queries = [decode_queries] + [swap(decode_queries, k) for k in range(1, devices)]
    packed = pack(history_cache, prompt_entries, meta, devices, local_heads, group)
    kv = [packed[0]] + [swap(packed[k], k) for k in range(1, devices)]
    parts = decode_partials(queries, decode_cache, decode_lengths, meta, local_heads, group)
    parts = [parts[0]] + [swap(parts[k], k) for k in range(1, devices)]
    decoded = decode_join(parts, decode_queries, decode_entries, meta, local_heads, group)

    def attended(slots, first, count):
        return attend(
            slots, first, count, block, prompt_queries, decode_queries, kv, decoded, out_weight, meta, h_rows, p_rows
        )

    chunks = [c * block // sum(CHUNKS) for c in CHUNKS]
    if any(c % 16 for c in chunks):
        chunks = [block]
    crossed, first = [], 0
    for count in chunks:
        keep, give = attended(list(range(2, devices)), first, count)
        taken = swap(give, 1)
        pair = (keep.astype(F32) + taken.astype(F32)).astype(BF16)
        crossed.append(
            (first, [swap(pair[(k // 2 - 1) * count : k // 2 * count], k) for k in range(2, devices, 2)])
        )
        first += count
    own, give = attended([0, 1], 0, block)
    given = swap(give, 1)
    gain = norm_gain[None, :]
    outs = []
    for first, pieces in crossed:
        outs = finish(first, residual, own, given, pieces, gain, outs)
    return tuple(outs)


def solution(mesh):
    placed = (
        P("rep", "tp"),
        P("rep", "tp", None),
        P("rep", "tp", None),
        P("rep", "tp"),
        P("rep", None, None),
        P("rep", None, "tp", None),
        P("rep"),
        P("rep"),
        P("tp", None),
        P("tp", "rep"),
        P(),
    )
    return jax.shard_map(
        per_device,
        mesh=mesh,
        in_specs=placed,
        out_specs=(P("tp", "rep"), P("tp", "rep")),
        check_vma=False,
    )
```

```python
import jax
import jax.numpy as jnp
import numpy as np
from jax import lax
from jax.experimental import pallas as pl
from jax.experimental.pallas import tpu as pltpu
from jax.sharding import PartitionSpec as P


HEAD_DIM = 128
MASKED = -1e30
EPS = 1e-05
CHUNKS = (64, 64)
COLUMNS = 512

F32 = jnp.float32
BF16 = jnp.bfloat16


def round_up(value, unit):
    return -(-value // unit) * unit


def smem():
    return pl.BlockSpec(memory_space=pltpu.SMEM)


def hbm():
    return pl.BlockSpec(memory_space=pl.ANY)


def in_hbm():
    return pl.BlockSpec(memory_space=pltpu.HBM)


def in_vmem():
    return pl.BlockSpec(memory_space=pltpu.VMEM)


def to_hbm(value):
    return pltpu.with_memory_space_constraint(value, pltpu.HBM)


def params(mib, **kwargs):
    return pltpu.CompilerParams(vmem_limit_bytes=mib << 20, **kwargs)


def pack_history(history, queries, meta, devices, local_heads, group):
    h_rows = history.shape[1]
    rows = queries.shape[0]
    span = 2 * h_rows + rows * local_heads

    def head_of(k):
        return lambda i, m: (0, 0, (m[0] ^ k) * local_heads // group)

    def body(m, *refs):
        q_ref = refs[devices]
        for k in range(devices):
            h_ref, o_ref = refs[k], refs[devices + 1 + k]
            for part in range(2):
                o_ref[part * h_rows : (part + 1) * h_rows, :] = h_ref[part]
            for h in range(local_heads):
                row = 2 * h_rows + h * rows
                o_ref[row : row + rows, :] = q_ref[:, h * HEAD_DIM : (h + 1) * HEAD_DIM]

    return pl.pallas_call(
        body,
        grid_spec=pltpu.PrefetchScalarGridSpec(
            num_scalar_prefetch=1,
            grid=(1,),
            in_specs=[pl.BlockSpec((2, h_rows, HEAD_DIM), head_of(k)) for k in range(devices)]
            + [pl.BlockSpec(queries.shape, lambda i, m: (0, 0))],
            out_specs=[pl.BlockSpec((span, HEAD_DIM), lambda i, m: (0, 0))] * devices,
        ),
        out_shape=[jax.ShapeDtypeStruct((span, HEAD_DIM), BF16)] * devices,
        compiler_params=params(8),
        name="pack_history",
    )(meta, *([to_hbm(history)] * devices), to_hbm(queries))


def stage(prompt, cache, prompt_queries, decode_queries, meta, devices, local_heads, group):
    p_rows = prompt.shape[1]
    p_pad = round_up(p_rows, 16)
    prompt_rows, decode_rows = prompt_queries.shape[0], decode_queries.shape[0]
    parts = 4
    per = cache.shape[1] // parts

    def head_of(k):
        return lambda i, m: (0, 0, (m[0] ^ k) * local_heads // group)

    def body(m, *refs):
        cache_hbm, q_hbm, dq_hbm = refs[devices : devices + 3]
        o_refs = refs[devices + 3 : 2 * devices + 3]
        cache_ref, q_ref, sem = refs[2 * devices + 3 :]
        copies = [
            pltpu.make_async_copy(q_hbm, q_ref.at[0:prompt_rows, :], sem.at[0]),
            pltpu.make_async_copy(dq_hbm, q_ref.at[prompt_rows : prompt_rows + decode_rows, :], sem.at[1]),
        ]
        for i in range(2 * parts):
            here = (i // parts, slice(i % parts * per, (i % parts + 1) * per))
            copies.append(pltpu.make_async_copy(cache_hbm.at[here], cache_ref.at[here], sem.at[2 + i]))
        for copy in copies:
            copy.start()
        for k in range(devices):
            p_ref, o_ref = refs[k], o_refs[k]
            for part in range(2):
                if p_pad > p_rows:
                    fresh = jnp.concatenate(
                        [p_ref[part].astype(F32), jnp.zeros((p_pad - p_rows, HEAD_DIM), F32)], axis=0
                    ).astype(BF16)
                else:
                    fresh = p_ref[part]
                o_ref[part * p_pad : (part + 1) * p_pad, :] = fresh
        for copy in copies:
            copy.wait()

    outs = pl.pallas_call(
        body,
        grid_spec=pltpu.PrefetchScalarGridSpec(
            num_scalar_prefetch=1,
            grid=(1,),
            in_specs=[pl.BlockSpec((2, p_rows, HEAD_DIM), head_of(k)) for k in range(devices)] + [in_hbm()] * 3,
            out_specs=[pl.BlockSpec((2 * p_pad, HEAD_DIM), lambda i, m: (0, 0))] * devices + [hbm(), hbm()],
            scratch_shapes=[pltpu.SemaphoreType.DMA((2 + 2 * parts,))],
        ),
        out_shape=[jax.ShapeDtypeStruct((2 * p_pad, HEAD_DIM), BF16)] * devices
        + [
            pltpu.VMEM(cache.shape, BF16),
            pltpu.VMEM((prompt_rows + decode_rows, prompt_queries.shape[1]), BF16),
        ],
        compiler_params=params(8),
        name="stage",
    )(meta, *([prompt] * devices), to_hbm(cache), to_hbm(prompt_queries), to_hbm(decode_queries))
    return outs[:devices], outs[devices], outs[devices + 1]


def decode_partials(history, cache, meta, h_rows, local_heads, group):
    devices = len(history)
    rows, span, width = cache.shape[1], cache.shape[2], cache.shape[3]
    kv_heads = width // HEAD_DIM
    heads = devices * local_heads
    factor = HEAD_DIM ** (-0.5) * float(np.log2(np.e))
    part_rows = rows * local_heads
    stat_rows = round_up(local_heads, 8)

    def body(m, *refs):
        h_refs, cache_ref = refs[:devices], refs[devices]
        o_refs = refs[devices + 1 : 2 * devices + 1]
        q_all = refs[2 * devices + 1]
        me = m[0]
        for k in range(devices):
            for h in range(local_heads):
                row = 2 * h_rows + h * rows
                q_all[k, pl.ds(h, rows, stride=local_heads), :] = h_refs[k][row : row + rows, :].astype(F32)

        slot = lax.broadcasted_iota(jnp.int32, (heads, 1), 0) // local_heads
        reads = ((slot ^ me) * local_heads) // group
        lane = lax.broadcasted_iota(jnp.int32, (heads, HEAD_DIM), 1)
        place = me * span + lax.broadcasted_iota(jnp.int32, (1, span), 1)
        scores = []
        for b in range(rows):
            here = slice(b * local_heads, (b + 1) * local_heads)
            q = jnp.concatenate([q_all[k, here, :] for k in range(devices)], axis=0)
            spread = jnp.concatenate(
                [jnp.where(reads == g, q, 0.0) for g in range(kv_heads)], axis=1
            ).astype(BF16)
            score = lax.dot_general(
                spread, cache_ref[0, b], (((1,), (1,)), ((), ())), preferred_element_type=F32
            )
            scores.append(jnp.where(place < m[2 + b], score, MASKED))
        scores = jnp.concatenate(scores, axis=0)
        top = jnp.max(scores, axis=-1, keepdims=True)
        weights = jnp.where(scores > 0.5 * MASKED, jnp.exp2((scores - top) * factor), 0.0)
        total = jnp.sum(weights, axis=-1, keepdims=True)
        weights = weights.astype(BF16)
        stats = jnp.zeros((heads, HEAD_DIM), F32)
        for b in range(rows):
            these = slice(b * heads, (b + 1) * heads)
            summed = jnp.dot(weights[these], cache_ref[1, b], preferred_element_type=F32)
            own = jnp.zeros((heads, HEAD_DIM), F32)
            for g in range(kv_heads):
                own = own + jnp.where(reads == g, summed[:, g * HEAD_DIM : (g + 1) * HEAD_DIM], 0.0)
            for k in range(devices):
                o_refs[k][b * local_heads : (b + 1) * local_heads, :] = own[k * local_heads : (k + 1) * local_heads]
            stats = jnp.where(lane == b, top[these], jnp.where(lane == rows + b, total[these], stats))
        for k in range(devices):
            o_refs[k][part_rows : part_rows + local_heads, :] = stats[k * local_heads : (k + 1) * local_heads, :]

    return pl.pallas_call(
        body,
        in_specs=[smem()] + [in_vmem()] * (devices + 1),
        out_specs=[in_vmem()] * devices,
        scratch_shapes=[pltpu.VMEM((devices, part_rows, HEAD_DIM), F32)],
        out_shape=[jax.ShapeDtypeStruct((part_rows + stat_rows, HEAD_DIM), F32)] * devices,
        compiler_params=params(16),
        name="decode",
    )(meta, *history, cache)


def decode_join(parts, history, entries, meta, h_rows, local_heads, group):
    devices = len(parts)
    rows = entries.shape[1]
    factor = HEAD_DIM ** (-0.5) * float(np.log2(np.e))
    part_rows = rows * local_heads

    def body(m, *refs):
        p_refs = refs[:devices]
        h_ref, e_ref, o_ref, q_all, out = refs[devices:]
        for h in range(local_heads):
            row = 2 * h_rows + h * rows
            q_all[pl.ds(h, rows, stride=local_heads), :] = h_ref[row : row + rows, :].astype(F32)
        stats = [p[part_rows : part_rows + local_heads, :] for p in p_refs]
        keys, values = e_ref[0].astype(F32), e_ref[1].astype(F32)
        for b in range(rows):
            here = slice(b * local_heads, (b + 1) * local_heads)
            own = jnp.sum(q_all[here, :] * keys[b : b + 1, :], axis=-1, keepdims=True)
            tops = [s[:, b : b + 1] for s in stats]
            top = own
            for t in tops:
                top = jnp.maximum(top, t)
            weight = jnp.exp2((own - top) * factor)
            total = weight
            summed = weight.astype(BF16).astype(F32) * values[b : b + 1, :]
            for s, t, p in zip(stats, tops, p_refs):
                share = jnp.exp2((t - top) * factor)
                total = total + share * s[:, rows + b : rows + b + 1]
                summed = summed + share * p[here, :]
            out[here, :] = summed / total
        for h in range(local_heads):
            o_ref[:, h * HEAD_DIM : (h + 1) * HEAD_DIM] = out[pl.ds(h, rows, stride=local_heads), :].astype(BF16)

    full = lambda i, m: (0, 0)
    return pl.pallas_call(
        body,
        grid_spec=pltpu.PrefetchScalarGridSpec(
            num_scalar_prefetch=1,
            grid=(1,),
            in_specs=[pl.BlockSpec(parts[0].shape, full)] * devices
            + [
                pl.BlockSpec(history.shape, full),
                pl.BlockSpec((2, rows, HEAD_DIM), lambda i, m: (0, 0, m[0] * local_heads // group)),
            ],
            out_specs=pl.BlockSpec((rows, local_heads * HEAD_DIM), full),
            scratch_shapes=[pltpu.VMEM((part_rows, HEAD_DIM), F32)] * 2,
        ),
        out_shape=jax.ShapeDtypeStruct((rows, local_heads * HEAD_DIM), BF16),
        compiler_params=params(8),
        name="join",
    )(meta, *parts, history, to_hbm(entries))


def attend(slots, first, count, block, queries, history, fresh, decoded, weight, meta, h_rows, p_rows):
    devices = len(history)
    p_pad = fresh[0].shape[0] // 2
    local_width = queries.shape[1]
    local_heads = local_width // HEAD_DIM
    model = weight.shape[1]
    h_keys, p_keys = devices * h_rows, devices * p_pad
    keys = h_keys + p_keys
    order = [s for s in slots if s % 2 == 0] + [s for s in slots if s % 2 == 1]
    half = len(order) // 2 * count
    factor = HEAD_DIM ** (-0.5) * float(np.log2(np.e))
    has_decode = decoded is not None
    decode_rows = decoded.shape[0] if has_decode else 0

    def body(m, q, *refs):
        h_refs, f_refs = refs[:devices], refs[devices : 2 * devices]
        rest = refs[2 * devices :]
        if has_decode:
            dec_ref, rest = rest[0], rest[1:]
        w, keep_ref, give_ref, k_all, v_all, att = rest
        me, valid_rows = m[0], m[1]
        for k in range(devices):
            for part, dst in ((0, k_all), (1, v_all)):
                dst[k * h_rows : (k + 1) * h_rows, :] = h_refs[k][part * h_rows : (part + 1) * h_rows, :]
                dst[h_keys + k * p_pad : h_keys + (k + 1) * p_pad, :] = f_refs[k][
                    part * p_pad : (part + 1) * p_pad, :
                ]
        column = lax.broadcasted_iota(jnp.int32, (1, h_keys), 1)
        place = ((column // h_rows) ^ me) * h_rows + column % h_rows
        history_bias = jnp.where(place < valid_rows, 0.0, MASKED)
        column = lax.broadcasted_iota(jnp.int32, (1, p_keys), 1)
        inner = column % p_pad
        seen_from = jnp.where(inner < p_rows, ((column // p_pad) ^ me) * p_rows + inner, 1 << 20)
        for i, slot in enumerate(order):
            target = slot ^ me
            row0 = pl.multiple_of(target * block + first, 16)
            rows = row0 + lax.broadcasted_iota(jnp.int32, (count, 1), 0)
            bias = jnp.where(seen_from <= rows, 0.0, MASKED)
            bias = jnp.concatenate([jnp.broadcast_to(history_bias, (count, h_keys)), bias], axis=1)
            for h in range(local_heads):
                here = slice(h * HEAD_DIM, (h + 1) * HEAD_DIM)
                scores = lax.dot_general(
                    q[pl.ds(row0, count), here], k_all[...], (((1,), (1,)), ((), ())), preferred_element_type=F32
                )
                scores = scores + bias
                top = jnp.max(scores, axis=-1, keepdims=True)
                weights = jnp.exp2((scores - top) * factor)
                total = jnp.sum(weights, axis=-1, keepdims=True)
                summed = jnp.dot(weights.astype(BF16), v_all[...], preferred_element_type=F32)
                att[i * count : (i + 1) * count, here] = (summed / total).astype(BF16)
            if has_decode:

                @pl.when(target == devices - 1)
                def _():
                    att[(i + 1) * count - decode_rows : (i + 1) * count, :] = dec_ref[...]

        for c in range(0, model, COLUMNS):
            out = jnp.dot(att[...], w[:, c : c + COLUMNS], preferred_element_type=F32).astype(BF16)
            keep_ref[:, c : c + COLUMNS] = out[:half]
            give_ref[:, c : c + COLUMNS] = out[half:]

    flops = 2 * len(order) * count * (2 * local_width * keys + local_width * model)
    n_vmem = 2 + 2 * devices + has_decode
    return pl.pallas_call(
        body,
        in_specs=[smem()] + [in_vmem()] * n_vmem,
        out_specs=[in_vmem()] * 2,
        out_shape=[jax.ShapeDtypeStruct((half, model), BF16)] * 2,
        scratch_shapes=[
            pltpu.VMEM((keys, HEAD_DIM), BF16),
            pltpu.VMEM((keys, HEAD_DIM), BF16),
            pltpu.VMEM((2 * half, local_width), BF16),
        ],
        compiler_params=params(24),
        cost_estimate=pl.CostEstimate(flops=flops, transcendentals=0, bytes_accessed=weight.size * 2),
    )(meta, queries, *history, *fresh, *([decoded] if has_decode else []), weight)


def finish(first, residual, own, given, crossed, gain, previous):
    block, model = residual.shape
    count = crossed[0].shape[0]
    tile = 16
    n_cross = len(crossed)

    def body(res_ref, own_ref, given_ref, *refs):
        cross = refs[:n_cross]
        gain_ref = refs[n_cross]
        hidden_ref, normed_ref = refs[-2:]
        hidden = res_ref[...].astype(F32) + own_ref[...].astype(F32) + given_ref[...].astype(F32)
        for c in cross:
            hidden = hidden + c[...].astype(F32)
        mean = jnp.mean(hidden * hidden, axis=-1, keepdims=True)
        hidden_ref[...] = hidden.astype(BF16)
        normed_ref[...] = (hidden * lax.rsqrt(mean + EPS) * gain_ref[...]).astype(BF16)

    here = pl.BlockSpec((tile, model), lambda i: (first // tile + i, 0))
    local = pl.BlockSpec((tile, model), lambda i: (i, 0))
    n_in = 3 + n_cross + 1
    return pl.pallas_call(
        body,
        grid=(count // tile,),
        in_specs=[here, here, here]
        + [local] * n_cross
        + [pl.BlockSpec((1, model), lambda i: (0, 0))]
        + [hbm()] * len(previous),
        out_specs=[here, here],
        out_shape=[jax.ShapeDtypeStruct((block, model), BF16)] * 2,
        input_output_aliases={n_in + i: i for i in range(len(previous))},
        compiler_params=params(16),
    )(residual, own, given, *crossed, gain, *previous)


def step(
    prompt_queries,
    prompt_entries,
    history_cache,
    decode_queries,
    decode_entries,
    decode_cache,
    decode_lengths,
    prompt_start,
    out_weight,
    residual,
    norm_gain,
):
    devices = lax.axis_size("tp")
    local_heads = prompt_queries.shape[1] // HEAD_DIM
    kv_heads = history_cache.shape[2] // HEAD_DIM
    group = devices * local_heads // kv_heads
    block = residual.shape[0]
    h_rows, p_rows = history_cache.shape[1], prompt_entries.shape[1]
    assert group % local_heads == 0 and devices & (devices - 1) == 0
    assert block >= decode_queries.shape[0]
    meta = jnp.concatenate([lax.axis_index("tp").astype(jnp.int32)[None], prompt_start, decode_lengths])

    def swap(value, k):
        return lax.ppermute(value, "tp", [(i, i ^ k) for i in range(devices)])

    def swapped(values):
        return [values[0]] + [swap(values[k], k) for k in range(1, devices)]

    history = swapped(pack_history(history_cache, decode_queries, meta, devices, local_heads, group))
    fresh, cache, queries = stage(
        prompt_entries, decode_cache, prompt_queries, decode_queries, meta, devices, local_heads, group
    )
    fresh = swapped(fresh)
    parts = swapped(decode_partials(history, cache, meta, h_rows, local_heads, group))
    decoded = decode_join(parts, history[0], decode_entries, meta, h_rows, local_heads, group)

    def attended(slots, first, count, decoded):
        return attend(slots, first, count, block, queries, history, fresh, decoded, out_weight, meta, h_rows, p_rows)

    chunks = [c * block // sum(CHUNKS) for c in CHUNKS]
    if any(c % 16 for c in chunks):
        chunks = [block]
    crossed, first = [], 0
    for count in chunks:
        keep, give = attended(list(range(2, devices)), first, count, decoded if first + count == block else None)
        taken = swap(give, 1)
        pair = (keep.astype(F32) + taken.astype(F32)).astype(BF16)
        crossed.append((first, [swap(pair[(k // 2 - 1) * count : k // 2 * count], k) for k in range(2, devices, 2)]))
        first += count
    own, give = attended([0, 1], 0, block, decoded)
    given = swap(give, 1)
    gain = norm_gain[None, :]
    outs = []
    for first, pieces in crossed:
        outs = finish(first, residual, own, given, pieces, gain, outs)
    return tuple(outs)


def solution(mesh):
    placed = (
        P("rep", "tp"),
        P("rep", "tp", None),
        P("rep", "tp", None),
        P("rep", "tp"),
        P("rep", None, None),
        P("rep", None, "tp", None),
        P("rep"),
        P("rep"),
        P("tp", None),
        P("tp", "rep"),
        P(),
    )
    return jax.shard_map(
        step,
        mesh=mesh,
        in_specs=placed,
        out_specs=(P("tp", "rep"), P("tp", "rep")),
        check_vma=False,
    )
```

```python
import jax
import jax.numpy as jnp
import numpy as np
from jax import lax
from jax.experimental import pallas as pl
from jax.experimental.pallas import tpu as pltpu
from jax.sharding import PartitionSpec as P


HEAD_DIM = 128
MASKED = -1e30
EPS = 1e-05
CHUNKS = (64, 64)
COLUMNS = 512
GROUP_ROWS = 256

F32 = jnp.float32
BF16 = jnp.bfloat16


def round_up(value, unit):
    return -(-value // unit) * unit


def smem():
    return pl.BlockSpec(memory_space=pltpu.SMEM)


def hbm():
    return pl.BlockSpec(memory_space=pl.ANY)


def in_hbm():
    return pl.BlockSpec(memory_space=pltpu.HBM)


def in_vmem():
    return pl.BlockSpec(memory_space=pltpu.VMEM)


def to_hbm(value):
    return pltpu.with_memory_space_constraint(value, pltpu.HBM)


def params(mib, **kwargs):
    return pltpu.CompilerParams(vmem_limit_bytes=mib << 20, **kwargs)


def pack_history(history, queries, meta, devices, local_heads, group):
    h_rows = history.shape[1]
    rows = queries.shape[0]
    span = 2 * h_rows + rows * local_heads

    def head_of(k):
        return lambda i, m: (0, 0, (m[0] ^ k) * local_heads // group)

    def body(m, *refs):
        q_ref = refs[devices]
        for k in range(devices):
            h_ref, o_ref = refs[k], refs[devices + 1 + k]
            for part in range(2):
                o_ref[part * h_rows : (part + 1) * h_rows, :] = h_ref[part]
            for h in range(local_heads):
                row = 2 * h_rows + h * rows
                o_ref[row : row + rows, :] = q_ref[:, h * HEAD_DIM : (h + 1) * HEAD_DIM]

    return pl.pallas_call(
        body,
        grid_spec=pltpu.PrefetchScalarGridSpec(
            num_scalar_prefetch=1,
            grid=(1,),
            in_specs=[pl.BlockSpec((2, h_rows, HEAD_DIM), head_of(k)) for k in range(devices)]
            + [pl.BlockSpec(queries.shape, lambda i, m: (0, 0))],
            out_specs=[pl.BlockSpec((span, HEAD_DIM), lambda i, m: (0, 0))] * devices,
        ),
        out_shape=[jax.ShapeDtypeStruct((span, HEAD_DIM), BF16)] * devices,
        compiler_params=params(8),
        name="pack_history",
    )(meta, *([to_hbm(history)] * devices), to_hbm(queries))


def pack_fresh(prompt, meta, devices, local_heads, group):
    p_rows = prompt.shape[1]
    p_pad = round_up(p_rows, 16)

    def head_of(k):
        return lambda i, m: (0, 0, (m[0] ^ k) * local_heads // group)

    def body(m, *refs):
        for k in range(devices):
            p_ref, o_ref = refs[k], refs[devices + k]
            for part in range(2):
                if p_pad > p_rows:
                    fresh = jnp.concatenate(
                        [p_ref[part].astype(F32), jnp.zeros((p_pad - p_rows, HEAD_DIM), F32)], axis=0
                    ).astype(BF16)
                else:
                    fresh = p_ref[part]
                o_ref[part * p_pad : (part + 1) * p_pad, :] = fresh

    return pl.pallas_call(
        body,
        grid_spec=pltpu.PrefetchScalarGridSpec(
            num_scalar_prefetch=1,
            grid=(1,),
            in_specs=[pl.BlockSpec((2, p_rows, HEAD_DIM), head_of(k)) for k in range(devices)],
            out_specs=[pl.BlockSpec((2 * p_pad, HEAD_DIM), lambda i, m: (0, 0))] * devices,
        ),
        out_shape=[jax.ShapeDtypeStruct((2 * p_pad, HEAD_DIM), BF16)] * devices,
        compiler_params=params(8),
        name="pack_fresh",
    )(meta, *([prompt] * devices))


def stage(cache, prompt_queries, decode_queries):
    prompt_rows, decode_rows = prompt_queries.shape[0], decode_queries.shape[0]
    parts = 4
    per = cache.shape[1] // parts

    def body(cache_hbm, q_hbm, dq_hbm, cache_ref, q_ref, sem):
        copies = [
            pltpu.make_async_copy(q_hbm, q_ref.at[0:prompt_rows, :], sem.at[0]),
            pltpu.make_async_copy(dq_hbm, q_ref.at[prompt_rows : prompt_rows + decode_rows, :], sem.at[1]),
        ]
        for i in range(2 * parts):
            here = (i // parts, slice(i % parts * per, (i % parts + 1) * per))
            copies.append(pltpu.make_async_copy(cache_hbm.at[here], cache_ref.at[here], sem.at[2 + i]))
        for copy in copies:
            copy.start()
        for copy in copies:
            copy.wait()

    return pl.pallas_call(
        body,
        in_specs=[in_hbm()] * 3,
        out_specs=[in_vmem()] * 2,
        out_shape=[
            pltpu.VMEM(cache.shape, BF16),
            pltpu.VMEM((prompt_rows + decode_rows, prompt_queries.shape[1]), BF16),
        ],
        scratch_shapes=[pltpu.SemaphoreType.DMA((2 + 2 * parts,))],
        compiler_params=params(2),
        name="stage",
    )(to_hbm(cache), to_hbm(prompt_queries), to_hbm(decode_queries))


def decode_partials(history, cache, meta, h_rows, local_heads, group):
    devices = len(history)
    rows, span, width = cache.shape[1], cache.shape[2], cache.shape[3]
    kv_heads = width // HEAD_DIM
    heads = devices * local_heads
    factor = HEAD_DIM ** (-0.5) * float(np.log2(np.e))
    part_rows = rows * local_heads
    stat_rows = round_up(local_heads, 8)

    def body(m, *refs):
        h_refs, cache_ref = refs[:devices], refs[devices]
        o_refs = refs[devices + 1 : 2 * devices + 1]
        q_all = refs[2 * devices + 1]
        me = m[0]
        for k in range(devices):
            for h in range(local_heads):
                row = 2 * h_rows + h * rows
                q_all[k, pl.ds(h, rows, stride=local_heads), :] = h_refs[k][row : row + rows, :].astype(F32)

        slot = lax.broadcasted_iota(jnp.int32, (heads, 1), 0) // local_heads
        reads = ((slot ^ me) * local_heads) // group
        lane = lax.broadcasted_iota(jnp.int32, (heads, HEAD_DIM), 1)
        place = me * span + lax.broadcasted_iota(jnp.int32, (1, span), 1)
        scores = []
        for b in range(rows):
            here = slice(b * local_heads, (b + 1) * local_heads)
            q = jnp.concatenate([q_all[k, here, :] for k in range(devices)], axis=0)
            spread = jnp.concatenate(
                [jnp.where(reads == g, q, 0.0) for g in range(kv_heads)], axis=1
            ).astype(BF16)
            score = lax.dot_general(
                spread, cache_ref[0, b], (((1,), (1,)), ((), ())), preferred_element_type=F32
            )
            scores.append(jnp.where(place < m[2 + b], score, MASKED))
        scores = jnp.concatenate(scores, axis=0)
        top = jnp.max(scores, axis=-1, keepdims=True)
        weights = jnp.where(scores > 0.5 * MASKED, jnp.exp2((scores - top) * factor), 0.0)
        total = jnp.sum(weights, axis=-1, keepdims=True)
        weights = weights.astype(BF16)
        stats = jnp.zeros((heads, HEAD_DIM), F32)
        for b in range(rows):
            these = slice(b * heads, (b + 1) * heads)
            summed = jnp.dot(weights[these], cache_ref[1, b], preferred_element_type=F32)
            own = jnp.zeros((heads, HEAD_DIM), F32)
            for g in range(kv_heads):
                own = own + jnp.where(reads == g, summed[:, g * HEAD_DIM : (g + 1) * HEAD_DIM], 0.0)
            for k in range(devices):
                o_refs[k][b * local_heads : (b + 1) * local_heads, :] = own[k * local_heads : (k + 1) * local_heads]
            stats = jnp.where(lane == b, top[these], jnp.where(lane == rows + b, total[these], stats))
        for k in range(devices):
            o_refs[k][part_rows : part_rows + local_heads, :] = stats[k * local_heads : (k + 1) * local_heads, :]

    return pl.pallas_call(
        body,
        in_specs=[smem()] + [in_vmem()] * (devices + 1),
        out_specs=[in_vmem()] * devices,
        scratch_shapes=[pltpu.VMEM((devices, part_rows, HEAD_DIM), F32)],
        out_shape=[jax.ShapeDtypeStruct((part_rows + stat_rows, HEAD_DIM), F32)] * devices,
        compiler_params=params(16),
        name="decode",
    )(meta, *history, cache)


def decode_join(parts, history, entries, meta, h_rows, local_heads, group):
    devices = len(parts)
    rows = entries.shape[1]
    factor = HEAD_DIM ** (-0.5) * float(np.log2(np.e))
    part_rows = rows * local_heads

    def body(m, *refs):
        p_refs = refs[:devices]
        h_ref, e_ref, o_ref, q_all, out = refs[devices:]
        for h in range(local_heads):
            row = 2 * h_rows + h * rows
            q_all[pl.ds(h, rows, stride=local_heads), :] = h_ref[row : row + rows, :].astype(F32)
        stats = [p[part_rows : part_rows + local_heads, :] for p in p_refs]
        keys, values = e_ref[0].astype(F32), e_ref[1].astype(F32)
        for b in range(rows):
            here = slice(b * local_heads, (b + 1) * local_heads)
            own = jnp.sum(q_all[here, :] * keys[b : b + 1, :], axis=-1, keepdims=True)
            tops = [s[:, b : b + 1] for s in stats]
            top = own
            for t in tops:
                top = jnp.maximum(top, t)
            weight = jnp.exp2((own - top) * factor)
            total = weight
            summed = weight.astype(BF16).astype(F32) * values[b : b + 1, :]
            for s, t, p in zip(stats, tops, p_refs):
                share = jnp.exp2((t - top) * factor)
                total = total + share * s[:, rows + b : rows + b + 1]
                summed = summed + share * p[here, :]
            out[here, :] = summed / total
        for h in range(local_heads):
            o_ref[:, h * HEAD_DIM : (h + 1) * HEAD_DIM] = out[pl.ds(h, rows, stride=local_heads), :].astype(BF16)

    full = lambda i, m: (0, 0)
    return pl.pallas_call(
        body,
        grid_spec=pltpu.PrefetchScalarGridSpec(
            num_scalar_prefetch=1,
            grid=(1,),
            in_specs=[pl.BlockSpec(parts[0].shape, full)] * devices
            + [
                pl.BlockSpec(history.shape, full),
                pl.BlockSpec((2, rows, HEAD_DIM), lambda i, m: (0, 0, m[0] * local_heads // group)),
            ],
            out_specs=pl.BlockSpec((rows, local_heads * HEAD_DIM), full),
            scratch_shapes=[pltpu.VMEM((part_rows, HEAD_DIM), F32)] * 2,
        ),
        out_shape=jax.ShapeDtypeStruct((rows, local_heads * HEAD_DIM), BF16),
        compiler_params=params(8),
        name="join",
    )(meta, *parts, history, to_hbm(entries))


def attend(slots, first, count, block, queries, history, fresh, decoded, weight, meta, h_rows, p_rows):
    devices = len(history)
    p_pad = fresh[0].shape[0] // 2
    local_width = queries.shape[1]
    local_heads = local_width // HEAD_DIM
    model = weight.shape[1]
    h_keys, p_keys = devices * h_rows, devices * p_pad
    keys = h_keys + p_keys
    order = [s for s in slots if s % 2 == 0] + [s for s in slots if s % 2 == 1]
    half = len(order) // 2 * count
    factor = HEAD_DIM ** (-0.5) * float(np.log2(np.e))
    per = max(1, min(local_heads, GROUP_ROWS // count))
    has_decode = decoded is not None
    decode_rows = decoded.shape[0] if has_decode else 0

    def body(m, q, *refs):
        h_refs, f_refs = refs[:devices], refs[devices : 2 * devices]
        rest = refs[2 * devices :]
        if has_decode:
            dec_ref, rest = rest[0], rest[1:]
        w, keep_ref, give_ref, k_all, v_all, att = rest
        me, valid_rows = m[0], m[1]
        for k in range(devices):
            for part, dst in ((0, k_all), (1, v_all)):
                dst[k * h_rows : (k + 1) * h_rows, :] = h_refs[k][part * h_rows : (part + 1) * h_rows, :]
                dst[h_keys + k * p_pad : h_keys + (k + 1) * p_pad, :] = f_refs[k][
                    part * p_pad : (part + 1) * p_pad, :
                ]
        column = lax.broadcasted_iota(jnp.int32, (1, h_keys), 1)
        place = ((column // h_rows) ^ me) * h_rows + column % h_rows
        history_bias = jnp.where(place < valid_rows, 0.0, MASKED)
        column = lax.broadcasted_iota(jnp.int32, (1, p_keys), 1)
        inner = column % p_pad
        seen_from = jnp.where(inner < p_rows, ((column // p_pad) ^ me) * p_rows + inner, 1 << 20)
        for i, slot in enumerate(order):
            target = slot ^ me
            row0 = pl.multiple_of(target * block + first, 16)
            rows = row0 + lax.broadcasted_iota(jnp.int32, (count, 1), 0)
            bias = jnp.where(seen_from <= rows, 0.0, MASKED)
            bias = jnp.concatenate([jnp.broadcast_to(history_bias, (count, h_keys)), bias], axis=1)
            bias = jnp.concatenate([bias] * per, axis=0)
            for g in range(0, local_heads, per):
                stacked = jnp.concatenate(
                    [q[pl.ds(row0, count), h * HEAD_DIM : (h + 1) * HEAD_DIM] for h in range(g, g + per)], axis=0
                )
                scores = lax.dot_general(
                    stacked, k_all[...], (((1,), (1,)), ((), ())), preferred_element_type=F32
                )
                scores = scores + bias
                top = jnp.max(scores, axis=-1, keepdims=True)
                weights = jnp.exp2((scores - top) * factor)
                total = jnp.sum(weights, axis=-1, keepdims=True)
                summed = jnp.dot(weights.astype(BF16), v_all[...], preferred_element_type=F32)
                summed = (summed / total).astype(BF16)
                for h in range(per):
                    att[i * count : (i + 1) * count, (g + h) * HEAD_DIM : (g + h + 1) * HEAD_DIM] = summed[
                        h * count : (h + 1) * count
                    ]
            if has_decode:

                @pl.when(target == devices - 1)
                def _():
                    att[(i + 1) * count - decode_rows : (i + 1) * count, :] = dec_ref[...]

        for c in range(0, model, COLUMNS):
            out = jnp.dot(att[...], w[:, c : c + COLUMNS], preferred_element_type=F32).astype(BF16)
            keep_ref[:, c : c + COLUMNS] = out[:half]
            give_ref[:, c : c + COLUMNS] = out[half:]

    flops = 2 * len(order) * count * (2 * local_width * keys + local_width * model)
    n_vmem = 2 + 2 * devices + has_decode
    return pl.pallas_call(
        body,
        in_specs=[smem()] + [in_vmem()] * n_vmem,
        out_specs=[in_vmem()] * 2,
        out_shape=[jax.ShapeDtypeStruct((half, model), BF16)] * 2,
        scratch_shapes=[
            pltpu.VMEM((keys, HEAD_DIM), BF16),
            pltpu.VMEM((keys, HEAD_DIM), BF16),
            pltpu.VMEM((2 * half, local_width), BF16),
        ],
        compiler_params=params(24),
        cost_estimate=pl.CostEstimate(flops=flops, transcendentals=0, bytes_accessed=weight.size * 2),
    )(meta, queries, *history, *fresh, *([decoded] if has_decode else []), weight)


def finish(first, residual, own, given, crossed, gain, previous):
    block, model = residual.shape
    count = crossed[0].shape[0]
    tile = 16
    n_cross = len(crossed)

    def body(res_ref, own_ref, given_ref, *refs):
        cross = refs[:n_cross]
        gain_ref = refs[n_cross]
        hidden_ref, normed_ref = refs[-2:]
        hidden = res_ref[...].astype(F32) + own_ref[...].astype(F32) + given_ref[...].astype(F32)
        for c in cross:
            hidden = hidden + c[...].astype(F32)
        mean = jnp.mean(hidden * hidden, axis=-1, keepdims=True)
        hidden_ref[...] = hidden.astype(BF16)
        normed_ref[...] = (hidden * lax.rsqrt(mean + EPS) * gain_ref[...]).astype(BF16)

    here = pl.BlockSpec((tile, model), lambda i: (first // tile + i, 0))
    local = pl.BlockSpec((tile, model), lambda i: (i, 0))
    n_in = 3 + n_cross + 1
    return pl.pallas_call(
        body,
        grid=(count // tile,),
        in_specs=[here, here, here]
        + [local] * n_cross
        + [pl.BlockSpec((1, model), lambda i: (0, 0))]
        + [hbm()] * len(previous),
        out_specs=[here, here],
        out_shape=[jax.ShapeDtypeStruct((block, model), BF16)] * 2,
        input_output_aliases={n_in + i: i for i in range(len(previous))},
        compiler_params=params(16),
    )(residual, own, given, *crossed, gain, *previous)


def step(
    prompt_queries,
    prompt_entries,
    history_cache,
    decode_queries,
    decode_entries,
    decode_cache,
    decode_lengths,
    prompt_start,
    out_weight,
    residual,
    norm_gain,
):
    devices = lax.axis_size("tp")
    local_heads = prompt_queries.shape[1] // HEAD_DIM
    kv_heads = history_cache.shape[2] // HEAD_DIM
    group = devices * local_heads // kv_heads
    block = residual.shape[0]
    h_rows, p_rows = history_cache.shape[1], prompt_entries.shape[1]
    assert group % local_heads == 0 and devices & (devices - 1) == 0
    assert block >= decode_queries.shape[0]
    meta = jnp.concatenate([lax.axis_index("tp").astype(jnp.int32)[None], prompt_start, decode_lengths])

    def swap(value, k):
        return lax.ppermute(value, "tp", [(i, i ^ k) for i in range(devices)])

    def swapped(values):
        return [values[0]] + [swap(values[k], k) for k in range(1, devices)]

    history = swapped(pack_history(history_cache, decode_queries, meta, devices, local_heads, group))
    fresh = swapped(pack_fresh(prompt_entries, meta, devices, local_heads, group))
    cache, queries = stage(decode_cache, prompt_queries, decode_queries)
    parts = swapped(decode_partials(history, cache, meta, h_rows, local_heads, group))
    decoded = decode_join(parts, history[0], decode_entries, meta, h_rows, local_heads, group)

    def attended(slots, first, count, decoded):
        return attend(slots, first, count, block, queries, history, fresh, decoded, out_weight, meta, h_rows, p_rows)

    chunks = [c * block // sum(CHUNKS) for c in CHUNKS]
    if any(c % 16 for c in chunks):
        chunks = [block]
    crossed, first = [], 0
    for count in chunks:
        keep, give = attended(list(range(2, devices)), first, count, decoded if first + count == block else None)
        taken = swap(give, 1)
        pair = (keep.astype(F32) + taken.astype(F32)).astype(BF16)
        crossed.append((first, [swap(pair[(k // 2 - 1) * count : k // 2 * count], k) for k in range(2, devices, 2)]))
        first += count
    own, give = attended([0, 1], 0, block, decoded)
    given = swap(give, 1)
    gain = norm_gain[None, :]
    outs = []
    for first, pieces in crossed:
        outs = finish(first, residual, own, given, pieces, gain, outs)
    return tuple(outs)


def solution(mesh):
    placed = (
        P("rep", "tp"),
        P("rep", "tp", None),
        P("rep", "tp", None),
        P("rep", "tp"),
        P("rep", None, None),
        P("rep", None, "tp", None),
        P("rep"),
        P("rep"),
        P("tp", None),
        P("tp", "rep"),
        P(),
    )
    return jax.shard_map(
        step,
        mesh=mesh,
        in_specs=placed,
        out_specs=(P("tp", "rep"), P("tp", "rep")),
        check_vma=False,
    )
```

```python
import jax
import jax.numpy as jnp
import numpy as np
from jax import lax
from jax.experimental import pallas as pl
from jax.experimental.pallas import tpu as pltpu
from jax.sharding import PartitionSpec as P


HEAD_DIM = 128
MASKED = -1e30
EPS = 1e-05
CHUNKS = (64, 64)
COLUMNS = 512
GROUP_ROWS = 256

F32 = jnp.float32
BF16 = jnp.bfloat16


def round_up(value, unit):
    return -(-value // unit) * unit


def smem():
    return pl.BlockSpec(memory_space=pltpu.SMEM)


def hbm():
    return pl.BlockSpec(memory_space=pl.ANY)


def in_hbm():
    return pl.BlockSpec(memory_space=pltpu.HBM)


def in_vmem():
    return pl.BlockSpec(memory_space=pltpu.VMEM)


def to_hbm(value):
    return pltpu.with_memory_space_constraint(value, pltpu.HBM)


def busy(us):
    return pl.CostEstimate(flops=us * 500_000_000, transcendentals=0, bytes_accessed=us * 1_000_000)


def params(mib, **kwargs):
    return pltpu.CompilerParams(vmem_limit_bytes=mib << 20, **kwargs)


def pack_history(history, queries, devices, local_heads, group):
    h_rows = history.shape[1]
    rows = queries.shape[0]

    def body(h_hbm, q_hbm, *refs):
        o_refs, q_ref, sem = refs[:devices], refs[devices], refs[devices + 1]
        me = lax.axis_index("tp")
        copies = []
        for k in range(devices):
            lane = pl.multiple_of((me ^ k) * local_heads // group * HEAD_DIM, HEAD_DIM)
            for part in range(2):
                copies.append(
                    pltpu.make_async_copy(
                        h_hbm.at[part, :, pl.ds(lane, HEAD_DIM)],
                        o_refs[k].at[part * h_rows : (part + 1) * h_rows, :],
                        sem.at[len(copies)],
                    )
                )
        for h in range(local_heads):
            copies.append(
                pltpu.make_async_copy(
                    q_hbm.at[:, h * HEAD_DIM : (h + 1) * HEAD_DIM],
                    q_ref.at[h * rows : (h + 1) * rows, :],
                    sem.at[len(copies)],
                )
            )
        for copy in copies:
            copy.start()
        for copy in copies:
            copy.wait()

    outs = pl.pallas_call(
        body,
        in_specs=[in_hbm()] * 2,
        out_specs=[in_vmem()] * (devices + 1),
        out_shape=[jax.ShapeDtypeStruct((2 * h_rows, HEAD_DIM), BF16)] * devices
        + [jax.ShapeDtypeStruct((rows * local_heads, HEAD_DIM), BF16)],
        scratch_shapes=[pltpu.SemaphoreType.DMA((2 * devices + local_heads,))],
        compiler_params=params(2),
        cost_estimate=busy(6),
        name="pack_history",
    )(to_hbm(history), to_hbm(queries))
    return outs[:devices], outs[devices]


def pack_fresh(prompt, meta, devices, local_heads, group):
    p_rows = prompt.shape[1]
    p_pad = round_up(p_rows, 16)

    def head_of(k):
        return lambda i, m: (0, 0, (m[0] ^ k) * local_heads // group)

    def body(m, *refs):
        for k in range(devices):
            p_ref, o_ref = refs[k], refs[devices + k]
            for part in range(2):
                if p_pad > p_rows:
                    fresh = jnp.concatenate(
                        [p_ref[part].astype(F32), jnp.zeros((p_pad - p_rows, HEAD_DIM), F32)], axis=0
                    ).astype(BF16)
                else:
                    fresh = p_ref[part]
                o_ref[part * p_pad : (part + 1) * p_pad, :] = fresh

    return pl.pallas_call(
        body,
        grid_spec=pltpu.PrefetchScalarGridSpec(
            num_scalar_prefetch=1,
            grid=(1,),
            in_specs=[pl.BlockSpec((2, p_rows, HEAD_DIM), head_of(k)) for k in range(devices)],
            out_specs=[pl.BlockSpec((2 * p_pad, HEAD_DIM), lambda i, m: (0, 0))] * devices,
        ),
        out_shape=[jax.ShapeDtypeStruct((2 * p_pad, HEAD_DIM), BF16)] * devices,
        compiler_params=params(8),
        cost_estimate=busy(6),
        name="pack_fresh",
    )(meta, *([prompt] * devices))


def stage(prompt_queries, decode_queries, entries, local_heads, group):
    prompt_rows, decode_rows = prompt_queries.shape[0], decode_queries.shape[0]

    def body(q_hbm, dq_hbm, e_hbm, q_ref, e_ref, sem):
        lane = pl.multiple_of(lax.axis_index("tp") * local_heads // group * HEAD_DIM, HEAD_DIM)
        copies = [
            pltpu.make_async_copy(q_hbm, q_ref.at[0:prompt_rows, :], sem.at[0]),
            pltpu.make_async_copy(dq_hbm, q_ref.at[prompt_rows : prompt_rows + decode_rows, :], sem.at[1]),
            pltpu.make_async_copy(e_hbm.at[:, :, pl.ds(lane, HEAD_DIM)], e_ref, sem.at[2]),
        ]
        for copy in copies:
            copy.start()
        for copy in copies:
            copy.wait()

    return pl.pallas_call(
        body,
        in_specs=[in_hbm()] * 3,
        out_specs=[in_vmem()] * 2,
        out_shape=[
            pltpu.VMEM((prompt_rows + decode_rows, prompt_queries.shape[1]), BF16),
            pltpu.VMEM((2, decode_rows, HEAD_DIM), BF16),
        ],
        scratch_shapes=[pltpu.SemaphoreType.DMA((3,))],
        compiler_params=params(2),
        cost_estimate=busy(6),
        name="stage",
    )(to_hbm(prompt_queries), to_hbm(decode_queries), to_hbm(entries))


def split(value):
    terms = []
    for _ in range(3):
        terms.append(value.astype(BF16))
        value = value - terms[-1].astype(F32)
    return terms


def decode_partials(queries, cache, meta, local_heads, group):
    devices = len(queries)
    rows, span, width = cache.shape[1], cache.shape[2], cache.shape[3]
    kv_heads = width // HEAD_DIM
    heads = devices * local_heads
    factor = HEAD_DIM ** (-0.5) * float(np.log2(np.e))
    part_rows = rows * local_heads
    stat_rows = round_up(local_heads, 8)

    def body(m, *refs):
        q_refs, cache_ref = refs[:devices], refs[devices]
        o_refs = refs[devices + 1 : 2 * devices + 1]
        q_all, sums = refs[2 * devices + 1 :]
        me = m[0]
        for k in range(devices):
            for h in range(local_heads):
                q_all[k, pl.ds(h, rows, stride=local_heads), :] = q_refs[k][h * rows : (h + 1) * rows, :].astype(F32)

        slot = lax.broadcasted_iota(jnp.int32, (heads, 1), 0) // local_heads
        reads = ((slot ^ me) * local_heads) // group
        lane = lax.broadcasted_iota(jnp.int32, (heads, HEAD_DIM), 1)
        place = me * span + lax.broadcasted_iota(jnp.int32, (1, span), 1)
        scores = []
        for b in range(rows):
            here = slice(b * local_heads, (b + 1) * local_heads)
            q = jnp.concatenate([q_all[k, here, :] for k in range(devices)], axis=0)
            spread = jnp.concatenate(
                [jnp.where(reads == g, q, 0.0) for g in range(kv_heads)], axis=1
            ).astype(BF16)
            score = lax.dot_general(
                spread, cache_ref[0, b], (((1,), (1,)), ((), ())), preferred_element_type=F32
            )
            scores.append(jnp.where(place < m[2 + b], score, MASKED))
        scores = jnp.concatenate(scores, axis=0)
        top = jnp.max(scores, axis=-1, keepdims=True)
        weights = jnp.where(scores > 0.5 * MASKED, jnp.exp2((scores - top) * factor), 0.0)
        total = jnp.sum(weights, axis=-1, keepdims=True)
        weights = weights.astype(BF16)
        stats = jnp.zeros((heads, HEAD_DIM), F32)
        for b in range(rows):
            these = slice(b * heads, (b + 1) * heads)
            summed = jnp.dot(weights[these], cache_ref[1, b], preferred_element_type=F32)
            own = jnp.zeros((heads, HEAD_DIM), F32)
            for g in range(kv_heads):
                own = own + jnp.where(reads == g, summed[:, g * HEAD_DIM : (g + 1) * HEAD_DIM], 0.0)
            for k in range(devices):
                sums[k, b * local_heads : (b + 1) * local_heads, :] = own[k * local_heads : (k + 1) * local_heads]
            stats = jnp.where(lane == b, top[these], jnp.where(lane == rows + b, total[these], stats))
        terms = split(stats)
        for k in range(devices):
            o_refs[k][0:part_rows, :] = sums[k].astype(BF16)
            for i, term in enumerate(terms):
                row = part_rows + i * stat_rows
                o_refs[k][row : row + local_heads, :] = term[k * local_heads : (k + 1) * local_heads, :]

    return pl.pallas_call(
        body,
        in_specs=[smem()] + [in_vmem()] * (devices + 1),
        out_specs=[in_vmem()] * devices,
        scratch_shapes=[pltpu.VMEM((devices, part_rows, HEAD_DIM), F32)] * 2,
        out_shape=[jax.ShapeDtypeStruct((part_rows + 3 * stat_rows, HEAD_DIM), BF16)] * devices,
        compiler_params=params(12),
        cost_estimate=busy(6),
        name="decode",
    )(meta, *queries, cache)


def decode_join(parts, queries, entries, local_heads):
    devices = len(parts)
    rows = entries.shape[1]
    factor = HEAD_DIM ** (-0.5) * float(np.log2(np.e))
    part_rows = rows * local_heads
    stat_rows = round_up(local_heads, 8)

    def body(*refs):
        p_refs = refs[:devices]
        q_ref, e_ref, o_ref, q_all, out = refs[devices:]
        for h in range(local_heads):
            q_all[pl.ds(h, rows, stride=local_heads), :] = q_ref[h * rows : (h + 1) * rows, :].astype(F32)
        stats = []
        for p in p_refs:
            starts = [part_rows + i * stat_rows for i in range(3)]
            high, middle, low = [p[row : row + local_heads, :].astype(F32) for row in starts]
            stats.append(high + middle + low)
        keys, values = e_ref[0].astype(F32), e_ref[1].astype(F32)
        sums = [p[0:part_rows, :].astype(F32) for p in p_refs]
        for b in range(rows):
            here = slice(b * local_heads, (b + 1) * local_heads)
            own = jnp.sum(q_all[here, :] * keys[b : b + 1, :], axis=-1, keepdims=True)
            tops = [s[:, b : b + 1] for s in stats]
            top = own
            for t in tops:
                top = jnp.maximum(top, t)
            weight = jnp.exp2((own - top) * factor)
            total = weight
            summed = weight.astype(BF16).astype(F32) * values[b : b + 1, :]
            for s, t, p in zip(stats, tops, sums):
                share = jnp.exp2((t - top) * factor)
                total = total + share * s[:, rows + b : rows + b + 1]
                summed = summed + share * p[here, :]
            out[here, :] = summed / total
        for h in range(local_heads):
            o_ref[:, h * HEAD_DIM : (h + 1) * HEAD_DIM] = out[pl.ds(h, rows, stride=local_heads), :].astype(BF16)

    return pl.pallas_call(
        body,
        in_specs=[in_vmem()] * (devices + 2),
        out_specs=in_vmem(),
        scratch_shapes=[pltpu.VMEM((part_rows, HEAD_DIM), F32)] * 2,
        out_shape=jax.ShapeDtypeStruct((rows, local_heads * HEAD_DIM), BF16),
        compiler_params=params(4),
        cost_estimate=busy(1),
        name="join",
    )(*parts, queries, entries)


def attend(slots, first, count, block, queries, history, fresh, decoded, weight, meta, h_rows, p_rows):
    devices = len(history)
    p_pad = fresh[0].shape[0] // 2
    local_width = queries.shape[1]
    local_heads = local_width // HEAD_DIM
    model = weight.shape[1]
    h_keys, p_keys = devices * h_rows, devices * p_pad
    keys = h_keys + p_keys
    order = [s for s in slots if s % 2 == 0] + [s for s in slots if s % 2 == 1]
    half = len(order) // 2 * count
    factor = HEAD_DIM ** (-0.5) * float(np.log2(np.e))
    per = max(1, min(local_heads, GROUP_ROWS // count))
    has_decode = decoded is not None
    decode_rows = decoded.shape[0] if has_decode else 0

    def body(m, q, *refs):
        h_refs, f_refs = refs[:devices], refs[devices : 2 * devices]
        rest = refs[2 * devices :]
        if has_decode:
            dec_ref, rest = rest[0], rest[1:]
        w, keep_ref, give_ref, k_all, v_all, att = rest
        me, valid_rows = m[0], m[1]
        for k in range(devices):
            for part, dst in ((0, k_all), (1, v_all)):
                dst[k * h_rows : (k + 1) * h_rows, :] = h_refs[k][part * h_rows : (part + 1) * h_rows, :]
                dst[h_keys + k * p_pad : h_keys + (k + 1) * p_pad, :] = f_refs[k][
                    part * p_pad : (part + 1) * p_pad, :
                ]
        column = lax.broadcasted_iota(jnp.int32, (1, h_keys), 1)
        place = ((column // h_rows) ^ me) * h_rows + column % h_rows
        history_bias = jnp.where(place < valid_rows, 0.0, MASKED)
        column = lax.broadcasted_iota(jnp.int32, (1, p_keys), 1)
        inner = column % p_pad
        seen_from = jnp.where(inner < p_rows, ((column // p_pad) ^ me) * p_rows + inner, 1 << 20)
        for i, slot in enumerate(order):
            target = slot ^ me
            row0 = pl.multiple_of(target * block + first, 16)
            rows = row0 + lax.broadcasted_iota(jnp.int32, (count, 1), 0)
            bias = jnp.where(seen_from <= rows, 0.0, MASKED)
            bias = jnp.concatenate([jnp.broadcast_to(history_bias, (count, h_keys)), bias], axis=1)
            bias = jnp.concatenate([bias] * per, axis=0)
            for g in range(0, local_heads, per):
                stacked = jnp.concatenate(
                    [q[pl.ds(row0, count), h * HEAD_DIM : (h + 1) * HEAD_DIM] for h in range(g, g + per)], axis=0
                )
                scores = lax.dot_general(
                    stacked, k_all[...], (((1,), (1,)), ((), ())), preferred_element_type=F32
                )
                scores = scores + bias
                top = jnp.max(scores, axis=-1, keepdims=True)
                weights = jnp.exp2((scores - top) * factor)
                total = jnp.sum(weights, axis=-1, keepdims=True)
                summed = jnp.dot(weights.astype(BF16), v_all[...], preferred_element_type=F32)
                summed = (summed / total).astype(BF16)
                for h in range(per):
                    att[i * count : (i + 1) * count, (g + h) * HEAD_DIM : (g + h + 1) * HEAD_DIM] = summed[
                        h * count : (h + 1) * count
                    ]
            if has_decode:

                @pl.when(target == devices - 1)
                def _():
                    att[(i + 1) * count - decode_rows : (i + 1) * count, :] = dec_ref[...]

        for c in range(0, model, COLUMNS):
            out = jnp.dot(att[...], w[:, c : c + COLUMNS], preferred_element_type=F32).astype(BF16)
            keep_ref[:, c : c + COLUMNS] = out[:half]
            give_ref[:, c : c + COLUMNS] = out[half:]

    flops = 2 * len(order) * count * (2 * local_width * keys + local_width * model)
    n_vmem = 2 + 2 * devices + has_decode
    return pl.pallas_call(
        body,
        in_specs=[smem()] + [in_vmem()] * n_vmem,
        out_specs=[in_vmem()] * 2,
        out_shape=[jax.ShapeDtypeStruct((half, model), BF16)] * 2,
        scratch_shapes=[
            pltpu.VMEM((keys, HEAD_DIM), BF16),
            pltpu.VMEM((keys, HEAD_DIM), BF16),
            pltpu.VMEM((2 * half, local_width), BF16),
        ],
        compiler_params=params(24),
        cost_estimate=pl.CostEstimate(flops=flops, transcendentals=0, bytes_accessed=weight.size * 2),
    )(meta, queries, *history, *fresh, *([decoded] if has_decode else []), weight)


def finish(first, residual, own, given, crossed, gain, previous):
    block, model = residual.shape
    count = crossed[0].shape[0]
    tile = 16
    n_cross = len(crossed)

    def body(res_ref, own_ref, given_ref, *refs):
        cross = refs[:n_cross]
        gain_ref = refs[n_cross]
        outs = refs[-5:-3]
        staged, sem = refs[-3:-1], refs[-1]
        copies = []
        for i in range(0, count, tile):
            here, local = slice(first + i, first + i + tile), slice(i, i + tile)
            hidden = res_ref[here, :].astype(F32) + own_ref[here, :].astype(F32) + given_ref[here, :].astype(F32)
            for c in cross:
                hidden = hidden + c[local, :].astype(F32)
            mean = jnp.mean(hidden * hidden, axis=-1, keepdims=True)
            staged[0][local, :] = hidden.astype(BF16)
            staged[1][local, :] = (hidden * lax.rsqrt(mean + EPS) * gain_ref[...]).astype(BF16)
            for source, target in zip(staged, outs):
                copies.append(pltpu.make_async_copy(source.at[local, :], target.at[here, :], sem.at[len(copies)]))
                copies[-1].start()
        for copy in copies:
            copy.wait()

    n_in = 3 + n_cross + 1
    return pl.pallas_call(
        body,
        in_specs=[in_vmem()] * n_in + [hbm()] * len(previous),
        out_specs=[hbm()] * 2,
        out_shape=[jax.ShapeDtypeStruct((block, model), BF16)] * 2,
        input_output_aliases={n_in + i: i for i in range(len(previous))},
        scratch_shapes=[pltpu.VMEM((count, model), BF16)] * 2 + [pltpu.SemaphoreType.DMA((2 * count // tile,))],
        compiler_params=params(8),
        cost_estimate=busy(2),
    )(residual, own, given, *crossed, gain, *previous)


def step(
    prompt_queries,
    prompt_entries,
    history_cache,
    decode_queries,
    decode_entries,
    decode_cache,
    decode_lengths,
    prompt_start,
    out_weight,
    residual,
    norm_gain,
):
    devices = lax.axis_size("tp")
    local_heads = prompt_queries.shape[1] // HEAD_DIM
    kv_heads = history_cache.shape[2] // HEAD_DIM
    group = devices * local_heads // kv_heads
    block = residual.shape[0]
    h_rows, p_rows = history_cache.shape[1], prompt_entries.shape[1]
    assert group % local_heads == 0 and devices & (devices - 1) == 0
    assert block >= decode_queries.shape[0]

    def swap(value, k):
        return lax.ppermute(value, "tp", [(i, i ^ k) for i in range(devices)])

    def swapped(values):
        return [values[0]] + [swap(values[k], k) for k in range(1, devices)]

    packed, own_query = pack_history(history_cache, decode_queries, devices, local_heads, group)
    decode_rows = {0: own_query}
    for k in range(2, devices, 2):
        decode_rows[k] = swap(own_query, k)
    for k in range(1, devices, 2):
        decode_rows[k] = swap(decode_rows[k ^ 1], 1)
    history = swapped(packed)
    meta = jnp.concatenate([lax.axis_index("tp").astype(jnp.int32)[None], prompt_start, decode_lengths])
    fresh = swapped(pack_fresh(prompt_entries, meta, devices, local_heads, group))
    queries, entries = stage(prompt_queries, decode_queries, decode_entries, local_heads, group)
    ordered = [decode_rows[k] for k in range(devices)]
    parts = swapped(decode_partials(ordered, decode_cache, meta, local_heads, group))
    decoded = decode_join(parts, own_query, entries, local_heads)

    def attended(slots, first, count, decoded):
        return attend(slots, first, count, block, queries, history, fresh, decoded, out_weight, meta, h_rows, p_rows)

    chunks = [c * block // sum(CHUNKS) for c in CHUNKS]
    if any(c % 16 for c in chunks):
        chunks = [block]
    crossed, first = [], 0
    for count in chunks:
        keep, give = attended(list(range(2, devices)), first, count, decoded if first + count == block else None)
        taken = swap(give, 1)
        pair = (keep.astype(F32) + taken.astype(F32)).astype(BF16)
        crossed.append((first, [swap(pair[(k // 2 - 1) * count : k // 2 * count], k) for k in range(2, devices, 2)]))
        first += count
    own, give = attended([0, 1], 0, block, decoded)
    given = swap(give, 1)
    gain = norm_gain[None, :]
    outs = []
    for first, pieces in crossed:
        outs = finish(first, residual, own, given, pieces, gain, outs)
    return tuple(outs)


def solution(mesh):
    placed = (
        P("rep", "tp"),
        P("rep", "tp", None),
        P("rep", "tp", None),
        P("rep", "tp"),
        P("rep", None, None),
        P("rep", None, "tp", None),
        P("rep"),
        P("rep"),
        P("tp", None),
        P("tp", "rep"),
        P(),
    )
    return jax.shard_map(
        step,
        mesh=mesh,
        in_specs=placed,
        out_specs=(P("tp", "rep"), P("tp", "rep")),
        check_vma=False,
    )
```

```python
import jax
import jax.numpy as jnp
import numpy as np
from jax import lax
from jax.experimental import pallas as pl
from jax.experimental.pallas import tpu as pltpu
from jax.sharding import PartitionSpec as P


HEAD_DIM = 128
MASKED = -1e30
EPS = 1e-05
CHUNKS = (64, 64)
COLUMNS = 512
GROUP_ROWS = 256

F32 = jnp.float32
BF16 = jnp.bfloat16


def round_up(value, unit):
    return -(-value // unit) * unit


def smem():
    return pl.BlockSpec(memory_space=pltpu.SMEM)


def hbm():
    return pl.BlockSpec(memory_space=pl.ANY)


def in_hbm():
    return pl.BlockSpec(memory_space=pltpu.HBM)


def in_vmem():
    return pl.BlockSpec(memory_space=pltpu.VMEM)


def to_hbm(value):
    return pltpu.with_memory_space_constraint(value, pltpu.HBM)


def busy(us):
    return pl.CostEstimate(flops=us * 500_000_000, transcendentals=0, bytes_accessed=us * 1_000_000)


def params(mib, **kwargs):
    return pltpu.CompilerParams(vmem_limit_bytes=mib << 20, **kwargs)


def pack_history(history, queries, devices, local_heads, group):
    h_rows = history.shape[1]
    rows = queries.shape[0]

    def body(h_hbm, q_hbm, *refs):
        o_refs, q_ref, sem = refs[:devices], refs[devices], refs[devices + 1]
        me = lax.axis_index("tp")
        copies = []
        for k in range(devices):
            lane = pl.multiple_of((me ^ k) * local_heads // group * HEAD_DIM, HEAD_DIM)
            for part in range(2):
                copies.append(
                    pltpu.make_async_copy(
                        h_hbm.at[part, :, pl.ds(lane, HEAD_DIM)],
                        o_refs[k].at[part * h_rows : (part + 1) * h_rows, :],
                        sem.at[len(copies)],
                    )
                )
        for h in range(local_heads):
            copies.append(
                pltpu.make_async_copy(
                    q_hbm.at[:, h * HEAD_DIM : (h + 1) * HEAD_DIM],
                    q_ref.at[h * rows : (h + 1) * rows, :],
                    sem.at[len(copies)],
                )
            )
        for copy in copies:
            copy.start()
        for copy in copies:
            copy.wait()

    outs = pl.pallas_call(
        body,
        in_specs=[in_hbm()] * 2,
        out_specs=[in_vmem()] * (devices + 1),
        out_shape=[jax.ShapeDtypeStruct((2 * h_rows, HEAD_DIM), BF16)] * devices
        + [jax.ShapeDtypeStruct((rows * local_heads, HEAD_DIM), BF16)],
        scratch_shapes=[pltpu.SemaphoreType.DMA((2 * devices + local_heads,))],
        compiler_params=params(2),
        cost_estimate=busy(6),
        name="pack_history",
    )(to_hbm(history), to_hbm(queries))
    return outs[:devices], outs[devices]


def pack_fresh(prompt, meta, devices, local_heads, group):
    p_rows = prompt.shape[1]
    p_pad = round_up(p_rows, 16)

    def head_of(k):
        return lambda i, m: (0, 0, (m[0] ^ k) * local_heads // group)

    def body(m, *refs):
        for k in range(devices):
            p_ref, o_ref = refs[k], refs[devices + k]
            for part in range(2):
                if p_pad > p_rows:
                    fresh = jnp.concatenate(
                        [p_ref[part].astype(F32), jnp.zeros((p_pad - p_rows, HEAD_DIM), F32)], axis=0
                    ).astype(BF16)
                else:
                    fresh = p_ref[part]
                o_ref[part * p_pad : (part + 1) * p_pad, :] = fresh

    return pl.pallas_call(
        body,
        grid_spec=pltpu.PrefetchScalarGridSpec(
            num_scalar_prefetch=1,
            grid=(1,),
            in_specs=[pl.BlockSpec((2, p_rows, HEAD_DIM), head_of(k)) for k in range(devices)],
            out_specs=[pl.BlockSpec((2 * p_pad, HEAD_DIM), lambda i, m: (0, 0))] * devices,
        ),
        out_shape=[jax.ShapeDtypeStruct((2 * p_pad, HEAD_DIM), BF16)] * devices,
        compiler_params=params(8),
        cost_estimate=busy(12),
        name="pack_fresh",
    )(meta, *([prompt] * devices))


def split(value):
    terms = []
    for _ in range(3):
        terms.append(value.astype(BF16))
        value = value - terms[-1].astype(F32)
    return terms


def decode_partials(queries, cache, prompt_queries, decode_queries, entries, meta, local_heads, group):
    devices = len(queries)
    rows, span, width = cache.shape[1], cache.shape[2], cache.shape[3]
    kv_heads = width // HEAD_DIM
    heads = devices * local_heads
    factor = HEAD_DIM ** (-0.5) * float(np.log2(np.e))
    part_rows = rows * local_heads
    stat_rows = round_up(local_heads, 8)
    prompt_rows = prompt_queries.shape[0]

    def body(m, *refs):
        q_refs, refs = refs[:devices], refs[devices:]
        cache_ref, pq_hbm, dq_hbm, e_hbm = refs[:4]
        o_refs, refs = refs[4 : 4 + devices], refs[4 + devices :]
        q_ref, e_ref, q_all, sums, sem = refs
        me = m[0]
        lane = pl.multiple_of(me * local_heads // group * HEAD_DIM, HEAD_DIM)
        copies = [
            pltpu.make_async_copy(pq_hbm, q_ref.at[0:prompt_rows, :], sem.at[0]),
            pltpu.make_async_copy(dq_hbm, q_ref.at[prompt_rows : prompt_rows + rows, :], sem.at[1]),
            pltpu.make_async_copy(e_hbm.at[:, :, pl.ds(lane, HEAD_DIM)], e_ref, sem.at[2]),
        ]
        for copy in copies:
            copy.start()
        for k in range(devices):
            for h in range(local_heads):
                q_all[k, pl.ds(h, rows, stride=local_heads), :] = q_refs[k][h * rows : (h + 1) * rows, :].astype(F32)

        slot = lax.broadcasted_iota(jnp.int32, (heads, 1), 0) // local_heads
        reads = ((slot ^ me) * local_heads) // group
        lane = lax.broadcasted_iota(jnp.int32, (heads, HEAD_DIM), 1)
        place = me * span + lax.broadcasted_iota(jnp.int32, (1, span), 1)
        scores = []
        for b in range(rows):
            here = slice(b * local_heads, (b + 1) * local_heads)
            q = jnp.concatenate([q_all[k, here, :] for k in range(devices)], axis=0)
            spread = jnp.concatenate(
                [jnp.where(reads == g, q, 0.0) for g in range(kv_heads)], axis=1
            ).astype(BF16)
            score = lax.dot_general(
                spread, cache_ref[0, b], (((1,), (1,)), ((), ())), preferred_element_type=F32
            )
            scores.append(jnp.where(place < m[2 + b], score, MASKED))
        scores = jnp.concatenate(scores, axis=0)
        top = jnp.max(scores, axis=-1, keepdims=True)
        weights = jnp.where(scores > 0.5 * MASKED, jnp.exp2((scores - top) * factor), 0.0)
        total = jnp.sum(weights, axis=-1, keepdims=True)
        weights = weights.astype(BF16)
        stats = jnp.zeros((heads, HEAD_DIM), F32)
        for b in range(rows):
            these = slice(b * heads, (b + 1) * heads)
            summed = jnp.dot(weights[these], cache_ref[1, b], preferred_element_type=F32)
            own = jnp.zeros((heads, HEAD_DIM), F32)
            for g in range(kv_heads):
                own = own + jnp.where(reads == g, summed[:, g * HEAD_DIM : (g + 1) * HEAD_DIM], 0.0)
            for k in range(devices):
                sums[k, b * local_heads : (b + 1) * local_heads, :] = own[k * local_heads : (k + 1) * local_heads]
            stats = jnp.where(lane == b, top[these], jnp.where(lane == rows + b, total[these], stats))
        terms = split(stats)
        for k in range(devices):
            o_refs[k][0:part_rows, :] = sums[k].astype(BF16)
            for i, term in enumerate(terms):
                row = part_rows + i * stat_rows
                o_refs[k][row : row + local_heads, :] = term[k * local_heads : (k + 1) * local_heads, :]
        for copy in copies:
            copy.wait()

    outs = pl.pallas_call(
        body,
        in_specs=[smem()] + [in_vmem()] * (devices + 1) + [in_hbm()] * 3,
        out_specs=[in_vmem()] * (devices + 2),
        scratch_shapes=[pltpu.VMEM((devices, part_rows, HEAD_DIM), F32)] * 2 + [pltpu.SemaphoreType.DMA((3,))],
        out_shape=[jax.ShapeDtypeStruct((part_rows + 3 * stat_rows, HEAD_DIM), BF16)] * devices
        + [
            pltpu.VMEM((prompt_rows + rows, prompt_queries.shape[1]), BF16),
            pltpu.VMEM((2, rows, HEAD_DIM), BF16),
        ],
        compiler_params=params(12),
        cost_estimate=busy(12),
        name="decode",
    )(meta, *queries, cache, to_hbm(prompt_queries), to_hbm(decode_queries), to_hbm(entries))
    return outs[:devices], outs[devices], outs[devices + 1]


def decode_join(parts, queries, entries, local_heads):
    devices = len(parts)
    rows = entries.shape[1]
    factor = HEAD_DIM ** (-0.5) * float(np.log2(np.e))
    part_rows = rows * local_heads
    stat_rows = round_up(local_heads, 8)

    def body(*refs):
        p_refs = refs[:devices]
        q_ref, e_ref, o_ref, q_all, out = refs[devices:]
        for h in range(local_heads):
            q_all[pl.ds(h, rows, stride=local_heads), :] = q_ref[h * rows : (h + 1) * rows, :].astype(F32)
        stats = []
        for p in p_refs:
            starts = [part_rows + i * stat_rows for i in range(3)]
            high, middle, low = [p[row : row + local_heads, :].astype(F32) for row in starts]
            stats.append(high + middle + low)
        keys, values = e_ref[0].astype(F32), e_ref[1].astype(F32)
        sums = [p[0:part_rows, :].astype(F32) for p in p_refs]
        for b in range(rows):
            here = slice(b * local_heads, (b + 1) * local_heads)
            own = jnp.sum(q_all[here, :] * keys[b : b + 1, :], axis=-1, keepdims=True)
            tops = [s[:, b : b + 1] for s in stats]
            top = own
            for t in tops:
                top = jnp.maximum(top, t)
            weight = jnp.exp2((own - top) * factor)
            total = weight
            summed = weight.astype(BF16).astype(F32) * values[b : b + 1, :]
            for s, t, p in zip(stats, tops, sums):
                share = jnp.exp2((t - top) * factor)
                total = total + share * s[:, rows + b : rows + b + 1]
                summed = summed + share * p[here, :]
            out[here, :] = summed / total
        for h in range(local_heads):
            o_ref[:, h * HEAD_DIM : (h + 1) * HEAD_DIM] = out[pl.ds(h, rows, stride=local_heads), :].astype(BF16)

    return pl.pallas_call(
        body,
        in_specs=[in_vmem()] * (devices + 2),
        out_specs=in_vmem(),
        scratch_shapes=[pltpu.VMEM((part_rows, HEAD_DIM), F32)] * 2,
        out_shape=jax.ShapeDtypeStruct((rows, local_heads * HEAD_DIM), BF16),
        compiler_params=params(4),
        cost_estimate=busy(1),
        name="join",
    )(*parts, queries, entries)


def product(att, w, start, stop, half, keep_ref, give_ref):
    for c in range(start, stop, COLUMNS):
        out = jnp.dot(att[...], w[:, c : c + COLUMNS], preferred_element_type=F32).astype(BF16)
        keep_ref[:, c - start : c - start + COLUMNS] = out[:half]
        give_ref[:, c - start : c - start + COLUMNS] = out[half:]


def project(att, weight, start):
    rows, model = att.shape[0], weight.shape[1]

    def body(att_ref, w, keep_ref, give_ref):
        product(att_ref, w, start, model, rows // 2, keep_ref, give_ref)

    return pl.pallas_call(
        body,
        in_specs=[in_vmem()] * 2,
        out_specs=[in_vmem()] * 2,
        out_shape=[jax.ShapeDtypeStruct((rows // 2, model - start), BF16)] * 2,
        compiler_params=params(8),
        cost_estimate=busy(2),
        name="project",
    )(att, weight)


def attend(slots, first, count, block, queries, history, fresh, decoded, weight, meta, h_rows, p_rows, columns):
    devices = len(history)
    p_pad = fresh[0].shape[0] // 2
    local_width = queries.shape[1]
    local_heads = local_width // HEAD_DIM
    model = weight.shape[1]
    h_keys, p_keys = devices * h_rows, devices * p_pad
    keys = h_keys + p_keys
    order = [s for s in slots if s % 2 == 0] + [s for s in slots if s % 2 == 1]
    half = len(order) // 2 * count
    factor = HEAD_DIM ** (-0.5) * float(np.log2(np.e))
    per = max(1, min(local_heads, GROUP_ROWS // count))
    has_decode = decoded is not None
    decode_rows = decoded.shape[0] if has_decode else 0

    def body(m, q, *refs):
        h_refs, f_refs = refs[:devices], refs[devices : 2 * devices]
        rest = refs[2 * devices :]
        if has_decode:
            dec_ref, rest = rest[0], rest[1:]
        w, keep_ref, give_ref, att, k_all, v_all = rest
        me, valid_rows = m[0], m[1]
        for k in range(devices):
            for part, dst in ((0, k_all), (1, v_all)):
                dst[k * h_rows : (k + 1) * h_rows, :] = h_refs[k][part * h_rows : (part + 1) * h_rows, :]
                dst[h_keys + k * p_pad : h_keys + (k + 1) * p_pad, :] = f_refs[k][
                    part * p_pad : (part + 1) * p_pad, :
                ]
        column = lax.broadcasted_iota(jnp.int32, (1, h_keys), 1)
        place = ((column // h_rows) ^ me) * h_rows + column % h_rows
        history_bias = jnp.where(place < valid_rows, 0.0, MASKED)
        column = lax.broadcasted_iota(jnp.int32, (1, p_keys), 1)
        inner = column % p_pad
        seen_from = jnp.where(inner < p_rows, ((column // p_pad) ^ me) * p_rows + inner, 1 << 20)
        for i, slot in enumerate(order):
            target = slot ^ me
            row0 = pl.multiple_of(target * block + first, 16)
            rows = row0 + lax.broadcasted_iota(jnp.int32, (count, 1), 0)
            bias = jnp.where(seen_from <= rows, 0.0, MASKED)
            bias = jnp.concatenate([jnp.broadcast_to(history_bias, (count, h_keys)), bias], axis=1)
            bias = jnp.concatenate([bias] * per, axis=0)
            for g in range(0, local_heads, per):
                stacked = jnp.concatenate(
                    [q[pl.ds(row0, count), h * HEAD_DIM : (h + 1) * HEAD_DIM] for h in range(g, g + per)], axis=0
                )
                scores = lax.dot_general(
                    stacked, k_all[...], (((1,), (1,)), ((), ())), preferred_element_type=F32
                )
                scores = scores + bias
                top = jnp.max(scores, axis=-1, keepdims=True)
                weights = jnp.exp2((scores - top) * factor)
                total = jnp.sum(weights, axis=-1, keepdims=True)
                summed = jnp.dot(weights.astype(BF16), v_all[...], preferred_element_type=F32)
                summed = (summed / total).astype(BF16)
                for h in range(per):
                    att[i * count : (i + 1) * count, (g + h) * HEAD_DIM : (g + h + 1) * HEAD_DIM] = summed[
                        h * count : (h + 1) * count
                    ]
            if has_decode:

                @pl.when(target == devices - 1)
                def _():
                    att[(i + 1) * count - decode_rows : (i + 1) * count, :] = dec_ref[...]

        product(att, w, 0, columns, half, keep_ref, give_ref)

    flops = 2 * len(order) * count * (2 * local_width * keys + local_width * model)
    n_vmem = 2 + 2 * devices + has_decode
    return pl.pallas_call(
        body,
        in_specs=[smem()] + [in_vmem()] * n_vmem,
        out_specs=[in_vmem()] * 3,
        out_shape=[jax.ShapeDtypeStruct((half, columns), BF16)] * 2 + [pltpu.VMEM((2 * half, local_width), BF16)],
        scratch_shapes=[
            pltpu.VMEM((keys, HEAD_DIM), BF16),
            pltpu.VMEM((keys, HEAD_DIM), BF16),
        ],
        compiler_params=params(24),
        cost_estimate=pl.CostEstimate(flops=flops, transcendentals=0, bytes_accessed=weight.size * 2),
    )(meta, queries, *history, *fresh, *([decoded] if has_decode else []), weight)


def finish(first, residual, own, given, crossed, gain, previous):
    block, model = residual.shape
    count = crossed[0].shape[0]
    tile = 16
    n_cross = len(crossed)
    n_columns = model // crossed[0].shape[1]

    def body(res_ref, own_ref, given_ref, *refs):
        cross = refs[:n_cross]
        gain_ref = refs[n_cross]
        outs = refs[-5:-3]
        staged, sem = refs[-3:-1], refs[-1]
        copies = []
        for i in range(0, count, tile):
            here, local = slice(first + i, first + i + tile), slice(i, i + tile)
            hidden = res_ref[here, :].astype(F32) + own_ref[here, :].astype(F32) + given_ref[here, :].astype(F32)
            for c in range(0, n_cross, n_columns):
                pieces = [piece[local, :].astype(F32) for piece in cross[c : c + n_columns]]
                hidden = hidden + (jnp.concatenate(pieces, axis=1) if n_columns > 1 else pieces[0])
            mean = jnp.mean(hidden * hidden, axis=-1, keepdims=True)
            staged[0][local, :] = hidden.astype(BF16)
            staged[1][local, :] = (hidden * lax.rsqrt(mean + EPS) * gain_ref[...]).astype(BF16)
            for source, target in zip(staged, outs):
                copies.append(pltpu.make_async_copy(source.at[local, :], target.at[here, :], sem.at[len(copies)]))
                copies[-1].start()
        for copy in copies:
            copy.wait()

    n_in = 3 + n_cross + 1
    return pl.pallas_call(
        body,
        in_specs=[in_vmem()] * n_in + [hbm()] * len(previous),
        out_specs=[hbm()] * 2,
        out_shape=[jax.ShapeDtypeStruct((block, model), BF16)] * 2,
        input_output_aliases={n_in + i: i for i in range(len(previous))},
        scratch_shapes=[pltpu.VMEM((count, model), BF16)] * 2 + [pltpu.SemaphoreType.DMA((2 * count // tile,))],
        compiler_params=params(8),
        cost_estimate=busy(2),
    )(residual, own, given, *crossed, gain, *previous)


def step(
    prompt_queries,
    prompt_entries,
    history_cache,
    decode_queries,
    decode_entries,
    decode_cache,
    decode_lengths,
    prompt_start,
    out_weight,
    residual,
    norm_gain,
):
    devices = lax.axis_size("tp")
    local_heads = prompt_queries.shape[1] // HEAD_DIM
    kv_heads = history_cache.shape[2] // HEAD_DIM
    group = devices * local_heads // kv_heads
    block = residual.shape[0]
    h_rows, p_rows = history_cache.shape[1], prompt_entries.shape[1]
    assert group % local_heads == 0 and devices & (devices - 1) == 0
    assert block >= decode_queries.shape[0]

    def swap(value, k):
        return lax.ppermute(value, "tp", [(i, i ^ k) for i in range(devices)])

    def swapped(values):
        return [values[0]] + [swap(values[k], k) for k in range(1, devices)]

    packed, own_query = pack_history(history_cache, decode_queries, devices, local_heads, group)
    decode_rows = {0: own_query}
    for k in range(2, devices, 2):
        decode_rows[k] = swap(own_query, k)
    for k in range(1, devices, 2):
        decode_rows[k] = swap(decode_rows[k ^ 1], 1)
    history = swapped(packed)
    meta = jnp.concatenate([lax.axis_index("tp").astype(jnp.int32)[None], prompt_start, decode_lengths])
    fresh = swapped(pack_fresh(prompt_entries, meta, devices, local_heads, group))
    ordered = [decode_rows[k] for k in range(devices)]
    parts, queries, entries = decode_partials(
        ordered, decode_cache, prompt_queries, decode_queries, decode_entries, meta, local_heads, group
    )
    parts = swapped(parts)
    decoded = decode_join(parts, own_query, entries, local_heads)

    def attended(slots, first, count, decoded, columns):
        return attend(
            slots, first, count, block, queries, history, fresh, decoded, out_weight, meta, h_rows, p_rows, columns
        )

    def chip_sum(keep, give):
        return keep.astype(F32) + swap(give, 1).astype(F32)

    def cross(pair, count, start, stop):
        return [
            swap(pair[k * count + start : k * count + stop].astype(BF16), 2 * k + 2)
            for k in range(devices // 2 - 1)
        ]

    chunks = [c * block // sum(CHUNKS) for c in CHUNKS]
    if any(c % 16 for c in chunks):
        chunks = [block]
    model = out_weight.shape[1]
    others = list(range(2, devices))
    crossed, first = [], 0
    for count in chunks:
        last = first + count == block
        columns = model if last else model // 2
        keep, give, att = attended(others, first, count, decoded if last else None, columns)
        pair = chip_sum(keep, give)
        if last:
            half = count // 2 if count % 32 == 0 else count
            for start in range(0, count, half):
                crossed.append((first + start, cross(pair, count, start, start + half)))
        else:
            pieces = [cross(pair, count, 0, count)]
            keep, give = project(att, out_weight, columns)
            pair = chip_sum(keep, give)
            pieces.append(cross(pair, count, 0, count))
            crossed.append((first, [piece for both in zip(*pieces) for piece in both]))
        first += count
    own, give, _ = attended([0, 1], 0, block, decoded, model)
    given = swap(give, 1)
    gain = norm_gain[None, :]
    outs = []
    for first, pieces in crossed:
        outs = finish(first, residual, own, given, pieces, gain, outs)
    return tuple(outs)


def solution(mesh):
    placed = (
        P("rep", "tp"),
        P("rep", "tp", None),
        P("rep", "tp", None),
        P("rep", "tp"),
        P("rep", None, None),
        P("rep", None, "tp", None),
        P("rep"),
        P("rep"),
        P("tp", None),
        P("tp", "rep"),
        P(),
    )
    return jax.shard_map(
        step,
        mesh=mesh,
        in_specs=placed,
        out_specs=(P("tp", "rep"), P("tp", "rep")),
        check_vma=False,
    )
```

```python
import jax
import jax.numpy as jnp
import numpy as np
from jax import lax
from jax.experimental import pallas as pl
from jax.experimental.pallas import tpu as pltpu
from jax.sharding import PartitionSpec as P


HEAD_DIM = 128
MASKED = -1e30
EPS = 1e-05
CHUNKS = (64, 64)
COLUMNS = 512
GROUP_ROWS = 256
PIPE, ONES, SPLITQ = True, True, True

F32 = jnp.float32
BF16 = jnp.bfloat16


def round_up(value, unit):
    return -(-value // unit) * unit


def smem():
    return pl.BlockSpec(memory_space=pltpu.SMEM)


def hbm():
    return pl.BlockSpec(memory_space=pl.ANY)


def in_hbm():
    return pl.BlockSpec(memory_space=pltpu.HBM)


def in_vmem():
    return pl.BlockSpec(memory_space=pltpu.VMEM)


def to_hbm(value):
    return pltpu.with_memory_space_constraint(value, pltpu.HBM)


def busy(us):
    return pl.CostEstimate(flops=us * 500_000_000, transcendentals=0, bytes_accessed=us * 1_000_000)


def params(mib, **kwargs):
    return pltpu.CompilerParams(vmem_limit_bytes=mib << 20, **kwargs)


def pack_history(history, queries, slots, local_heads, group):
    h_rows = history.shape[1]
    rows = queries.shape[0]
    devices = len(slots)

    def body(h_hbm, q_hbm, *refs):
        o_refs, q_ref, sem = refs[:devices], refs[devices], refs[devices + 1]
        me = lax.axis_index("tp")
        copies = []
        for i, k in enumerate(slots):
            lane = pl.multiple_of((me ^ k) * local_heads // group * HEAD_DIM, HEAD_DIM)
            for part in range(2):
                copies.append(
                    pltpu.make_async_copy(
                        h_hbm.at[part, :, pl.ds(lane, HEAD_DIM)],
                        o_refs[i].at[part * h_rows : (part + 1) * h_rows, :],
                        sem.at[len(copies)],
                    )
                )
        for h in range(local_heads):
            copies.append(
                pltpu.make_async_copy(
                    q_hbm.at[:, h * HEAD_DIM : (h + 1) * HEAD_DIM],
                    q_ref.at[h * rows : (h + 1) * rows, :],
                    sem.at[len(copies)],
                )
            )
        for copy in copies:
            copy.start()
        for copy in copies:
            copy.wait()

    outs = pl.pallas_call(
        body,
        in_specs=[in_hbm()] * 2,
        out_specs=[in_vmem()] * (devices + 1),
        out_shape=[jax.ShapeDtypeStruct((2 * h_rows, HEAD_DIM), BF16)] * devices
        + [jax.ShapeDtypeStruct((rows * local_heads, HEAD_DIM), BF16)],
        scratch_shapes=[pltpu.SemaphoreType.DMA((2 * devices + local_heads,))],
        compiler_params=params(2),
        cost_estimate=busy(6),
        name="pack_history",
    )(to_hbm(history), to_hbm(queries))
    return dict(zip(slots, outs)), outs[devices]


def pack_fresh(prompt, history, queries, meta, slots, local_heads, group):
    h_rows, p_rows = history.shape[1], prompt.shape[1]
    p_pad = round_up(p_rows, 16)
    q_rows = queries[0].shape[0]
    every = [1] + slots
    n = len(every)

    def head_of(k):
        return lambda i, m: (0, 0, (m[0] ^ k) * local_heads // group)

    def body(m, *refs):
        p_refs, refs = refs[:n], refs[n:]
        h_hbm, refs = refs[0], refs[1:]
        q_refs, refs = refs[: len(queries)], refs[len(queries) :]
        o_refs, sem = refs[:n], refs[n]
        lane = pl.multiple_of((m[0] ^ 1) * local_heads // group * HEAD_DIM, HEAD_DIM)
        copies = [
            pltpu.make_async_copy(
                h_hbm.at[part, :, pl.ds(lane, HEAD_DIM)],
                o_refs[0].at[part * h_rows : (part + 1) * h_rows, :],
                sem.at[part],
            )
            for part in range(2)
        ]
        for copy in copies:
            copy.start()
        for i in range(n):
            row = 2 * h_rows if i == 0 else 0
            for part in range(2):
                if p_pad > p_rows:
                    fresh = jnp.concatenate(
                        [p_refs[i][part].astype(F32), jnp.zeros((p_pad - p_rows, HEAD_DIM), F32)], axis=0
                    ).astype(BF16)
                else:
                    fresh = p_refs[i][part]
                o_refs[i][row + part * p_pad : row + (part + 1) * p_pad, :] = fresh
        row = 2 * (h_rows + p_pad)
        for i, q_ref in enumerate(q_refs):
            o_refs[0][row + i * q_rows : row + (i + 1) * q_rows, :] = q_ref[...]
        for copy in copies:
            copy.wait()

    sizes = [2 * (h_rows + p_pad) + len(queries) * q_rows] + [2 * p_pad] * len(slots)
    outs = pl.pallas_call(
        body,
        grid_spec=pltpu.PrefetchScalarGridSpec(
            num_scalar_prefetch=1,
            grid=(1,),
            in_specs=[pl.BlockSpec((2, p_rows, HEAD_DIM), head_of(k)) for k in every]
            + [in_hbm()]
            + [in_vmem()] * len(queries),
            out_specs=[in_vmem()] * n,
            scratch_shapes=[pltpu.SemaphoreType.DMA((2,))],
        ),
        out_shape=[jax.ShapeDtypeStruct((size, HEAD_DIM), BF16) for size in sizes],
        compiler_params=params(8),
        cost_estimate=busy(12),
        name="pack_fresh",
    )(meta, *([prompt] * n), to_hbm(history), *queries)
    return outs[0], dict(zip(slots, outs[1:]))


def split(value):
    terms = []
    for _ in range(3):
        terms.append(value.astype(BF16))
        value = value - terms[-1].astype(F32)
    return terms


def decode_partials(queries, bundle, cache, prompt_queries, decode_queries, entries, meta, local_heads, group):
    devices = 2 * len(queries)
    rows, span, width = cache.shape[1], cache.shape[2], cache.shape[3]
    kv_heads = width // HEAD_DIM
    heads = devices * local_heads
    factor = HEAD_DIM ** (-0.5) * float(np.log2(np.e))
    part_rows = rows * local_heads
    stat_rows = round_up(local_heads, 8)
    prompt_rows = prompt_queries.shape[0]

    def body(m, *refs):
        q_refs, refs = refs[: devices // 2], refs[devices // 2 :]
        bundle_ref, cache_ref, pq_hbm, dq_hbm, e_hbm = refs[:5]
        o_refs, refs = refs[5 : 5 + devices], refs[5 + devices :]
        q_ref, e_ref, q_all, sums, sem = refs
        me = m[0]
        lane = pl.multiple_of(me * local_heads // group * HEAD_DIM, HEAD_DIM)
        copies = [
            pltpu.make_async_copy(pq_hbm, q_ref.at[0:prompt_rows, :], sem.at[0]),
            pltpu.make_async_copy(dq_hbm, q_ref.at[prompt_rows : prompt_rows + rows, :], sem.at[1]),
            pltpu.make_async_copy(e_hbm.at[:, :, pl.ds(lane, HEAD_DIM)], e_ref, sem.at[2]),
        ]
        for copy in copies:
            copy.start()
        for k in range(devices):
            base = bundle.shape[0] - (devices // 2 - k // 2) * part_rows if k % 2 else 0
            q_ref_k = bundle_ref if k % 2 else q_refs[k // 2]
            for h in range(local_heads):
                row = base + h * rows
                q_all[k, pl.ds(h, rows, stride=local_heads), :] = q_ref_k[row : row + rows, :].astype(F32)

        slot = lax.broadcasted_iota(jnp.int32, (heads, 1), 0) // local_heads
        reads = ((slot ^ me) * local_heads) // group
        lane = lax.broadcasted_iota(jnp.int32, (heads, HEAD_DIM), 1)
        place = me * span + lax.broadcasted_iota(jnp.int32, (1, span), 1)
        scores = []
        for b in range(rows):
            here = slice(b * local_heads, (b + 1) * local_heads)
            q = jnp.concatenate([q_all[k, here, :] for k in range(devices)], axis=0)
            spread = jnp.concatenate(
                [jnp.where(reads == g, q, 0.0) for g in range(kv_heads)], axis=1
            ).astype(BF16)
            score = lax.dot_general(
                spread, cache_ref[0, b], (((1,), (1,)), ((), ())), preferred_element_type=F32
            )
            scores.append(jnp.where(place < m[2 + b], score, MASKED))
        scores = jnp.concatenate(scores, axis=0)
        top = jnp.max(scores, axis=-1, keepdims=True)
        weights = jnp.where(scores > 0.5 * MASKED, jnp.exp2((scores - top) * factor), 0.0)
        total = jnp.sum(weights, axis=-1, keepdims=True)
        weights = weights.astype(BF16)
        stats = jnp.zeros((heads, HEAD_DIM), F32)
        for b in range(rows):
            these = slice(b * heads, (b + 1) * heads)
            summed = jnp.dot(weights[these], cache_ref[1, b], preferred_element_type=F32)
            own = jnp.zeros((heads, HEAD_DIM), F32)
            for g in range(kv_heads):
                own = own + jnp.where(reads == g, summed[:, g * HEAD_DIM : (g + 1) * HEAD_DIM], 0.0)
            for k in range(devices):
                sums[k, b * local_heads : (b + 1) * local_heads, :] = own[k * local_heads : (k + 1) * local_heads]
            stats = jnp.where(lane == b, top[these], jnp.where(lane == rows + b, total[these], stats))
        terms = split(stats)
        for k in range(devices):
            o_refs[k][0:part_rows, :] = sums[k].astype(BF16)
            for i, term in enumerate(terms):
                row = part_rows + i * stat_rows
                o_refs[k][row : row + local_heads, :] = term[k * local_heads : (k + 1) * local_heads, :]
        for copy in copies:
            copy.wait()

    outs = pl.pallas_call(
        body,
        in_specs=[smem()] + [in_vmem()] * (devices // 2 + 2) + [in_hbm()] * 3,
        out_specs=[in_vmem()] * (devices + 2),
        scratch_shapes=[pltpu.VMEM((devices, part_rows, HEAD_DIM), F32)] * 2 + [pltpu.SemaphoreType.DMA((3,))],
        out_shape=[jax.ShapeDtypeStruct((part_rows + 3 * stat_rows, HEAD_DIM), BF16)] * devices
        + [
            pltpu.VMEM((prompt_rows + rows, prompt_queries.shape[1]), BF16),
            pltpu.VMEM((2, rows, HEAD_DIM), BF16),
        ],
        compiler_params=params(12),
        cost_estimate=busy(12),
        name="decode",
    )(meta, *queries, bundle, cache, to_hbm(prompt_queries), to_hbm(decode_queries), to_hbm(entries))
    return outs[:devices], outs[devices], outs[devices + 1]


def decode_join(parts, queries, entries, local_heads):
    devices = len(parts)
    rows = entries.shape[1]
    factor = HEAD_DIM ** (-0.5) * float(np.log2(np.e))
    part_rows = rows * local_heads
    stat_rows = round_up(local_heads, 8)

    def body(*refs):
        p_refs = refs[:devices]
        q_ref, e_ref, o_ref, q_all, out = refs[devices:]
        for h in range(local_heads):
            q_all[pl.ds(h, rows, stride=local_heads), :] = q_ref[h * rows : (h + 1) * rows, :].astype(F32)
        stats = []
        for p in p_refs:
            starts = [part_rows + i * stat_rows for i in range(3)]
            high, middle, low = [p[row : row + local_heads, :].astype(F32) for row in starts]
            stats.append(high + middle + low)
        keys, values = e_ref[0].astype(F32), e_ref[1].astype(F32)
        sums = [p[0:part_rows, :].astype(F32) for p in p_refs]
        for b in range(rows):
            here = slice(b * local_heads, (b + 1) * local_heads)
            own = jnp.sum(q_all[here, :] * keys[b : b + 1, :], axis=-1, keepdims=True)
            tops = [s[:, b : b + 1] for s in stats]
            top = own
            for t in tops:
                top = jnp.maximum(top, t)
            weight = jnp.exp2((own - top) * factor)
            total = weight
            summed = weight.astype(BF16).astype(F32) * values[b : b + 1, :]
            for s, t, p in zip(stats, tops, sums):
                share = jnp.exp2((t - top) * factor)
                total = total + share * s[:, rows + b : rows + b + 1]
                summed = summed + share * p[here, :]
            out[here, :] = summed / total
        for h in range(local_heads):
            o_ref[:, h * HEAD_DIM : (h + 1) * HEAD_DIM] = out[pl.ds(h, rows, stride=local_heads), :].astype(BF16)

    return pl.pallas_call(
        body,
        in_specs=[in_vmem()] * (devices + 2),
        out_specs=in_vmem(),
        scratch_shapes=[pltpu.VMEM((part_rows, HEAD_DIM), F32)] * 2,
        out_shape=jax.ShapeDtypeStruct((rows, local_heads * HEAD_DIM), BF16),
        compiler_params=params(4),
        cost_estimate=busy(1),
        name="join",
    )(*parts, queries, entries)


def product(att, w, start, stop, half, keep_ref, give_ref):
    for c in range(start, stop, COLUMNS):
        out = jnp.dot(att[...], w[:, c : c + COLUMNS], preferred_element_type=F32).astype(BF16)
        keep_ref[:, c - start : c - start + COLUMNS] = out[:half]
        give_ref[:, c - start : c - start + COLUMNS] = out[half:]


def project(att, weight, start):
    rows, model = att.shape[0], weight.shape[1]

    def body(att_ref, w, keep_ref, give_ref):
        product(att_ref, w, start, model, rows // 2, keep_ref, give_ref)

    return pl.pallas_call(
        body,
        in_specs=[in_vmem()] * 2,
        out_specs=[in_vmem()] * 2,
        out_shape=[jax.ShapeDtypeStruct((rows // 2, model - start), BF16)] * 2,
        compiler_params=params(8),
        cost_estimate=busy(2),
        name="project",
    )(att, weight)


def attend(slots, first, count, block, queries, history, fresh, bundle, decoded, weight, meta, h_rows, p_rows, columns):
    devices = len(history) + 1
    held = list(history)
    p_pad = fresh[0].shape[0] // 2
    local_width = queries.shape[1]
    local_heads = local_width // HEAD_DIM
    model = weight.shape[1]
    h_keys, p_keys = devices * h_rows, devices * p_pad
    keys = h_keys + p_keys
    order = [s for s in slots if s % 2 == 0] + [s for s in slots if s % 2 == 1]
    half = len(order) // 2 * count
    factor = HEAD_DIM ** (-0.5) * float(np.log2(np.e))
    per = max(1, min(local_heads, GROUP_ROWS // count))
    has_decode = decoded is not None
    decode_rows = decoded.shape[0] if has_decode else 0

    def body(m, q, *refs):
        bundle_ref, rest = refs[0], refs[1:]
        n = devices - 1
        cached = {1: (bundle_ref, 0), **{k: (ref, 0) for k, ref in zip(held, rest[:n])}}
        own = {1: (bundle_ref, 2 * h_rows), **{k: (ref, 0) for k, ref in zip(held, rest[n : 2 * n])}}
        rest = rest[2 * n :]
        if has_decode:
            dec_ref, rest = rest[0], rest[1:]
        w, keep_ref, give_ref, att, k_all, v_all = rest
        me, valid_rows = m[0], m[1]
        for k in range(devices):
            for part, dst in ((0, k_all), (1, v_all)):
                for copy in range(2 if SPLITQ and part == 0 else 1):
                    lanes = slice(copy * HEAD_DIM, (copy + 1) * HEAD_DIM)
                    ref, row = cached[k]
                    row += part * h_rows
                    dst[k * h_rows : (k + 1) * h_rows, lanes] = ref[row : row + h_rows, :]
                    ref, row = own[k]
                    row += part * p_pad
                    dst[h_keys + k * p_pad : h_keys + (k + 1) * p_pad, lanes] = ref[row : row + p_pad, :]
        if ONES:
            v_all[:, HEAD_DIM:] = jnp.ones((keys, HEAD_DIM), BF16)
        column = lax.broadcasted_iota(jnp.int32, (1, h_keys), 1)
        place = ((column // h_rows) ^ me) * h_rows + column % h_rows
        history_bias = jnp.where(place < valid_rows, 0.0, MASKED)
        column = lax.broadcasted_iota(jnp.int32, (1, p_keys), 1)
        inner = column % p_pad
        seen_from = jnp.where(inner < p_rows, ((column // p_pad) ^ me) * p_rows + inner, 1 << 20)
        steps = [(i, g) for i in range(len(order)) for g in range(0, local_heads, per)]
        biases = []
        for i, slot in enumerate(order):
            rows = (slot ^ me) * block + first + lax.broadcasted_iota(jnp.int32, (count, 1), 0)
            bias = jnp.where(seen_from <= rows, 0.0, MASKED)
            biases.append(jnp.concatenate([jnp.broadcast_to(history_bias, (count, h_keys)), bias], axis=1))

        def scores_of(i, g):
            row0 = pl.multiple_of((order[i] ^ me) * block + first, 16)
            stacked = jnp.concatenate(
                [q[pl.ds(row0, count), h * HEAD_DIM : (h + 1) * HEAD_DIM] for h in range(g, g + per)], axis=0
            )
            if SPLITQ:
                scaled = stacked.astype(F32) * factor
                high = scaled.astype(BF16)
                low = (scaled - high.astype(F32)).astype(BF16)
                stacked = jnp.concatenate([high, low], axis=1)
            scores = lax.dot_general(
                stacked, k_all[...], (((1,), (1,)), ((), ())), preferred_element_type=F32
            )
            return (scores.reshape(per, count, keys) + biases[i][None]).reshape(per * count, keys)

        ahead = scores_of(*steps[0])
        for t, (i, g) in enumerate(steps):
            scores = ahead
            if PIPE and t + 1 < len(steps):
                ahead = scores_of(*steps[t + 1])
            top = jnp.max(scores, axis=-1, keepdims=True)
            weights = jnp.exp2(scores - top) if SPLITQ else jnp.exp2((scores - top) * factor)
            if not ONES:
                total = jnp.sum(weights, axis=-1, keepdims=True)
            summed = jnp.dot(weights.astype(BF16), v_all[...], preferred_element_type=F32)
            if ONES:
                total = summed[:, HEAD_DIM:]
                summed = summed[:, :HEAD_DIM]
            summed = (summed / total).astype(BF16)
            for h in range(per):
                att[i * count : (i + 1) * count, (g + h) * HEAD_DIM : (g + h + 1) * HEAD_DIM] = summed[
                    h * count : (h + 1) * count
                ]
            if not PIPE and t + 1 < len(steps):
                ahead = scores_of(*steps[t + 1])
        if has_decode:
            for i, slot in enumerate(order):

                @pl.when(slot ^ me == devices - 1)
                def _():
                    att[(i + 1) * count - decode_rows : (i + 1) * count, :] = dec_ref[...]

        product(att, w, 0, columns, half, keep_ref, give_ref)

    flops = 2 * len(order) * count * (2 * local_width * keys + local_width * model)
    n_vmem = 1 + 2 * devices + has_decode
    return pl.pallas_call(
        body,
        in_specs=[smem()] + [in_vmem()] * n_vmem,
        out_specs=[in_vmem()] * 3,
        out_shape=[jax.ShapeDtypeStruct((half, columns), BF16)] * 2 + [pltpu.VMEM((2 * half, local_width), BF16)],
        scratch_shapes=[
            pltpu.VMEM((keys, HEAD_DIM * (2 if SPLITQ else 1)), BF16),
            pltpu.VMEM((keys, HEAD_DIM * (2 if ONES else 1)), BF16),
        ],
        compiler_params=params(24),
        cost_estimate=pl.CostEstimate(flops=flops, transcendentals=0, bytes_accessed=weight.size * 2),
    )(meta, queries, bundle, *history.values(), *fresh.values(), *([decoded] if has_decode else []), weight)


def finish(first, begin, residual, own, given, crossed, gain, previous):
    block, model = residual.shape
    count = crossed[0].shape[0]
    tile = 16
    n_cross = len(crossed)
    n_columns = model // crossed[0].shape[1]

    def body(res_ref, own_ref, given_ref, *refs):
        cross = refs[:n_cross]
        gain_ref = refs[n_cross]
        outs = refs[-5:-3]
        staged, sem = refs[-3:-1], refs[-1]
        copies = []
        for i in range(0, count, tile):
            here, local = slice(first + i, first + i + tile), slice(i, i + tile)
            mine = slice(begin + i, begin + i + tile)
            hidden = res_ref[here, :].astype(F32) + own_ref[mine, :].astype(F32) + given_ref[mine, :].astype(F32)
            for c in range(0, n_cross, n_columns):
                pieces = [piece[local, :].astype(F32) for piece in cross[c : c + n_columns]]
                hidden = hidden + (jnp.concatenate(pieces, axis=1) if n_columns > 1 else pieces[0])
            mean = jnp.mean(hidden * hidden, axis=-1, keepdims=True)
            staged[0][local, :] = hidden.astype(BF16)
            staged[1][local, :] = (hidden * lax.rsqrt(mean + EPS) * gain_ref[...]).astype(BF16)
            for source, target in zip(staged, outs):
                copies.append(pltpu.make_async_copy(source.at[local, :], target.at[here, :], sem.at[len(copies)]))
                copies[-1].start()
        for copy in copies:
            copy.wait()

    n_in = 3 + n_cross + 1
    return pl.pallas_call(
        body,
        in_specs=[in_vmem()] * n_in + [hbm()] * len(previous),
        out_specs=[hbm()] * 2,
        out_shape=[jax.ShapeDtypeStruct((block, model), BF16)] * 2,
        input_output_aliases={n_in + i: i for i in range(len(previous))},
        scratch_shapes=[pltpu.VMEM((count, model), BF16)] * 2 + [pltpu.SemaphoreType.DMA((2 * count // tile,))],
        compiler_params=params(8),
        cost_estimate=busy(2),
    )(residual, own, given, *crossed, gain, *previous)


def step(
    prompt_queries,
    prompt_entries,
    history_cache,
    decode_queries,
    decode_entries,
    decode_cache,
    decode_lengths,
    prompt_start,
    out_weight,
    residual,
    norm_gain,
):
    devices = lax.axis_size("tp")
    local_heads = prompt_queries.shape[1] // HEAD_DIM
    kv_heads = history_cache.shape[2] // HEAD_DIM
    group = devices * local_heads // kv_heads
    block = residual.shape[0]
    h_rows, p_rows = history_cache.shape[1], prompt_entries.shape[1]
    assert group % local_heads == 0 and devices & (devices - 1) == 0
    assert block >= decode_queries.shape[0]

    def swap(value, k):
        return lax.ppermute(value, "tp", [(i, i ^ k) for i in range(devices)])

    def swapped(values):
        return [values[0]] + [swap(values[k], k) for k in range(1, devices)]

    slots = [0] + list(range(2, devices))
    packed, own_query = pack_history(history_cache, decode_queries, slots, local_heads, group)
    even_queries = [own_query] + [swap(own_query, k) for k in range(2, devices, 2)]
    history = {k: swap(packed[k], k) if k else packed[k] for k in slots}
    meta = jnp.concatenate([lax.axis_index("tp").astype(jnp.int32)[None], prompt_start, decode_lengths])
    bundle, packed = pack_fresh(prompt_entries, history_cache, even_queries, meta, slots, local_heads, group)
    bundle = swap(bundle, 1)
    fresh = {k: swap(packed[k], k) if k else packed[k] for k in slots}
    parts, queries, entries = decode_partials(
        even_queries, bundle, decode_cache, prompt_queries, decode_queries, decode_entries, meta, local_heads, group
    )
    parts = swapped(parts)
    decoded = decode_join(parts, own_query, entries, local_heads)

    def attended(slots, first, count, decoded, columns):
        return attend(
            slots, first, count, block, queries, history, fresh, bundle, decoded, out_weight, meta, h_rows, p_rows, columns
        )

    def chip_sum(keep, give):
        return keep.astype(F32) + swap(give, 1).astype(F32)

    def cross(pair, count, start, stop):
        return [
            swap(pair[k * count + start : k * count + stop].astype(BF16), 2 * k + 2)
            for k in range(devices // 2 - 1)
        ]

    chunks = [c * block // sum(CHUNKS) for c in CHUNKS]
    if any(c % 16 for c in chunks):
        chunks = [block]
    model = out_weight.shape[1]
    others = list(range(2, devices))
    crossed, first = [], 0
    for count in chunks:
        last = first + count == block
        columns = model if last else model // 2
        keep, give, att = attended(others, first, count, decoded if last else None, columns)
        pair = chip_sum(keep, give)
        if last:
            half = count // 2 if count % 32 == 0 else count
            for start in range(0, count, half):
                crossed.append((first + start, cross(pair, count, start, start + half)))
        else:
            pieces = [cross(pair, count, 0, count)]
            keep, give = project(att, out_weight, columns)
            pair = chip_sum(keep, give)
            pieces.append(cross(pair, count, 0, count))
            crossed.append((first, [piece for both in zip(*pieces) for piece in both]))
        first += count
    owned, first = [], 0
    for count in chunks:
        here = decoded if first + count == block else None
        own, give, _ = attended([0, 1], first, count, here, model)
        owned.append((first, own, swap(give, 1)))
        first += count
    gain = norm_gain[None, :]
    outs = []
    for first, pieces in crossed:
        begin, own, given = [o for o in owned if o[0] <= first][-1]
        outs = finish(first, first - begin, residual, own, given, pieces, gain, outs)
    return tuple(outs)


def solution(mesh):
    placed = (
        P("rep", "tp"),
        P("rep", "tp", None),
        P("rep", "tp", None),
        P("rep", "tp"),
        P("rep", None, None),
        P("rep", None, "tp", None),
        P("rep"),
        P("rep"),
        P("tp", None),
        P("tp", "rep"),
        P(),
    )
    return jax.shard_map(
        step,
        mesh=mesh,
        in_specs=placed,
        out_specs=(P("tp", "rep"), P("tp", "rep")),
        check_vma=False,
    )
```

```python
import jax
import jax.numpy as jnp
import numpy as np
from jax import lax
from jax.experimental import pallas as pl
from jax.experimental.pallas import tpu as pltpu
from jax.sharding import PartitionSpec as P


HEAD_DIM = 128
MASKED = -1e30
EPS = 1e-05
CHUNKS = (64, 64)
COLUMNS = 512
FIRST_PART = 4
GROUP_ROWS = 256

F32 = jnp.float32
BF16 = jnp.bfloat16


def round_up(value, unit):
    return -(-value // unit) * unit


def smem():
    return pl.BlockSpec(memory_space=pltpu.SMEM)


def hbm():
    return pl.BlockSpec(memory_space=pl.ANY)


def in_hbm():
    return pl.BlockSpec(memory_space=pltpu.HBM)


def in_vmem():
    return pl.BlockSpec(memory_space=pltpu.VMEM)


def to_hbm(value):
    return pltpu.with_memory_space_constraint(value, pltpu.HBM)


def busy(us):
    return pl.CostEstimate(flops=us * 500_000_000, transcendentals=0, bytes_accessed=us * 1_000_000)


def params(mib, **kwargs):
    return pltpu.CompilerParams(vmem_limit_bytes=mib << 20, **kwargs)


def pack_history(history, queries, slots, local_heads, group):
    h_rows = history.shape[1]
    rows = queries.shape[0]
    devices = len(slots)

    def body(h_hbm, q_hbm, *refs):
        o_refs, q_ref, sem = refs[:devices], refs[devices], refs[devices + 1]
        me = lax.axis_index("tp")
        copies = []
        for i, k in enumerate(slots):
            lane = pl.multiple_of((me ^ k) * local_heads // group * HEAD_DIM, HEAD_DIM)
            for part in range(2):
                copies.append(
                    pltpu.make_async_copy(
                        h_hbm.at[part, :, pl.ds(lane, HEAD_DIM)],
                        o_refs[i].at[part * h_rows : (part + 1) * h_rows, :],
                        sem.at[len(copies)],
                    )
                )
        for h in range(local_heads):
            copies.append(
                pltpu.make_async_copy(
                    q_hbm.at[:, h * HEAD_DIM : (h + 1) * HEAD_DIM],
                    q_ref.at[h * rows : (h + 1) * rows, :],
                    sem.at[len(copies)],
                )
            )
        for copy in copies:
            copy.start()
        for copy in copies:
            copy.wait()

    outs = pl.pallas_call(
        body,
        in_specs=[in_hbm()] * 2,
        out_specs=[in_vmem()] * (devices + 1),
        out_shape=[jax.ShapeDtypeStruct((2 * h_rows, HEAD_DIM), BF16)] * devices
        + [jax.ShapeDtypeStruct((rows * local_heads, HEAD_DIM), BF16)],
        scratch_shapes=[pltpu.SemaphoreType.DMA((2 * devices + local_heads,))],
        compiler_params=params(2),
        cost_estimate=busy(6),
        name="pack_history",
    )(to_hbm(history), to_hbm(queries))
    return dict(zip(slots, outs)), outs[devices]


def pack_fresh(prompt, history, queries, meta, slots, local_heads, group):
    h_rows, p_rows = history.shape[0] // 2, prompt.shape[1]
    p_pad = round_up(p_rows, 16)
    q_rows = queries[0].shape[0]
    every = [1] + slots
    n = len(every)

    def head_of(k):
        return lambda i, m: (0, 0, (m[0] ^ k) * local_heads // group)

    def body(m, *refs):
        p_refs, refs = refs[:n], refs[n:]
        h_ref, refs = refs[0], refs[1:]
        q_refs, o_refs = refs[: len(queries)], refs[len(queries) :]
        o_refs[0][0 : 2 * h_rows, :] = h_ref[...]
        for i in range(n):
            row = 2 * h_rows if i == 0 else 0
            for part in range(2):
                if p_pad > p_rows:
                    fresh = jnp.concatenate(
                        [p_refs[i][part].astype(F32), jnp.zeros((p_pad - p_rows, HEAD_DIM), F32)], axis=0
                    ).astype(BF16)
                else:
                    fresh = p_refs[i][part]
                o_refs[i][row + part * p_pad : row + (part + 1) * p_pad, :] = fresh
        row = 2 * (h_rows + p_pad)
        for i, q_ref in enumerate(q_refs):
            o_refs[0][row + i * q_rows : row + (i + 1) * q_rows, :] = q_ref[...]

    sizes = [2 * (h_rows + p_pad) + len(queries) * q_rows] + [2 * p_pad] * len(slots)
    outs = pl.pallas_call(
        body,
        grid_spec=pltpu.PrefetchScalarGridSpec(
            num_scalar_prefetch=1,
            grid=(1,),
            in_specs=[pl.BlockSpec((2, p_rows, HEAD_DIM), head_of(k)) for k in every]
            + [in_vmem()] * (1 + len(queries)),
            out_specs=[in_vmem()] * n,
        ),
        out_shape=[jax.ShapeDtypeStruct((size, HEAD_DIM), BF16) for size in sizes],
        compiler_params=params(8),
        cost_estimate=busy(12),
        name="pack_fresh",
    )(meta, *([prompt] * n), history, *queries)
    return outs[0], dict(zip(slots, outs[1:]))


def split(value):
    terms = []
    for _ in range(3):
        terms.append(value.astype(BF16))
        value = value - terms[-1].astype(F32)
    return terms


def decode_partials(queries, bundle, cache, prompt_queries, decode_queries, entries, meta, local_heads, group):
    devices = 2 * len(queries)
    rows, span, width = cache.shape[1], cache.shape[2], cache.shape[3]
    kv_heads = width // HEAD_DIM
    heads = devices * local_heads
    factor = HEAD_DIM ** (-0.5) * float(np.log2(np.e))
    part_rows = rows * local_heads
    stat_rows = round_up(local_heads, 8)
    prompt_rows = prompt_queries.shape[0]

    def body(m, *refs):
        q_refs, refs = refs[: devices // 2], refs[devices // 2 :]
        bundle_ref, cache_ref, pq_hbm, dq_hbm, e_hbm = refs[:5]
        o_refs, refs = refs[5 : 5 + devices], refs[5 + devices :]
        q_ref, e_ref, q_all, sums, sem = refs
        me = m[0]
        lane = pl.multiple_of(me * local_heads // group * HEAD_DIM, HEAD_DIM)
        copies = [
            pltpu.make_async_copy(pq_hbm, q_ref.at[0:prompt_rows, :], sem.at[0]),
            pltpu.make_async_copy(dq_hbm, q_ref.at[prompt_rows : prompt_rows + rows, :], sem.at[1]),
            pltpu.make_async_copy(e_hbm.at[:, :, pl.ds(lane, HEAD_DIM)], e_ref, sem.at[2]),
        ]
        for copy in copies:
            copy.start()
        for k in range(devices):
            base = bundle.shape[0] - (devices // 2 - k // 2) * part_rows if k % 2 else 0
            q_ref_k = bundle_ref if k % 2 else q_refs[k // 2]
            for h in range(local_heads):
                row = base + h * rows
                q_all[k, pl.ds(h, rows, stride=local_heads), :] = q_ref_k[row : row + rows, :].astype(F32)

        slot = lax.broadcasted_iota(jnp.int32, (heads, 1), 0) // local_heads
        reads = ((slot ^ me) * local_heads) // group
        lane = lax.broadcasted_iota(jnp.int32, (heads, HEAD_DIM), 1)
        place = me * span + lax.broadcasted_iota(jnp.int32, (1, span), 1)
        scores = []
        for b in range(rows):
            here = slice(b * local_heads, (b + 1) * local_heads)
            q = jnp.concatenate([q_all[k, here, :] for k in range(devices)], axis=0)
            spread = jnp.concatenate(
                [jnp.where(reads == g, q, 0.0) for g in range(kv_heads)], axis=1
            ).astype(BF16)
            score = lax.dot_general(
                spread, cache_ref[0, b], (((1,), (1,)), ((), ())), preferred_element_type=F32
            )
            scores.append(jnp.where(place < m[2 + b], score, MASKED))
        scores = jnp.concatenate(scores, axis=0)
        top = jnp.max(scores, axis=-1, keepdims=True)
        weights = jnp.where(scores > 0.5 * MASKED, jnp.exp2((scores - top) * factor), 0.0)
        total = jnp.sum(weights, axis=-1, keepdims=True)
        weights = weights.astype(BF16)
        stats = jnp.zeros((heads, HEAD_DIM), F32)
        for b in range(rows):
            these = slice(b * heads, (b + 1) * heads)
            summed = jnp.dot(weights[these], cache_ref[1, b], preferred_element_type=F32)
            own = jnp.zeros((heads, HEAD_DIM), F32)
            for g in range(kv_heads):
                own = own + jnp.where(reads == g, summed[:, g * HEAD_DIM : (g + 1) * HEAD_DIM], 0.0)
            for k in range(devices):
                sums[k, b * local_heads : (b + 1) * local_heads, :] = own[k * local_heads : (k + 1) * local_heads]
            stats = jnp.where(lane == b, top[these], jnp.where(lane == rows + b, total[these], stats))
        terms = split(stats)
        for k in range(devices):
            o_refs[k][0:part_rows, :] = sums[k].astype(BF16)
            for i, term in enumerate(terms):
                row = part_rows + i * stat_rows
                o_refs[k][row : row + local_heads, :] = term[k * local_heads : (k + 1) * local_heads, :]
        for copy in copies:
            copy.wait()

    outs = pl.pallas_call(
        body,
        in_specs=[smem()] + [in_vmem()] * (devices // 2 + 2) + [in_hbm()] * 3,
        out_specs=[in_vmem()] * (devices + 2),
        scratch_shapes=[pltpu.VMEM((devices, part_rows, HEAD_DIM), F32)] * 2 + [pltpu.SemaphoreType.DMA((3,))],
        out_shape=[jax.ShapeDtypeStruct((part_rows + 3 * stat_rows, HEAD_DIM), BF16)] * devices
        + [
            pltpu.VMEM((prompt_rows + rows, prompt_queries.shape[1]), BF16),
            pltpu.VMEM((2, rows, HEAD_DIM), BF16),
        ],
        compiler_params=params(12),
        cost_estimate=busy(12),
        name="decode",
    )(meta, *queries, bundle, cache, to_hbm(prompt_queries), to_hbm(decode_queries), to_hbm(entries))
    return outs[:devices], outs[devices], outs[devices + 1]


def decode_join(parts, queries, entries, local_heads):
    devices = len(parts)
    rows = entries.shape[1]
    factor = HEAD_DIM ** (-0.5) * float(np.log2(np.e))
    part_rows = rows * local_heads
    stat_rows = round_up(local_heads, 8)

    def body(*refs):
        p_refs = refs[:devices]
        q_ref, e_ref, o_ref, q_all, out = refs[devices:]
        for h in range(local_heads):
            q_all[pl.ds(h, rows, stride=local_heads), :] = q_ref[h * rows : (h + 1) * rows, :].astype(F32)
        stats = []
        for p in p_refs:
            starts = [part_rows + i * stat_rows for i in range(3)]
            high, middle, low = [p[row : row + local_heads, :].astype(F32) for row in starts]
            stats.append(high + middle + low)
        keys, values = e_ref[0].astype(F32), e_ref[1].astype(F32)
        sums = [p[0:part_rows, :].astype(F32) for p in p_refs]
        for b in range(rows):
            here = slice(b * local_heads, (b + 1) * local_heads)
            own = jnp.sum(q_all[here, :] * keys[b : b + 1, :], axis=-1, keepdims=True)
            tops = [s[:, b : b + 1] for s in stats]
            top = own
            for t in tops:
                top = jnp.maximum(top, t)
            weight = jnp.exp2((own - top) * factor)
            total = weight
            summed = weight.astype(BF16).astype(F32) * values[b : b + 1, :]
            for s, t, p in zip(stats, tops, sums):
                share = jnp.exp2((t - top) * factor)
                total = total + share * s[:, rows + b : rows + b + 1]
                summed = summed + share * p[here, :]
            out[here, :] = summed / total
        for h in range(local_heads):
            o_ref[:, h * HEAD_DIM : (h + 1) * HEAD_DIM] = out[pl.ds(h, rows, stride=local_heads), :].astype(BF16)

    return pl.pallas_call(
        body,
        in_specs=[in_vmem()] * (devices + 2),
        out_specs=in_vmem(),
        scratch_shapes=[pltpu.VMEM((part_rows, HEAD_DIM), F32)] * 2,
        out_shape=jax.ShapeDtypeStruct((rows, local_heads * HEAD_DIM), BF16),
        compiler_params=params(4),
        cost_estimate=busy(1),
        name="join",
    )(*parts, queries, entries)


def product(att, w, start, stop, half, keep_ref, give_ref):
    for c in range(start, stop, COLUMNS):
        out = jnp.dot(att[...], w[:, c : c + COLUMNS], preferred_element_type=F32).astype(BF16)
        keep_ref[:, c - start : c - start + COLUMNS] = out[:half]
        give_ref[:, c - start : c - start + COLUMNS] = out[half:]


def project(att, weight, start):
    rows, model = att.shape[0], weight.shape[1]

    def body(att_ref, w, keep_ref, give_ref):
        product(att_ref, w, start, model, rows // 2, keep_ref, give_ref)

    return pl.pallas_call(
        body,
        in_specs=[in_vmem()] * 2,
        out_specs=[in_vmem()] * 2,
        out_shape=[jax.ShapeDtypeStruct((rows // 2, model - start), BF16)] * 2,
        compiler_params=params(8),
        cost_estimate=busy(2),
        name="project",
    )(att, weight)


def attend(slots, first, count, block, queries, history, fresh, bundle, decoded, weight, meta, h_rows, p_rows, columns):
    devices = len(history) + 1
    held = list(history)
    p_pad = fresh[0].shape[0] // 2
    local_width = queries.shape[1]
    local_heads = local_width // HEAD_DIM
    model = weight.shape[1]
    h_keys, p_keys = devices * h_rows, devices * p_pad
    keys = h_keys + p_keys
    order = [s for s in slots if s % 2 == 0] + [s for s in slots if s % 2 == 1]
    half = len(order) // 2 * count
    factor = HEAD_DIM ** (-0.5) * float(np.log2(np.e))
    per = max(1, min(local_heads, GROUP_ROWS // count))
    has_decode = decoded is not None
    decode_rows = decoded.shape[0] if has_decode else 0

    def body(m, q, *refs):
        bundle_ref, rest = refs[0], refs[1:]
        n = devices - 1
        cached = {1: (bundle_ref, 0), **{k: (ref, 0) for k, ref in zip(held, rest[:n])}}
        own = {1: (bundle_ref, 2 * h_rows), **{k: (ref, 0) for k, ref in zip(held, rest[n : 2 * n])}}
        rest = rest[2 * n :]
        if has_decode:
            dec_ref, rest = rest[0], rest[1:]
        w, keep_ref, give_ref, att, k_all, v_all = rest
        me, valid_rows = m[0], m[1]
        for k in range(devices):
            for part, dst in ((0, k_all), (1, v_all)):
                for copy in range(2 - part):
                    lanes = slice(copy * HEAD_DIM, (copy + 1) * HEAD_DIM)
                    ref, row = cached[k]
                    row += part * h_rows
                    dst[k * h_rows : (k + 1) * h_rows, lanes] = ref[row : row + h_rows, :]
                    ref, row = own[k]
                    row += part * p_pad
                    dst[h_keys + k * p_pad : h_keys + (k + 1) * p_pad, lanes] = ref[row : row + p_pad, :]
        v_all[:, HEAD_DIM:] = jnp.ones((keys, HEAD_DIM), BF16)
        column = lax.broadcasted_iota(jnp.int32, (1, h_keys), 1)
        place = ((column // h_rows) ^ me) * h_rows + column % h_rows
        history_bias = jnp.where(place < valid_rows, 0.0, MASKED)
        column = lax.broadcasted_iota(jnp.int32, (1, p_keys), 1)
        inner = column % p_pad
        seen_from = jnp.where(inner < p_rows, ((column // p_pad) ^ me) * p_rows + inner, 1 << 20)
        steps = [(i, g) for i in range(len(order)) for g in range(0, local_heads, per)]
        biases = []
        for i, slot in enumerate(order):
            rows = (slot ^ me) * block + first + lax.broadcasted_iota(jnp.int32, (count, 1), 0)
            bias = jnp.where(seen_from <= rows, 0.0, MASKED)
            biases.append(jnp.concatenate([jnp.broadcast_to(history_bias, (count, h_keys)), bias], axis=1))

        def scores_of(i, g):
            row0 = pl.multiple_of((order[i] ^ me) * block + first, 16)
            stacked = jnp.concatenate(
                [q[pl.ds(row0, count), h * HEAD_DIM : (h + 1) * HEAD_DIM] for h in range(g, g + per)], axis=0
            )
            scaled = stacked.astype(F32) * factor
            high = scaled.astype(BF16)
            low = (scaled - high.astype(F32)).astype(BF16)
            stacked = jnp.concatenate([high, low], axis=1)
            scores = lax.dot_general(
                stacked, k_all[...], (((1,), (1,)), ((), ())), preferred_element_type=F32
            )
            return (scores.reshape(per, count, keys) + biases[i][None]).reshape(per * count, keys)

        ahead = scores_of(*steps[0])
        for t, (i, g) in enumerate(steps):
            scores = ahead
            if t + 1 < len(steps):
                ahead = scores_of(*steps[t + 1])
            top = jnp.max(scores, axis=-1, keepdims=True)
            weights = jnp.exp2(scores - top)
            summed = jnp.dot(weights.astype(BF16), v_all[...], preferred_element_type=F32)
            summed = (summed[:, :HEAD_DIM] / summed[:, HEAD_DIM:]).astype(BF16)
            for h in range(per):
                att[i * count : (i + 1) * count, (g + h) * HEAD_DIM : (g + h + 1) * HEAD_DIM] = summed[
                    h * count : (h + 1) * count
                ]
        if has_decode:
            for i, slot in enumerate(order):

                @pl.when(slot ^ me == devices - 1)
                def _():
                    att[(i + 1) * count - decode_rows : (i + 1) * count, :] = dec_ref[...]

        product(att, w, 0, columns, half, keep_ref, give_ref)

    flops = 2 * len(order) * count * (2 * local_width * keys + local_width * model)
    n_vmem = 1 + 2 * devices + has_decode
    return pl.pallas_call(
        body,
        in_specs=[smem()] + [in_vmem()] * n_vmem,
        out_specs=[in_vmem()] * 3,
        out_shape=[jax.ShapeDtypeStruct((half, columns), BF16)] * 2 + [pltpu.VMEM((2 * half, local_width), BF16)],
        scratch_shapes=[
            pltpu.VMEM((keys, 2 * HEAD_DIM), BF16),
            pltpu.VMEM((keys, 2 * HEAD_DIM), BF16),
        ],
        compiler_params=params(24),
        cost_estimate=pl.CostEstimate(flops=flops, transcendentals=0, bytes_accessed=weight.size * 2),
    )(meta, queries, bundle, *history.values(), *fresh.values(), *([decoded] if has_decode else []), weight)


def finish(first, begin, residual, own, given, crossed, gain, previous):
    block, model = residual.shape
    count = crossed[0].shape[0]
    tile = 16
    n_cross = len(crossed)
    n_columns = 1 if crossed[0].shape[1] == model else 2

    def body(res_ref, own_ref, given_ref, *refs):
        cross = refs[:n_cross]
        gain_ref = refs[n_cross]
        outs = refs[-5:-3]
        staged, sem = refs[-3:-1], refs[-1]
        copies = []
        for i in range(0, count, tile):
            here, local = slice(first + i, first + i + tile), slice(i, i + tile)
            mine = slice(begin + i, begin + i + tile)
            hidden = res_ref[here, :].astype(F32) + own_ref[mine, :].astype(F32) + given_ref[mine, :].astype(F32)
            for c in range(0, n_cross, n_columns):
                pieces = [piece[local, :].astype(F32) for piece in cross[c : c + n_columns]]
                hidden = hidden + (jnp.concatenate(pieces, axis=1) if n_columns > 1 else pieces[0])
            mean = jnp.mean(hidden * hidden, axis=-1, keepdims=True)
            staged[0][local, :] = hidden.astype(BF16)
            staged[1][local, :] = (hidden * lax.rsqrt(mean + EPS) * gain_ref[...]).astype(BF16)
            for source, target in zip(staged, outs):
                copies.append(pltpu.make_async_copy(source.at[local, :], target.at[here, :], sem.at[len(copies)]))
                copies[-1].start()
        for copy in copies:
            copy.wait()

    n_in = 3 + n_cross + 1
    return pl.pallas_call(
        body,
        in_specs=[in_vmem()] * n_in + [hbm()] * len(previous),
        out_specs=[hbm()] * 2,
        out_shape=[jax.ShapeDtypeStruct((block, model), BF16)] * 2,
        input_output_aliases={n_in + i: i for i in range(len(previous))},
        scratch_shapes=[pltpu.VMEM((count, model), BF16)] * 2 + [pltpu.SemaphoreType.DMA((2 * count // tile,))],
        compiler_params=params(8),
        cost_estimate=busy(2),
    )(residual, own, given, *crossed, gain, *previous)


def step(
    prompt_queries,
    prompt_entries,
    history_cache,
    decode_queries,
    decode_entries,
    decode_cache,
    decode_lengths,
    prompt_start,
    out_weight,
    residual,
    norm_gain,
):
    devices = lax.axis_size("tp")
    local_heads = prompt_queries.shape[1] // HEAD_DIM
    kv_heads = history_cache.shape[2] // HEAD_DIM
    group = devices * local_heads // kv_heads
    block = residual.shape[0]
    h_rows, p_rows = history_cache.shape[1], prompt_entries.shape[1]
    assert group % local_heads == 0 and devices & (devices - 1) == 0
    assert block >= decode_queries.shape[0]

    def swap(value, k):
        return lax.ppermute(value, "tp", [(i, i ^ k) for i in range(devices)])

    def swapped(values):
        return [values[0]] + [swap(values[k], k) for k in range(1, devices)]

    slots = [0] + list(range(2, devices))
    packed, own_query = pack_history(history_cache, decode_queries, [1] + slots, local_heads, group)
    even_queries = [own_query] + [swap(own_query, k) for k in range(2, devices, 2)]
    history = {k: swap(packed[k], k) if k else packed[k] for k in slots}
    meta = jnp.concatenate([lax.axis_index("tp").astype(jnp.int32)[None], prompt_start, decode_lengths])
    bundle, packed = pack_fresh(prompt_entries, packed[1], even_queries, meta, slots, local_heads, group)
    bundle = swap(bundle, 1)
    fresh = {k: swap(packed[k], k) if k else packed[k] for k in slots}
    parts, queries, entries = decode_partials(
        even_queries, bundle, decode_cache, prompt_queries, decode_queries, decode_entries, meta, local_heads, group
    )
    parts = swapped(parts)
    decoded = decode_join(parts, own_query, entries, local_heads)

    def attended(slots, first, count, decoded, columns):
        return attend(
            slots, first, count, block, queries, history, fresh, bundle, decoded, out_weight, meta, h_rows, p_rows, columns
        )

    def chip_sum(keep, give):
        return keep.astype(F32) + swap(give, 1).astype(F32)

    def cross(pair, count, start, stop):
        return [
            swap(pair[k * count + start : k * count + stop].astype(BF16), 2 * k + 2)
            for k in range(devices // 2 - 1)
        ]

    chunks = [c * block // sum(CHUNKS) for c in CHUNKS]
    if any(c % 16 for c in chunks):
        chunks = [block]
    model = out_weight.shape[1]
    others = list(range(2, devices))
    crossed, first = [], 0
    for count in chunks:
        last = first + count == block
        columns = model if last else model // FIRST_PART
        keep, give, att = attended(others, first, count, decoded if last else None, columns)
        pair = chip_sum(keep, give)
        if last:
            cut = count - 16 if count > 16 else 0
            for start, stop in [(0, cut), (cut, count)] if cut else [(0, count)]:
                crossed.append((first + start, cross(pair, count, start, stop)))
        else:
            pieces = [cross(pair, count, 0, count)]
            keep, give = project(att, out_weight, columns)
            pair = chip_sum(keep, give)
            pieces.append(cross(pair, count, 0, count))
            crossed.append((first, [piece for both in zip(*pieces) for piece in both]))
        first += count
    owned, first = [], 0
    for count in chunks:
        here = decoded if first + count == block else None
        own, give, _ = attended([0, 1], first, count, here, model)
        owned.append((first, own, swap(give, 1)))
        first += count
    gain = norm_gain[None, :]
    outs = []
    for first, pieces in crossed:
        begin, own, given = [o for o in owned if o[0] <= first][-1]
        outs = finish(first, first - begin, residual, own, given, pieces, gain, outs)
    return tuple(outs)


def solution(mesh):
    placed = (
        P("rep", "tp"),
        P("rep", "tp", None),
        P("rep", "tp", None),
        P("rep", "tp"),
        P("rep", None, None),
        P("rep", None, "tp", None),
        P("rep"),
        P("rep"),
        P("tp", None),
        P("tp", "rep"),
        P(),
    )
    return jax.shard_map(
        step,
        mesh=mesh,
        in_specs=placed,
        out_specs=(P("tp", "rep"), P("tp", "rep")),
        check_vma=False,
    )
```

```python
import jax
import jax.numpy as jnp
import numpy as np
from jax import lax
from jax.experimental import pallas as pl
from jax.experimental.pallas import tpu as pltpu
from jax.sharding import PartitionSpec as P


HEAD_DIM = 128
MASKED = -1e30
EPS = 1e-05
CHUNKS = (64, 64)
COLUMNS = 512
FIRST_EIGHTHS = 3
GROUP_ROWS = 256

F32 = jnp.float32
BF16 = jnp.bfloat16


def round_up(value, unit):
    return -(-value // unit) * unit


def smem():
    return pl.BlockSpec(memory_space=pltpu.SMEM)


def hbm():
    return pl.BlockSpec(memory_space=pl.ANY)


def in_hbm():
    return pl.BlockSpec(memory_space=pltpu.HBM)


def in_vmem():
    return pl.BlockSpec(memory_space=pltpu.VMEM)


def to_hbm(value):
    return pltpu.with_memory_space_constraint(value, pltpu.HBM)


def busy(us):
    return pl.CostEstimate(flops=us * 500_000_000, transcendentals=0, bytes_accessed=us * 1_000_000)


def params(mib, **kwargs):
    return pltpu.CompilerParams(vmem_limit_bytes=mib << 20, **kwargs)


def pack_history(history, queries, slots, local_heads, group):
    h_rows = history.shape[1]
    rows = queries.shape[0]
    devices = len(slots)

    def body(h_hbm, q_hbm, *refs):
        o_refs, q_ref, sem = refs[:devices], refs[devices], refs[devices + 1]
        me = lax.axis_index("tp")
        copies = []
        for i, k in enumerate(slots):
            lane = pl.multiple_of((me ^ k) * local_heads // group * HEAD_DIM, HEAD_DIM)
            for part in range(2):
                copies.append(
                    pltpu.make_async_copy(
                        h_hbm.at[part, :, pl.ds(lane, HEAD_DIM)],
                        o_refs[i].at[part * h_rows : (part + 1) * h_rows, :],
                        sem.at[len(copies)],
                    )
                )
        for h in range(local_heads):
            copies.append(
                pltpu.make_async_copy(
                    q_hbm.at[:, h * HEAD_DIM : (h + 1) * HEAD_DIM],
                    q_ref.at[h * rows : (h + 1) * rows, :],
                    sem.at[len(copies)],
                )
            )
        for copy in copies:
            copy.start()
        for copy in copies:
            copy.wait()

    outs = pl.pallas_call(
        body,
        in_specs=[in_hbm()] * 2,
        out_specs=[in_vmem()] * (devices + 1),
        out_shape=[jax.ShapeDtypeStruct((2 * h_rows, HEAD_DIM), BF16)] * devices
        + [jax.ShapeDtypeStruct((rows * local_heads, HEAD_DIM), BF16)],
        scratch_shapes=[pltpu.SemaphoreType.DMA((2 * devices + local_heads,))],
        compiler_params=params(2),
        cost_estimate=busy(6),
        name="pack_history",
    )(to_hbm(history), to_hbm(queries))
    return dict(zip(slots, outs)), outs[devices]


def pack_fresh(prompt, history, queries, meta, slots, local_heads, group):
    h_rows, p_rows = history.shape[0] // 2, prompt.shape[1]
    p_pad = round_up(p_rows, 16)
    q_rows = queries[0].shape[0]
    every = [1] + slots
    n = len(every)

    def head_of(k):
        return lambda i, m: (0, 0, (m[0] ^ k) * local_heads // group)

    def body(m, *refs):
        p_refs, refs = refs[:n], refs[n:]
        h_ref, refs = refs[0], refs[1:]
        q_refs, o_refs = refs[: len(queries)], refs[len(queries) :]
        o_refs[0][0 : 2 * h_rows, :] = h_ref[...]
        for i in range(n):
            row = 2 * h_rows if i == 0 else 0
            for part in range(2):
                if p_pad > p_rows:
                    fresh = jnp.concatenate(
                        [p_refs[i][part].astype(F32), jnp.zeros((p_pad - p_rows, HEAD_DIM), F32)], axis=0
                    ).astype(BF16)
                else:
                    fresh = p_refs[i][part]
                o_refs[i][row + part * p_pad : row + (part + 1) * p_pad, :] = fresh
        row = 2 * (h_rows + p_pad)
        for i, q_ref in enumerate(q_refs):
            o_refs[0][row + i * q_rows : row + (i + 1) * q_rows, :] = q_ref[...]

    sizes = [2 * (h_rows + p_pad) + len(queries) * q_rows] + [2 * p_pad] * len(slots)
    outs = pl.pallas_call(
        body,
        grid_spec=pltpu.PrefetchScalarGridSpec(
            num_scalar_prefetch=1,
            grid=(1,),
            in_specs=[pl.BlockSpec((2, p_rows, HEAD_DIM), head_of(k)) for k in every]
            + [in_vmem()] * (1 + len(queries)),
            out_specs=[in_vmem()] * n,
        ),
        out_shape=[jax.ShapeDtypeStruct((size, HEAD_DIM), BF16) for size in sizes],
        compiler_params=params(8),
        cost_estimate=busy(12),
        name="pack_fresh",
    )(meta, *([prompt] * n), history, *queries)
    return outs[0], dict(zip(slots, outs[1:]))


def split(value):
    terms = []
    for _ in range(3):
        terms.append(value.astype(BF16))
        value = value - terms[-1].astype(F32)
    return terms


def decode_partials(queries, bundle, cache, prompt_queries, decode_queries, entries, meta, local_heads, group):
    devices = 2 * len(queries)
    rows, span, width = cache.shape[1], cache.shape[2], cache.shape[3]
    kv_heads = width // HEAD_DIM
    heads = devices * local_heads
    factor = HEAD_DIM ** (-0.5) * float(np.log2(np.e))
    part_rows = rows * local_heads
    stat_rows = round_up(local_heads, 8)
    prompt_rows = prompt_queries.shape[0]

    def body(m, *refs):
        q_refs, refs = refs[: devices // 2], refs[devices // 2 :]
        bundle_ref, cache_ref, pq_ref, dq_hbm, e_hbm = refs[:5]
        o_refs, refs = refs[5 : 5 + devices], refs[5 + devices :]
        q_ref, e_ref, q_all, sums, sem = refs
        me = m[0]
        lane = pl.multiple_of(me * local_heads // group * HEAD_DIM, HEAD_DIM)
        copies = [
            pltpu.make_async_copy(dq_hbm, q_ref.at[prompt_rows : prompt_rows + rows, :], sem.at[0]),
            pltpu.make_async_copy(e_hbm.at[:, :, pl.ds(lane, HEAD_DIM)], e_ref, sem.at[1]),
        ]
        for copy in copies:
            copy.start()
        q_ref[0:prompt_rows, :] = pq_ref[...]
        for k in range(devices):
            base = bundle.shape[0] - (devices // 2 - k // 2) * part_rows if k % 2 else 0
            q_ref_k = bundle_ref if k % 2 else q_refs[k // 2]
            for h in range(local_heads):
                row = base + h * rows
                q_all[k, pl.ds(h, rows, stride=local_heads), :] = q_ref_k[row : row + rows, :].astype(F32)

        slot = lax.broadcasted_iota(jnp.int32, (heads, 1), 0) // local_heads
        reads = ((slot ^ me) * local_heads) // group
        lane = lax.broadcasted_iota(jnp.int32, (heads, HEAD_DIM), 1)
        place = me * span + lax.broadcasted_iota(jnp.int32, (1, span), 1)
        scores = []
        for b in range(rows):
            here = slice(b * local_heads, (b + 1) * local_heads)
            q = jnp.concatenate([q_all[k, here, :] for k in range(devices)], axis=0)
            spread = jnp.concatenate(
                [jnp.where(reads == g, q, 0.0) for g in range(kv_heads)], axis=1
            ).astype(BF16)
            score = lax.dot_general(
                spread, cache_ref[0, b], (((1,), (1,)), ((), ())), preferred_element_type=F32
            )
            scores.append(jnp.where(place < m[2 + b], score, MASKED))
        scores = jnp.concatenate(scores, axis=0)
        top = jnp.max(scores, axis=-1, keepdims=True)
        weights = jnp.where(scores > 0.5 * MASKED, jnp.exp2((scores - top) * factor), 0.0)
        total = jnp.sum(weights, axis=-1, keepdims=True)
        weights = weights.astype(BF16)
        stats = jnp.zeros((heads, HEAD_DIM), F32)
        for b in range(rows):
            these = slice(b * heads, (b + 1) * heads)
            summed = jnp.dot(weights[these], cache_ref[1, b], preferred_element_type=F32)
            own = jnp.zeros((heads, HEAD_DIM), F32)
            for g in range(kv_heads):
                own = own + jnp.where(reads == g, summed[:, g * HEAD_DIM : (g + 1) * HEAD_DIM], 0.0)
            for k in range(devices):
                sums[k, b * local_heads : (b + 1) * local_heads, :] = own[k * local_heads : (k + 1) * local_heads]
            stats = jnp.where(lane == b, top[these], jnp.where(lane == rows + b, total[these], stats))
        terms = split(stats)
        for k in range(devices):
            o_refs[k][0:part_rows, :] = sums[k].astype(BF16)
            for i, term in enumerate(terms):
                row = part_rows + i * stat_rows
                o_refs[k][row : row + local_heads, :] = term[k * local_heads : (k + 1) * local_heads, :]
        for copy in copies:
            copy.wait()

    outs = pl.pallas_call(
        body,
        in_specs=[smem()] + [in_vmem()] * (devices // 2 + 3) + [in_hbm()] * 2,
        out_specs=[in_vmem()] * (devices + 2),
        scratch_shapes=[pltpu.VMEM((devices, part_rows, HEAD_DIM), F32)] * 2 + [pltpu.SemaphoreType.DMA((2,))],
        out_shape=[jax.ShapeDtypeStruct((part_rows + 3 * stat_rows, HEAD_DIM), BF16)] * devices
        + [
            pltpu.VMEM((prompt_rows + rows, prompt_queries.shape[1]), BF16),
            pltpu.VMEM((2, rows, HEAD_DIM), BF16),
        ],
        compiler_params=params(12),
        cost_estimate=busy(12),
        name="decode",
    )(meta, *queries, bundle, cache, prompt_queries, to_hbm(decode_queries), to_hbm(entries))
    return outs[:devices], outs[devices], outs[devices + 1]


def decode_join(parts, queries, entries, local_heads):
    devices = len(parts)
    rows = entries.shape[1]
    factor = HEAD_DIM ** (-0.5) * float(np.log2(np.e))
    part_rows = rows * local_heads
    stat_rows = round_up(local_heads, 8)

    def body(*refs):
        p_refs = refs[:devices]
        q_ref, e_ref, o_ref, q_all, out = refs[devices:]
        for h in range(local_heads):
            q_all[pl.ds(h, rows, stride=local_heads), :] = q_ref[h * rows : (h + 1) * rows, :].astype(F32)
        stats = []
        for p in p_refs:
            starts = [part_rows + i * stat_rows for i in range(3)]
            high, middle, low = [p[row : row + local_heads, :].astype(F32) for row in starts]
            stats.append(high + middle + low)
        keys, values = e_ref[0].astype(F32), e_ref[1].astype(F32)
        sums = [p[0:part_rows, :].astype(F32) for p in p_refs]
        for b in range(rows):
            here = slice(b * local_heads, (b + 1) * local_heads)
            own = jnp.sum(q_all[here, :] * keys[b : b + 1, :], axis=-1, keepdims=True)
            tops = [s[:, b : b + 1] for s in stats]
            top = own
            for t in tops:
                top = jnp.maximum(top, t)
            weight = jnp.exp2((own - top) * factor)
            total = weight
            summed = weight.astype(BF16).astype(F32) * values[b : b + 1, :]
            for s, t, p in zip(stats, tops, sums):
                share = jnp.exp2((t - top) * factor)
                total = total + share * s[:, rows + b : rows + b + 1]
                summed = summed + share * p[here, :]
            out[here, :] = summed / total
        for h in range(local_heads):
            o_ref[:, h * HEAD_DIM : (h + 1) * HEAD_DIM] = out[pl.ds(h, rows, stride=local_heads), :].astype(BF16)

    return pl.pallas_call(
        body,
        in_specs=[in_vmem()] * (devices + 2),
        out_specs=in_vmem(),
        scratch_shapes=[pltpu.VMEM((part_rows, HEAD_DIM), F32)] * 2,
        out_shape=jax.ShapeDtypeStruct((rows, local_heads * HEAD_DIM), BF16),
        compiler_params=params(4),
        cost_estimate=busy(1),
        name="join",
    )(*parts, queries, entries)


def product(att, w, start, stop, targets):
    for c in range(start, stop, COLUMNS):
        width = min(COLUMNS, stop - c)
        out = jnp.dot(att, w[:, c : c + width], preferred_element_type=F32).astype(BF16)
        row = 0
        for target in targets:
            target[:, c - start : c - start + width] = out[row : row + target.shape[0]]
            row += target.shape[0]


def project(atts, weight, start):
    model = weight.shape[1]
    n = len(atts)

    def body(*refs):
        att = jnp.concatenate([ref[...] for ref in refs[:n]], axis=0)
        product(att, refs[n], start, model, refs[n + 1 :])

    return pl.pallas_call(
        body,
        in_specs=[in_vmem()] * (n + 1),
        out_specs=[in_vmem()] * n,
        out_shape=[jax.ShapeDtypeStruct((att.shape[0], model - start), BF16) for att in atts],
        compiler_params=params(8),
        cost_estimate=busy(2),
        name="project",
    )(*atts, weight)


def attend(order, first, count, block, queries, pieces, joined, decoded, weight, meta, h_rows, p_rows, columns):
    history, fresh, bundle = pieces
    devices = len(history) + 1
    held = list(history)
    p_pad = fresh[0].shape[0] // 2
    local_width = queries.shape[1]
    local_heads = local_width // HEAD_DIM
    model = weight.shape[1]
    h_keys, p_keys = devices * h_rows, devices * p_pad
    keys = h_keys + p_keys
    shares = [sum(count for s in order if s % 2 == parity) for parity in (0, 1)]
    shares = [share for share in shares if share]
    factor = HEAD_DIM ** (-0.5) * float(np.log2(np.e))
    per = max(1, min(local_heads, GROUP_ROWS // count))
    has_decode = decoded is not None
    decode_rows = decoded.shape[0] if has_decode else 0

    def join_pieces(refs, k_all, v_all):
        n = devices - 1
        cached = {1: (refs[0], 0), **{k: (ref, 0) for k, ref in zip(held, refs[1:])}}
        own = {1: (refs[0], 2 * h_rows), **{k: (ref, 0) for k, ref in zip(held, refs[1 + n :])}}
        for k in range(devices):
            for part, dst in ((0, k_all), (1, v_all)):
                for copy in range(2 - part):
                    lanes = slice(copy * HEAD_DIM, (copy + 1) * HEAD_DIM)
                    ref, row = cached[k]
                    row += part * h_rows
                    dst[k * h_rows : (k + 1) * h_rows, lanes] = ref[row : row + h_rows, :]
                    ref, row = own[k]
                    row += part * p_pad
                    dst[h_keys + k * p_pad : h_keys + (k + 1) * p_pad, lanes] = ref[row : row + p_pad, :]
        v_all[:, HEAD_DIM:] = jnp.ones((keys, HEAD_DIM), BF16)

    def body(m, q, w, *refs):
        if has_decode:
            dec_ref, refs = refs[0], refs[1:]
        if joined is None:
            parts, refs = refs[: 2 * devices - 1], refs[2 * devices - 1 :]
            k_all, v_all = refs[-2:]
            join_pieces(parts, k_all, v_all)
            targets, att = refs[:-3], refs[-3]
        else:
            k_all, v_all = refs[:2]
            targets, att = refs[2:-1], refs[-1]
        me, valid_rows = m[0], m[1]
        column = lax.broadcasted_iota(jnp.int32, (1, h_keys), 1)
        place = ((column // h_rows) ^ me) * h_rows + column % h_rows
        history_bias = jnp.where(place < valid_rows, 0.0, MASKED)
        column = lax.broadcasted_iota(jnp.int32, (1, p_keys), 1)
        inner = column % p_pad
        seen_from = jnp.where(inner < p_rows, ((column // p_pad) ^ me) * p_rows + inner, 1 << 20)
        steps = [(i, g) for i in range(len(order)) for g in range(0, local_heads, per)]
        biases = []
        for i, slot in enumerate(order):
            rows = (slot ^ me) * block + first + lax.broadcasted_iota(jnp.int32, (count, 1), 0)
            bias = jnp.where(seen_from <= rows, 0.0, MASKED)
            biases.append(jnp.concatenate([jnp.broadcast_to(history_bias, (count, h_keys)), bias], axis=1))

        def scores_of(i, g):
            row0 = pl.multiple_of((order[i] ^ me) * block + first, 16)
            stacked = jnp.concatenate(
                [q[pl.ds(row0, count), h * HEAD_DIM : (h + 1) * HEAD_DIM] for h in range(g, g + per)], axis=0
            )
            scaled = stacked.astype(F32) * factor
            high = scaled.astype(BF16)
            low = (scaled - high.astype(F32)).astype(BF16)
            stacked = jnp.concatenate([high, low], axis=1)
            scores = lax.dot_general(
                stacked, k_all[...], (((1,), (1,)), ((), ())), preferred_element_type=F32
            )
            return (scores.reshape(per, count, keys) + biases[i][None]).reshape(per * count, keys)

        ahead = scores_of(*steps[0])
        for t, (i, g) in enumerate(steps):
            scores = ahead
            if t + 1 < len(steps):
                ahead = scores_of(*steps[t + 1])
            top = jnp.max(scores, axis=-1, keepdims=True)
            weights = jnp.exp2(scores - top)
            summed = jnp.dot(weights.astype(BF16), v_all[...], preferred_element_type=F32)
            summed = (summed[:, :HEAD_DIM] / summed[:, HEAD_DIM:]).astype(BF16)
            for h in range(per):
                att[i * count : (i + 1) * count, (g + h) * HEAD_DIM : (g + h + 1) * HEAD_DIM] = summed[
                    h * count : (h + 1) * count
                ]
        if has_decode:
            for i, slot in enumerate(order):

                @pl.when(slot ^ me == devices - 1)
                def _():
                    att[(i + 1) * count - decode_rows : (i + 1) * count, :] = dec_ref[...]

        product(att[...], w, 0, columns, targets)

    flops = 2 * len(order) * count * (2 * local_width * keys + local_width * model)
    operands = [queries, weight] + ([decoded] if has_decode else [])
    out_shape = [jax.ShapeDtypeStruct((share, columns), BF16) for share in shares]
    out_shape.append(jax.ShapeDtypeStruct((len(order) * count, local_width), BF16))
    if joined is None:
        operands += [bundle, *history.values(), *fresh.values()]
        out_shape += [jax.ShapeDtypeStruct((keys, 2 * HEAD_DIM), BF16)] * 2
    else:
        operands += joined
    outs = pl.pallas_call(
        body,
        in_specs=[smem()] + [in_vmem()] * len(operands),
        out_specs=[in_vmem()] * len(out_shape),
        out_shape=out_shape,
        compiler_params=params(24),
        cost_estimate=pl.CostEstimate(flops=flops, transcendentals=0, bytes_accessed=weight.size * 2),
    )(meta, *operands)
    n = len(shares)
    return outs[:n], outs[n], joined or list(outs[n + 1 :])


def finish(first, begin, residual, own, given, crossed, gain, previous):
    block, model = residual.shape
    count = crossed[0].shape[0]
    tile = 16
    n_cross = len(crossed)
    n_columns = 1 if crossed[0].shape[1] == model else 2

    def body(res_ref, own_ref, given_ref, *refs):
        cross = refs[:n_cross]
        gain_ref = refs[n_cross]
        outs = refs[-5:-3]
        staged, sem = refs[-3:-1], refs[-1]
        copies = []
        for i in range(0, count, tile):
            here, local = slice(first + i, first + i + tile), slice(i, i + tile)
            mine = slice(begin + i, begin + i + tile)
            hidden = res_ref[here, :].astype(F32) + own_ref[mine, :].astype(F32) + given_ref[mine, :].astype(F32)
            for c in range(0, n_cross, n_columns):
                pieces = [piece[local, :].astype(F32) for piece in cross[c : c + n_columns]]
                hidden = hidden + (jnp.concatenate(pieces, axis=1) if n_columns > 1 else pieces[0])
            mean = jnp.mean(hidden * hidden, axis=-1, keepdims=True)
            staged[0][local, :] = hidden.astype(BF16)
            staged[1][local, :] = (hidden * lax.rsqrt(mean + EPS) * gain_ref[...]).astype(BF16)
            for source, target in zip(staged, outs):
                copies.append(pltpu.make_async_copy(source.at[local, :], target.at[here, :], sem.at[len(copies)]))
                copies[-1].start()
        for copy in copies:
            copy.wait()

    n_in = 3 + n_cross + 1
    return pl.pallas_call(
        body,
        in_specs=[in_vmem()] * n_in + [hbm()] * len(previous),
        out_specs=[hbm()] * 2,
        out_shape=[jax.ShapeDtypeStruct((block, model), BF16)] * 2,
        input_output_aliases={n_in + i: i for i in range(len(previous))},
        scratch_shapes=[pltpu.VMEM((count, model), BF16)] * 2 + [pltpu.SemaphoreType.DMA((2 * count // tile,))],
        compiler_params=params(8),
        cost_estimate=busy(2),
    )(residual, own, given, *crossed, gain, *previous)


def step(
    prompt_queries,
    prompt_entries,
    history_cache,
    decode_queries,
    decode_entries,
    decode_cache,
    decode_lengths,
    prompt_start,
    out_weight,
    residual,
    norm_gain,
):
    devices = lax.axis_size("tp")
    local_heads = prompt_queries.shape[1] // HEAD_DIM
    kv_heads = history_cache.shape[2] // HEAD_DIM
    group = devices * local_heads // kv_heads
    block = residual.shape[0]
    h_rows, p_rows = history_cache.shape[1], prompt_entries.shape[1]
    assert group % local_heads == 0 and devices & (devices - 1) == 0
    assert block >= decode_queries.shape[0]

    def swap(value, k):
        return lax.ppermute(value, "tp", [(i, i ^ k) for i in range(devices)])

    def swapped(values):
        return [values[0]] + [swap(values[k], k) for k in range(1, devices)]

    slots = [0] + list(range(2, devices))
    packed, own_query = pack_history(history_cache, decode_queries, [1] + slots, local_heads, group)
    even_queries = [own_query] + [swap(own_query, k) for k in range(2, devices, 2)]
    history = {k: swap(packed[k], k) if k else packed[k] for k in slots}
    meta = jnp.concatenate([lax.axis_index("tp").astype(jnp.int32)[None], prompt_start, decode_lengths])
    bundle, packed = pack_fresh(prompt_entries, packed[1], even_queries, meta, slots, local_heads, group)
    bundle = swap(bundle, 1)
    fresh = {k: swap(packed[k], k) if k else packed[k] for k in slots}
    parts, queries, entries = decode_partials(
        even_queries, bundle, decode_cache, prompt_queries, decode_queries, decode_entries, meta, local_heads, group
    )
    parts = swapped(parts)
    decoded = decode_join(parts, own_query, entries, local_heads)

    joined = None

    def attended(order, first, count, decoded, columns):
        nonlocal joined
        outs, att, joined = attend(
            order,
            first,
            count,
            block,
            queries,
            (history, fresh, bundle),
            joined,
            decoded,
            out_weight,
            meta,
            h_rows,
            p_rows,
            columns,
        )
        return outs, att

    def chip_sum(keep, give):
        return keep.astype(F32) + swap(give, 1).astype(F32)

    def cross(pair, count, start, stop):
        return [
            swap(pair[k * count + start : k * count + stop].astype(BF16), 2 * k + 2)
            for k in range(devices // 2 - 1)
        ]

    chunks = [c * block // sum(CHUNKS) for c in CHUNKS]
    if any(c % 16 for c in chunks):
        chunks = [block]
    model = out_weight.shape[1]
    stays, leaves = list(range(2, devices, 2)), list(range(3, devices, 2))
    crossed, first = [], 0
    for count in chunks:
        last = first + count == block
        if last:
            (keep, give), _ = attended(stays + leaves, first, count, decoded, model)
            pair = chip_sum(keep, give)
            cut = count - 16 if count > 16 else 0
            for start, stop in [(0, cut), (cut, count)] if cut else [(0, count)]:
                crossed.append((first + start, cross(pair, count, start, stop)))
        else:
            columns = model // 8 * FIRST_EIGHTHS
            (give,), gone = attended(leaves, first, count, None, columns)
            (keep,), kept = attended(stays, first, count, None, columns)
            pieces = [cross(chip_sum(keep, give), count, 0, count)]
            keep, give = project([kept, gone], out_weight, columns)
            pieces.append(cross(chip_sum(keep, give), count, 0, count))
            crossed.append((first, [piece for both in zip(*pieces) for piece in both]))
        first += count
    owned, first = [], 0
    for count in chunks:
        here = decoded if first + count == block else None
        (own, give), _ = attended([0, 1], first, count, here, model)
        owned.append((first, own, swap(give, 1)))
        first += count
    gain = norm_gain[None, :]
    outs = []
    for first, pieces in crossed:
        begin, own, given = [o for o in owned if o[0] <= first][-1]
        outs = finish(first, first - begin, residual, own, given, pieces, gain, outs)
    return tuple(outs)


def solution(mesh):
    placed = (
        P("rep", "tp"),
        P("rep", "tp", None),
        P("rep", "tp", None),
        P("rep", "tp"),
        P("rep", None, None),
        P("rep", None, "tp", None),
        P("rep"),
        P("rep"),
        P("tp", None),
        P("tp", "rep"),
        P(),
    )
    return jax.shard_map(
        step,
        mesh=mesh,
        in_specs=placed,
        out_specs=(P("tp", "rep"), P("tp", "rep")),
        check_vma=False,
    )
```

```python
import jax
import jax.numpy as jnp
import numpy as np
from jax import lax
from jax.experimental import pallas as pl
from jax.experimental.pallas import tpu as pltpu
from jax.sharding import PartitionSpec as P


HEAD_DIM = 128
MASKED = -1e30
EPS = 1e-05
CHUNKS = (64, 64)
COLUMNS = 512
FIRST_EIGHTHS = 3
GROUP_ROWS = 256

F32 = jnp.float32
BF16 = jnp.bfloat16


def round_up(value, unit):
    return -(-value // unit) * unit


def hbm():
    return pl.BlockSpec(memory_space=pl.ANY)


def in_hbm():
    return pl.BlockSpec(memory_space=pltpu.HBM)


def in_vmem():
    return pl.BlockSpec(memory_space=pltpu.VMEM)


def to_hbm(value):
    return pltpu.with_memory_space_constraint(value, pltpu.HBM)


def busy(us):
    return pl.CostEstimate(flops=us * 500_000_000, transcendentals=0, bytes_accessed=us * 1_000_000)


def params(mib, **kwargs):
    return pltpu.CompilerParams(vmem_limit_bytes=mib << 20, **kwargs)


def pack_history(history, queries, entries, slots, local_heads, group):
    h_rows = history.shape[1]
    rows = queries.shape[0]
    devices = len(slots)

    def body(h_hbm, q_hbm, e_hbm, *refs):
        o_refs, (q_ref, e_ref, sem) = refs[:devices], refs[devices:]
        me = lax.axis_index("tp")
        lane = pl.multiple_of(me * local_heads // group * HEAD_DIM, HEAD_DIM)
        copies = [pltpu.make_async_copy(e_hbm.at[:, :, pl.ds(lane, HEAD_DIM)], e_ref, sem.at[0])]
        for i, k in enumerate(slots):
            lane = pl.multiple_of((me ^ k) * local_heads // group * HEAD_DIM, HEAD_DIM)
            for part in range(2):
                copies.append(
                    pltpu.make_async_copy(
                        h_hbm.at[part, :, pl.ds(lane, HEAD_DIM)],
                        o_refs[i].at[part * h_rows : (part + 1) * h_rows, :],
                        sem.at[len(copies)],
                    )
                )
        for h in range(local_heads):
            copies.append(
                pltpu.make_async_copy(
                    q_hbm.at[:, h * HEAD_DIM : (h + 1) * HEAD_DIM],
                    q_ref.at[h * rows : (h + 1) * rows, :],
                    sem.at[len(copies)],
                )
            )
        for copy in copies:
            copy.start()
        for copy in copies:
            copy.wait()

    outs = pl.pallas_call(
        body,
        in_specs=[in_hbm()] * 3,
        out_specs=[in_vmem()] * (devices + 2),
        out_shape=[jax.ShapeDtypeStruct((2 * h_rows, HEAD_DIM), BF16)] * devices
        + [
            jax.ShapeDtypeStruct((rows * local_heads, HEAD_DIM), BF16),
            pltpu.VMEM((2, rows, HEAD_DIM), BF16),
        ],
        scratch_shapes=[pltpu.SemaphoreType.DMA((1 + 2 * devices + local_heads,))],
        compiler_params=params(2),
        cost_estimate=busy(6),
        name="pack_history",
    )(to_hbm(history), to_hbm(queries), to_hbm(entries))
    return dict(zip(slots, outs)), outs[devices], outs[devices + 1]


def pack_fresh(prompt, history, query, slots, local_heads, group):
    h_rows, p_rows = history.shape[0] // 2, prompt.shape[1]
    p_pad = round_up(p_rows, 16)
    every = [1] + slots
    n = len(every)

    def body(p_ref, h_ref, q_ref, *o_refs):
        me = lax.axis_index("tp")
        o_refs[0][0 : 2 * h_rows, :] = h_ref[...]
        for i, k in enumerate(every):
            lane = pl.multiple_of((me ^ k) * local_heads // group * HEAD_DIM, HEAD_DIM)
            row = 2 * h_rows if i == 0 else 0
            for part in range(2):
                fresh = p_ref[part, :, pl.ds(lane, HEAD_DIM)]
                if p_pad > p_rows:
                    fresh = jnp.concatenate(
                        [fresh.astype(F32), jnp.zeros((p_pad - p_rows, HEAD_DIM), F32)], axis=0
                    ).astype(BF16)
                o_refs[i][row + part * p_pad : row + (part + 1) * p_pad, :] = fresh
        o_refs[0][2 * (h_rows + p_pad) :, :] = q_ref[...]

    sizes = [2 * (h_rows + p_pad) + query.shape[0]] + [2 * p_pad] * len(slots)
    outs = pl.pallas_call(
        body,
        in_specs=[in_vmem()] * 3,
        out_specs=[in_vmem()] * n,
        out_shape=[jax.ShapeDtypeStruct((size, HEAD_DIM), BF16) for size in sizes],
        compiler_params=params(8),
        cost_estimate=busy(12),
        name="pack_fresh",
    )(prompt, history, query)
    return outs[0], dict(zip(slots, outs[1:]))


def split(value):
    terms = []
    for _ in range(3):
        terms.append(value.astype(BF16))
        value = value - terms[-1].astype(F32)
    return terms


def decode_partials(queries, bundle, cache, prompt_queries, limits, local_heads, group):
    devices = len(queries) + 1
    held = list(queries)
    rows, span, width = cache.shape[1], cache.shape[2], cache.shape[3]
    kv_heads = width // HEAD_DIM
    heads = devices * local_heads
    factor = HEAD_DIM ** (-0.5) * float(np.log2(np.e))
    part_rows = rows * local_heads
    stat_rows = round_up(local_heads, 8)
    prompt_rows, local_width = prompt_queries.shape

    def body(limits_ref, *refs):
        q_refs, refs = dict(zip(held, refs)), refs[devices - 1 :]
        bundle_ref, cache_ref, pq_ref = refs[:3]
        o_refs, refs = refs[3 : 3 + devices], refs[3 + devices :]
        q_ref, q_all, sums = refs
        me = lax.axis_index("tp")
        q_ref[0:prompt_rows, :] = pq_ref[...]
        q_ref[prompt_rows:, :] = jnp.zeros((rows, local_width), BF16)
        for k in range(devices):
            q_ref_k, base = (bundle_ref, bundle.shape[0] - part_rows) if k == 1 else (q_refs[k], 0)
            for h in range(local_heads):
                row = base + h * rows
                q_all[k, pl.ds(h, rows, stride=local_heads), :] = q_ref_k[row : row + rows, :].astype(F32)

        slot = lax.broadcasted_iota(jnp.int32, (heads, 1), 0) // local_heads
        reads = ((slot ^ me) * local_heads) // group
        lane = lax.broadcasted_iota(jnp.int32, (heads, HEAD_DIM), 1)
        place = me * span + lax.broadcasted_iota(jnp.int32, (1, span), 1)
        scores = []
        for b in range(rows):
            here = slice(b * local_heads, (b + 1) * local_heads)
            q = jnp.concatenate([q_all[k, here, :] for k in range(devices)], axis=0)
            spread = jnp.concatenate(
                [jnp.where(reads == g, q, 0.0) for g in range(kv_heads)], axis=1
            ).astype(BF16)
            score = lax.dot_general(
                spread, cache_ref[0, b], (((1,), (1,)), ((), ())), preferred_element_type=F32
            )
            scores.append(jnp.where(place < limits_ref[1 + b : 2 + b, 0:1], score, MASKED))
        scores = jnp.concatenate(scores, axis=0)
        top = jnp.max(scores, axis=-1, keepdims=True)
        weights = jnp.where(scores > 0.5 * MASKED, jnp.exp2((scores - top) * factor), 0.0)
        total = jnp.sum(weights, axis=-1, keepdims=True)
        weights = weights.astype(BF16)
        stats = jnp.zeros((heads, HEAD_DIM), F32)
        for b in range(rows):
            these = slice(b * heads, (b + 1) * heads)
            summed = jnp.dot(weights[these], cache_ref[1, b], preferred_element_type=F32)
            own = jnp.zeros((heads, HEAD_DIM), F32)
            for g in range(kv_heads):
                own = own + jnp.where(reads == g, summed[:, g * HEAD_DIM : (g + 1) * HEAD_DIM], 0.0)
            for k in range(devices):
                sums[k, b * local_heads : (b + 1) * local_heads, :] = own[k * local_heads : (k + 1) * local_heads]
            stats = jnp.where(lane == b, top[these], jnp.where(lane == rows + b, total[these], stats))
        terms = split(stats)
        for k in range(devices):
            o_refs[k][0:part_rows, :] = sums[k].astype(BF16)
            for i, term in enumerate(terms):
                row = part_rows + i * stat_rows
                o_refs[k][row : row + local_heads, :] = term[k * local_heads : (k + 1) * local_heads, :]

    outs = pl.pallas_call(
        body,
        in_specs=[in_vmem()] * (devices + 3),
        out_specs=[in_vmem()] * (devices + 1),
        scratch_shapes=[pltpu.VMEM((devices, part_rows, HEAD_DIM), F32)] * 2,
        out_shape=[jax.ShapeDtypeStruct((part_rows + 3 * stat_rows, HEAD_DIM), BF16)] * devices
        + [pltpu.VMEM((prompt_rows + rows, local_width), BF16)],
        compiler_params=params(12),
        cost_estimate=busy(12),
        name="decode",
    )(limits, *queries.values(), bundle, cache, prompt_queries)
    return outs[:devices], outs[devices]


def decode_join(parts, queries, entries, local_heads):
    devices = len(parts)
    rows = entries.shape[1]
    factor = HEAD_DIM ** (-0.5) * float(np.log2(np.e))
    part_rows = rows * local_heads
    stat_rows = round_up(local_heads, 8)

    def body(*refs):
        p_refs = refs[:devices]
        q_ref, e_ref, o_ref, q_all, out = refs[devices:]
        for h in range(local_heads):
            q_all[pl.ds(h, rows, stride=local_heads), :] = q_ref[h * rows : (h + 1) * rows, :].astype(F32)
        stats = []
        for p in p_refs:
            starts = [part_rows + i * stat_rows for i in range(3)]
            high, middle, low = [p[row : row + local_heads, :].astype(F32) for row in starts]
            stats.append(high + middle + low)
        keys, values = e_ref[0].astype(F32), e_ref[1].astype(F32)
        sums = [p[0:part_rows, :].astype(F32) for p in p_refs]
        for b in range(rows):
            here = slice(b * local_heads, (b + 1) * local_heads)
            own = jnp.sum(q_all[here, :] * keys[b : b + 1, :], axis=-1, keepdims=True)
            tops = [s[:, b : b + 1] for s in stats]
            top = own
            for t in tops:
                top = jnp.maximum(top, t)
            weight = jnp.exp2((own - top) * factor)
            total = weight
            summed = weight.astype(BF16).astype(F32) * values[b : b + 1, :]
            for s, t, p in zip(stats, tops, sums):
                share = jnp.exp2((t - top) * factor)
                total = total + share * s[:, rows + b : rows + b + 1]
                summed = summed + share * p[here, :]
            out[here, :] = summed / total
        for h in range(local_heads):
            o_ref[:, h * HEAD_DIM : (h + 1) * HEAD_DIM] = out[pl.ds(h, rows, stride=local_heads), :].astype(BF16)

    return pl.pallas_call(
        body,
        in_specs=[in_vmem()] * (devices + 2),
        out_specs=in_vmem(),
        scratch_shapes=[pltpu.VMEM((part_rows, HEAD_DIM), F32)] * 2,
        out_shape=jax.ShapeDtypeStruct((rows, local_heads * HEAD_DIM), BF16),
        compiler_params=params(4),
        cost_estimate=busy(1),
        name="join",
    )(*parts, queries, entries)


def product(att, w, start, stop, targets):
    for c in range(start, stop, COLUMNS):
        width = min(COLUMNS, stop - c)
        out = jnp.dot(att, w[:, c : c + width], preferred_element_type=F32).astype(BF16)
        row = 0
        for target in targets:
            target[:, c - start : c - start + width] = out[row : row + target.shape[0]]
            row += target.shape[0]


def project(atts, weight, start):
    model = weight.shape[1]
    n = len(atts)

    def body(*refs):
        att = jnp.concatenate([ref[...] for ref in refs[:n]], axis=0)
        product(att, refs[n], start, model, refs[n + 1 :])

    return pl.pallas_call(
        body,
        in_specs=[in_vmem()] * (n + 1),
        out_specs=[in_vmem()] * n,
        out_shape=[jax.ShapeDtypeStruct((att.shape[0], model - start), BF16) for att in atts],
        compiler_params=params(8),
        cost_estimate=busy(2),
        name="project",
    )(*atts, weight)


def attend(order, first, count, block, queries, pieces, joined, decoded, weight, limits, h_rows, p_rows, columns, emit):
    history, fresh, bundle = pieces
    devices = len(history) + 1
    held = list(history)
    p_pad = fresh[0].shape[0] // 2
    local_width = queries.shape[1]
    local_heads = local_width // HEAD_DIM
    model = weight.shape[1]
    h_keys, p_keys = devices * h_rows, devices * p_pad
    keys = h_keys + p_keys
    pieces_given = joined is None
    shares = [sum(count for s in order if s % 2 == parity) for parity in (0, 1)]
    shares = [share for share in shares if share]
    factor = HEAD_DIM ** (-0.5) * float(np.log2(np.e))
    per = max(1, min(local_heads, GROUP_ROWS // count))
    has_decode = decoded is not None
    decode_rows = decoded.shape[0] if has_decode else 0

    def join_pieces(refs, k_all, v_all):
        n = devices - 1
        cached = {1: (refs[0], 0), **{k: (ref, 0) for k, ref in zip(held, refs[1:])}}
        own = {1: (refs[0], 2 * h_rows), **{k: (ref, 0) for k, ref in zip(held, refs[1 + n :])}}
        for k in range(devices):
            for part, dst in ((0, k_all), (1, v_all)):
                for copy in range(2 - part):
                    lanes = slice(copy * HEAD_DIM, (copy + 1) * HEAD_DIM)
                    ref, row = cached[k]
                    row += part * h_rows
                    dst[k * h_rows : (k + 1) * h_rows, lanes] = ref[row : row + h_rows, :]
                    ref, row = own[k]
                    row += part * p_pad
                    dst[h_keys + k * p_pad : h_keys + (k + 1) * p_pad, lanes] = ref[row : row + p_pad, :]
        v_all[:, HEAD_DIM:] = jnp.ones((keys, HEAD_DIM), BF16)

    def body(limits_ref, q, w, *refs):
        if has_decode:
            dec_ref, refs = refs[0], refs[1:]
        if pieces_given:
            parts, refs = refs[: 2 * devices - 1], refs[2 * devices - 1 :]
            k_all, v_all, refs = refs[0], refs[1], refs[2:]
            join_pieces(parts, k_all, v_all)
        else:
            k_all, v_all, refs = refs[0], refs[1], refs[2:]
        targets, att = refs[:-1], refs[-1]
        me = lax.axis_index("tp")
        column = lax.broadcasted_iota(jnp.int32, (1, h_keys), 1)
        place = ((column // h_rows) ^ me) * h_rows + column % h_rows
        history_bias = jnp.where(place < limits_ref[0:1, 0:1], 0.0, MASKED)
        column = lax.broadcasted_iota(jnp.int32, (1, p_keys), 1)
        inner = column % p_pad
        seen_from = jnp.where(inner < p_rows, ((column // p_pad) ^ me) * p_rows + inner, 1 << 20)
        steps = [(i, g) for i in range(len(order)) for g in range(0, local_heads, per)]
        biases = []
        for i, slot in enumerate(order):
            rows = (slot ^ me) * block + first + lax.broadcasted_iota(jnp.int32, (count, 1), 0)
            bias = jnp.where(seen_from <= rows, 0.0, MASKED)
            biases.append(jnp.concatenate([jnp.broadcast_to(history_bias, (count, h_keys)), bias], axis=1))

        def scores_of(i, g):
            row0 = pl.multiple_of((order[i] ^ me) * block + first, 16)
            stacked = jnp.concatenate(
                [q[pl.ds(row0, count), h * HEAD_DIM : (h + 1) * HEAD_DIM] for h in range(g, g + per)], axis=0
            )
            scaled = stacked.astype(F32) * factor
            high = scaled.astype(BF16)
            low = (scaled - high.astype(F32)).astype(BF16)
            stacked = jnp.concatenate([high, low], axis=1)
            scores = lax.dot_general(
                stacked, k_all[...], (((1,), (1,)), ((), ())), preferred_element_type=F32
            )
            return (scores.reshape(per, count, keys) + biases[i][None]).reshape(per * count, keys)

        ahead = scores_of(*steps[0])
        for t, (i, g) in enumerate(steps):
            scores = ahead
            if t + 1 < len(steps):
                ahead = scores_of(*steps[t + 1])
            top = jnp.max(scores, axis=-1, keepdims=True)
            weights = jnp.exp2(scores - top)
            summed = jnp.dot(weights.astype(BF16), v_all[...], preferred_element_type=F32)
            summed = (summed[:, :HEAD_DIM] / summed[:, HEAD_DIM:]).astype(BF16)
            for h in range(per):
                att[i * count : (i + 1) * count, (g + h) * HEAD_DIM : (g + h + 1) * HEAD_DIM] = summed[
                    h * count : (h + 1) * count
                ]
        if has_decode:
            for i, slot in enumerate(order):

                @pl.when(slot ^ me == devices - 1)
                def _():
                    att[(i + 1) * count - decode_rows : (i + 1) * count, :] = dec_ref[...]

        product(att[...], w, 0, columns, targets)

    flops = 2 * len(order) * count * (2 * local_width * keys + local_width * model)
    operands = [limits, queries, weight] + ([decoded] if has_decode else [])
    out_shape = [jax.ShapeDtypeStruct((share, columns), BF16) for share in shares]
    if pieces_given:
        operands += [bundle, *history.values(), *fresh.values()]
        out_shape = [jax.ShapeDtypeStruct((keys, 2 * HEAD_DIM), BF16)] * 2 + out_shape
    else:
        operands += joined
    attended = (len(order) * count, local_width)
    if emit:
        out_shape.append(jax.ShapeDtypeStruct(attended, BF16))
    outs = pl.pallas_call(
        body,
        in_specs=[in_vmem()] * len(operands),
        out_specs=[in_vmem()] * len(out_shape),
        out_shape=out_shape,
        scratch_shapes=[] if emit else [pltpu.VMEM(attended, BF16)],
        compiler_params=params(24),
        cost_estimate=pl.CostEstimate(flops=flops, transcendentals=0, bytes_accessed=weight.size * 2),
    )(*operands)
    if pieces_given:
        joined, outs = list(outs[:2]), outs[2:]
    return outs, joined


def finish(first, begin, residual, own, given, crossed, gain, previous):
    block, model = residual.shape
    count = crossed[0].shape[0]
    tile = 16
    n_cross = len(crossed)
    n_columns = 1 if crossed[0].shape[1] == model else 2

    def body(res_ref, own_ref, given_ref, *refs):
        cross = refs[:n_cross]
        gain_ref = refs[n_cross]
        outs = refs[-5:-3]
        staged, sem = refs[-3:-1], refs[-1]
        copies = []
        for i in range(0, count, tile):
            here, local = slice(first + i, first + i + tile), slice(i, i + tile)
            mine = slice(begin + i, begin + i + tile)
            hidden = res_ref[here, :].astype(F32) + own_ref[mine, :].astype(F32) + given_ref[mine, :].astype(F32)
            for c in range(0, n_cross, n_columns):
                pieces = [piece[local, :].astype(F32) for piece in cross[c : c + n_columns]]
                hidden = hidden + (jnp.concatenate(pieces, axis=1) if n_columns > 1 else pieces[0])
            mean = jnp.mean(hidden * hidden, axis=-1, keepdims=True)
            staged[0][local, :] = hidden.astype(BF16)
            staged[1][local, :] = (hidden * lax.rsqrt(mean + EPS) * gain_ref[...]).astype(BF16)
            for source, target in zip(staged, outs):
                copies.append(pltpu.make_async_copy(source.at[local, :], target.at[here, :], sem.at[len(copies)]))
                copies[-1].start()
        for copy in copies:
            copy.wait()

    n_in = 3 + n_cross + 1
    return pl.pallas_call(
        body,
        in_specs=[in_vmem()] * n_in + [hbm()] * len(previous),
        out_specs=[hbm()] * 2,
        out_shape=[jax.ShapeDtypeStruct((block, model), BF16)] * 2,
        input_output_aliases={n_in + i: i for i in range(len(previous))},
        scratch_shapes=[pltpu.VMEM((count, model), BF16)] * 2 + [pltpu.SemaphoreType.DMA((2 * count // tile,))],
        compiler_params=params(8),
        cost_estimate=busy(2),
    )(residual, own, given, *crossed, gain, *previous)


def step(
    prompt_queries,
    prompt_entries,
    history_cache,
    decode_queries,
    decode_entries,
    decode_cache,
    decode_lengths,
    prompt_start,
    out_weight,
    residual,
    norm_gain,
):
    devices = lax.axis_size("tp")
    local_heads = prompt_queries.shape[1] // HEAD_DIM
    kv_heads = history_cache.shape[2] // HEAD_DIM
    group = devices * local_heads // kv_heads
    block = residual.shape[0]
    h_rows, p_rows = history_cache.shape[1], prompt_entries.shape[1]
    assert group % local_heads == 0 and devices & (devices - 1) == 0
    assert block >= decode_queries.shape[0]

    def swap(value, k):
        return lax.ppermute(value, "tp", [(i, i ^ k) for i in range(devices)])

    def swapped(values):
        return [values[0]] + [swap(values[k], k) for k in range(1, devices)]

    slots = [0] + list(range(2, devices))
    packed, own_query, entries = pack_history(
        history_cache, decode_queries, decode_entries, [1] + slots, local_heads, group
    )
    rows_of = {0: own_query}
    for k in range(2, devices, 2):
        rows_of[k] = swap(own_query, k)
        rows_of[k + 1] = swap(rows_of[k], 1)
    history = {k: swap(packed[k], k) if k else packed[k] for k in slots}
    limits = jnp.concatenate([prompt_start, decode_lengths])
    limits = jnp.broadcast_to(limits[:, None], (limits.shape[0], HEAD_DIM))
    bundle, packed = pack_fresh(prompt_entries, packed[1], own_query, slots, local_heads, group)
    bundle = swap(bundle, 1)
    fresh = {k: swap(packed[k], k) if k else packed[k] for k in slots}
    parts, queries = decode_partials(rows_of, bundle, decode_cache, prompt_queries, limits, local_heads, group)
    parts = swapped(parts)
    decoded = decode_join(parts, own_query, entries, local_heads)

    joined = None

    def attended(order, first, count, decoded, columns, emit=False):
        nonlocal joined
        outs, joined = attend(
            order,
            first,
            count,
            block,
            queries,
            (history, fresh, bundle),
            joined,
            decoded,
            out_weight,
            limits,
            h_rows,
            p_rows,
            columns,
            emit,
        )
        return outs

    def chip_sum(keep, give):
        return keep.astype(F32) + swap(give, 1).astype(F32)

    def cross(pair, count, start, stop):
        return [
            swap(pair[k * count + start : k * count + stop].astype(BF16), 2 * k + 2)
            for k in range(devices // 2 - 1)
        ]

    chunks = [c * block // sum(CHUNKS) for c in CHUNKS]
    if any(c % 16 for c in chunks):
        chunks = [block]
    model = out_weight.shape[1]
    stays, leaves = list(range(2, devices, 2)), list(range(3, devices, 2))
    crossed, first = [], 0
    for count in chunks:
        last = first + count == block
        if last:
            keep, give = attended(stays + leaves, first, count, decoded, model)
            pair = chip_sum(keep, give)
            cut = count - 16 if count > 16 else 0
            for start, stop in [(0, cut), (cut, count)] if cut else [(0, count)]:
                crossed.append((first + start, cross(pair, count, start, stop)))
        else:
            columns = model // 8 * FIRST_EIGHTHS
            give, gone = attended(leaves, first, count, None, columns, emit=True)
            keep, kept = attended(stays, first, count, None, columns, emit=True)
            pieces = [cross(chip_sum(keep, give), count, 0, count)]
            keep, give = project([kept, gone], out_weight, columns)
            pieces.append(cross(chip_sum(keep, give), count, 0, count))
            crossed.append((first, [piece for both in zip(*pieces) for piece in both]))
        first += count
    owned, first = [], 0
    for count in chunks:
        here = decoded if first + count == block else None
        own, give = attended([0, 1], first, count, here, model)
        owned.append((first, own, swap(give, 1)))
        first += count
    gain = norm_gain[None, :]
    outs = []
    for first, pieces in crossed:
        begin, own, given = [o for o in owned if o[0] <= first][-1]
        outs = finish(first, first - begin, residual, own, given, pieces, gain, outs)
    return tuple(outs)


def solution(mesh):
    placed = (
        P("rep", "tp"),
        P("rep", "tp", None),
        P("rep", "tp", None),
        P("rep", "tp"),
        P("rep", None, None),
        P("rep", None, "tp", None),
        P("rep"),
        P("rep"),
        P("tp", None),
        P("tp", "rep"),
        P(),
    )
    return jax.shard_map(
        step,
        mesh=mesh,
        in_specs=placed,
        out_specs=(P("tp", "rep"), P("tp", "rep")),
        check_vma=False,
    )
```

```python
import jax
import jax.numpy as jnp
import numpy as np
from jax import lax
from jax.experimental import pallas as pl
from jax.experimental.pallas import tpu as pltpu
from jax.sharding import PartitionSpec as P


HEAD_DIM = 128
MASKED = -1e30
EPS = 1e-05
CHUNKS = (64, 64)
COLUMNS = 512
FIRST_EIGHTHS = 3
GROUP_ROWS = 256

F32 = jnp.float32
BF16 = jnp.bfloat16


def round_up(value, unit):
    return -(-value // unit) * unit


def hbm():
    return pl.BlockSpec(memory_space=pl.ANY)


def in_hbm():
    return pl.BlockSpec(memory_space=pltpu.HBM)


def in_vmem():
    return pl.BlockSpec(memory_space=pltpu.VMEM)


def to_hbm(value):
    return pltpu.with_memory_space_constraint(value, pltpu.HBM)


def busy(us):
    return pl.CostEstimate(flops=us * 500_000_000, transcendentals=0, bytes_accessed=us * 1_000_000)


def params(mib, **kwargs):
    return pltpu.CompilerParams(vmem_limit_bytes=mib << 20, **kwargs)


def pack_history(history, queries, entries, slots, local_heads, group):
    h_rows = history.shape[1]
    rows = queries.shape[0]
    devices = len(slots)

    def body(h_hbm, q_hbm, e_hbm, *refs):
        o_refs, (q_ref, e_ref, sem) = refs[:devices], refs[devices:]
        me = lax.axis_index("tp")
        lane = pl.multiple_of(me * local_heads // group * HEAD_DIM, HEAD_DIM)
        copies = [pltpu.make_async_copy(e_hbm.at[:, :, pl.ds(lane, HEAD_DIM)], e_ref, sem.at[0])]
        for i, k in enumerate(slots):
            lane = pl.multiple_of((me ^ k) * local_heads // group * HEAD_DIM, HEAD_DIM)
            for part in range(2):
                copies.append(
                    pltpu.make_async_copy(
                        h_hbm.at[part, :, pl.ds(lane, HEAD_DIM)],
                        o_refs[i].at[part * h_rows : (part + 1) * h_rows, :],
                        sem.at[len(copies)],
                    )
                )
        for h in range(local_heads):
            copies.append(
                pltpu.make_async_copy(
                    q_hbm.at[:, h * HEAD_DIM : (h + 1) * HEAD_DIM],
                    q_ref.at[h * rows : (h + 1) * rows, :],
                    sem.at[len(copies)],
                )
            )
        for copy in copies:
            copy.start()
        for copy in copies:
            copy.wait()

    outs = pl.pallas_call(
        body,
        in_specs=[in_hbm()] * 3,
        out_specs=[in_vmem()] * (devices + 2),
        out_shape=[jax.ShapeDtypeStruct((2 * h_rows, HEAD_DIM), BF16)] * devices
        + [
            jax.ShapeDtypeStruct((rows * local_heads, HEAD_DIM), BF16),
            pltpu.VMEM((2, rows, HEAD_DIM), BF16),
        ],
        scratch_shapes=[pltpu.SemaphoreType.DMA((1 + 2 * devices + local_heads,))],
        compiler_params=params(2),
        cost_estimate=busy(6),
        name="pack_history",
    )(to_hbm(history), to_hbm(queries), to_hbm(entries))
    return dict(zip(slots, outs)), outs[devices], outs[devices + 1]


def pack_fresh(prompt, history, queries, slots, local_heads, group):
    h_rows, p_rows = history.shape[0] // 2, prompt.shape[1]
    p_pad = round_up(p_rows, 16)
    q_rows = queries[0].shape[0]
    every = [1] + slots
    n = len(every)

    def body(p_ref, h_ref, *refs):
        q_refs, o_refs = refs[: len(queries)], refs[len(queries) :]
        me = lax.axis_index("tp")
        o_refs[0][0 : 2 * h_rows, :] = h_ref[...]
        for i, k in enumerate(every):
            lane = pl.multiple_of((me ^ k) * local_heads // group * HEAD_DIM, HEAD_DIM)
            row = 2 * h_rows if i == 0 else 0
            for part in range(2):
                fresh = p_ref[part, :, pl.ds(lane, HEAD_DIM)]
                if p_pad > p_rows:
                    fresh = jnp.concatenate(
                        [fresh.astype(F32), jnp.zeros((p_pad - p_rows, HEAD_DIM), F32)], axis=0
                    ).astype(BF16)
                o_refs[i][row + part * p_pad : row + (part + 1) * p_pad, :] = fresh
        row = 2 * (h_rows + p_pad)
        for i, q_ref in enumerate(q_refs):
            o_refs[0][row + i * q_rows : row + (i + 1) * q_rows, :] = q_ref[...]

    sizes = [2 * (h_rows + p_pad) + len(queries) * q_rows] + [2 * p_pad] * len(slots)
    outs = pl.pallas_call(
        body,
        in_specs=[in_vmem()] * (2 + len(queries)),
        out_specs=[in_vmem()] * n,
        out_shape=[jax.ShapeDtypeStruct((size, HEAD_DIM), BF16) for size in sizes],
        compiler_params=params(8),
        cost_estimate=busy(12),
        name="pack_fresh",
    )(prompt, history, *queries)
    return outs[0], dict(zip(slots, outs[1:]))


def split(value):
    terms = []
    for _ in range(3):
        terms.append(value.astype(BF16))
        value = value - terms[-1].astype(F32)
    return terms


def decode_partials(queries, bundle, cache, prompt_queries, limits, local_heads, group):
    devices = 2 * len(queries)
    rows, span, width = cache.shape[1], cache.shape[2], cache.shape[3]
    kv_heads = width // HEAD_DIM
    heads = devices * local_heads
    factor = HEAD_DIM ** (-0.5) * float(np.log2(np.e))
    part_rows = rows * local_heads
    stat_rows = round_up(local_heads, 8)
    prompt_rows, local_width = prompt_queries.shape

    def body(limits_ref, *refs):
        q_refs, refs = refs[: devices // 2], refs[devices // 2 :]
        bundle_ref, cache_ref, pq_ref = refs[:3]
        o_refs, refs = refs[3 : 3 + devices], refs[3 + devices :]
        q_ref, q_all, sums = refs
        me = lax.axis_index("tp")
        q_ref[0:prompt_rows, :] = pq_ref[...]
        q_ref[prompt_rows:, :] = jnp.zeros((rows, local_width), BF16)
        for k in range(devices):
            base = bundle.shape[0] - (devices // 2 - k // 2) * part_rows if k % 2 else 0
            q_ref_k = bundle_ref if k % 2 else q_refs[k // 2]
            for h in range(local_heads):
                row = base + h * rows
                q_all[k, pl.ds(h, rows, stride=local_heads), :] = q_ref_k[row : row + rows, :].astype(F32)

        slot = lax.broadcasted_iota(jnp.int32, (heads, 1), 0) // local_heads
        reads = ((slot ^ me) * local_heads) // group
        lane = lax.broadcasted_iota(jnp.int32, (heads, HEAD_DIM), 1)
        place = me * span + lax.broadcasted_iota(jnp.int32, (1, span), 1)
        scores = []
        for b in range(rows):
            here = slice(b * local_heads, (b + 1) * local_heads)
            q = jnp.concatenate([q_all[k, here, :] for k in range(devices)], axis=0)
            spread = jnp.concatenate(
                [jnp.where(reads == g, q, 0.0) for g in range(kv_heads)], axis=1
            ).astype(BF16)
            score = lax.dot_general(
                spread, cache_ref[0, b], (((1,), (1,)), ((), ())), preferred_element_type=F32
            )
            scores.append(jnp.where(place < limits_ref[1 + b : 2 + b, 0:1], score, MASKED))
        scores = jnp.concatenate(scores, axis=0)
        top = jnp.max(scores, axis=-1, keepdims=True)
        weights = jnp.where(scores > 0.5 * MASKED, jnp.exp2((scores - top) * factor), 0.0)
        total = jnp.sum(weights, axis=-1, keepdims=True)
        weights = weights.astype(BF16)
        stats = jnp.zeros((heads, HEAD_DIM), F32)
        for b in range(rows):
            these = slice(b * heads, (b + 1) * heads)
            summed = jnp.dot(weights[these], cache_ref[1, b], preferred_element_type=F32)
            own = jnp.zeros((heads, HEAD_DIM), F32)
            for g in range(kv_heads):
                own = own + jnp.where(reads == g, summed[:, g * HEAD_DIM : (g + 1) * HEAD_DIM], 0.0)
            for k in range(devices):
                sums[k, b * local_heads : (b + 1) * local_heads, :] = own[k * local_heads : (k + 1) * local_heads]
            stats = jnp.where(lane == b, top[these], jnp.where(lane == rows + b, total[these], stats))
        terms = split(stats)
        for k in range(devices):
            o_refs[k][0:part_rows, :] = sums[k].astype(BF16)
            for i, term in enumerate(terms):
                row = part_rows + i * stat_rows
                o_refs[k][row : row + local_heads, :] = term[k * local_heads : (k + 1) * local_heads, :]

    outs = pl.pallas_call(
        body,
        in_specs=[in_vmem()] * (devices // 2 + 4),
        out_specs=[in_vmem()] * (devices + 1),
        scratch_shapes=[pltpu.VMEM((devices, part_rows, HEAD_DIM), F32)] * 2,
        out_shape=[jax.ShapeDtypeStruct((part_rows + 3 * stat_rows, HEAD_DIM), BF16)] * devices
        + [pltpu.VMEM((prompt_rows + rows, local_width), BF16)],
        compiler_params=params(12),
        cost_estimate=busy(12),
        name="decode",
    )(limits, *queries, bundle, cache, prompt_queries)
    return outs[:devices], outs[devices]


def decode_join(parts, queries, entries, local_heads):
    devices = len(parts)
    rows = entries.shape[1]
    factor = HEAD_DIM ** (-0.5) * float(np.log2(np.e))
    part_rows = rows * local_heads
    stat_rows = round_up(local_heads, 8)

    def body(*refs):
        p_refs = refs[:devices]
        q_ref, e_ref, o_ref, q_all, out = refs[devices:]
        for h in range(local_heads):
            q_all[pl.ds(h, rows, stride=local_heads), :] = q_ref[h * rows : (h + 1) * rows, :].astype(F32)
        stats = []
        for p in p_refs:
            starts = [part_rows + i * stat_rows for i in range(3)]
            high, middle, low = [p[row : row + local_heads, :].astype(F32) for row in starts]
            stats.append(high + middle + low)
        keys, values = e_ref[0].astype(F32), e_ref[1].astype(F32)
        sums = [p[0:part_rows, :].astype(F32) for p in p_refs]
        for b in range(rows):
            here = slice(b * local_heads, (b + 1) * local_heads)
            own = jnp.sum(q_all[here, :] * keys[b : b + 1, :], axis=-1, keepdims=True)
            tops = [s[:, b : b + 1] for s in stats]
            top = own
            for t in tops:
                top = jnp.maximum(top, t)
            weight = jnp.exp2((own - top) * factor)
            total = weight
            summed = weight.astype(BF16).astype(F32) * values[b : b + 1, :]
            for s, t, p in zip(stats, tops, sums):
                share = jnp.exp2((t - top) * factor)
                total = total + share * s[:, rows + b : rows + b + 1]
                summed = summed + share * p[here, :]
            out[here, :] = summed / total
        for h in range(local_heads):
            o_ref[:, h * HEAD_DIM : (h + 1) * HEAD_DIM] = out[pl.ds(h, rows, stride=local_heads), :].astype(BF16)

    return pl.pallas_call(
        body,
        in_specs=[in_vmem()] * (devices + 2),
        out_specs=in_vmem(),
        scratch_shapes=[pltpu.VMEM((part_rows, HEAD_DIM), F32)] * 2,
        out_shape=jax.ShapeDtypeStruct((rows, local_heads * HEAD_DIM), BF16),
        compiler_params=params(4),
        cost_estimate=busy(1),
        name="join",
    )(*parts, queries, entries)


def product(att, w, start, stop, targets):
    for c in range(start, stop, COLUMNS):
        width = min(COLUMNS, stop - c)
        out = jnp.dot(att, w[:, c : c + width], preferred_element_type=F32).astype(BF16)
        row = 0
        for target in targets:
            target[:, c - start : c - start + width] = out[row : row + target.shape[0]]
            row += target.shape[0]


def project(atts, weight, start):
    model = weight.shape[1]
    n = len(atts)

    def body(*refs):
        att = jnp.concatenate([ref[...] for ref in refs[:n]], axis=0)
        product(att, refs[n], start, model, refs[n + 1 :])

    return pl.pallas_call(
        body,
        in_specs=[in_vmem()] * (n + 1),
        out_specs=[in_vmem()] * n,
        out_shape=[jax.ShapeDtypeStruct((att.shape[0], model - start), BF16) for att in atts],
        compiler_params=params(8),
        cost_estimate=busy(2),
        name="project",
    )(*atts, weight)


def attend(order, first, count, block, queries, pieces, joined, decoded, weight, limits, h_rows, p_rows, columns, emit):
    history, fresh, bundle = pieces
    devices = len(history) + 1
    held = list(history)
    p_pad = fresh[0].shape[0] // 2
    local_width = queries.shape[1]
    local_heads = local_width // HEAD_DIM
    model = weight.shape[1]
    h_keys, p_keys = devices * h_rows, devices * p_pad
    keys = h_keys + p_keys
    pieces_given = joined is None
    shares = [sum(count for s in order if s % 2 == parity) for parity in (0, 1)]
    shares = [share for share in shares if share]
    factor = HEAD_DIM ** (-0.5) * float(np.log2(np.e))
    per = max(1, min(local_heads, GROUP_ROWS // count))
    has_decode = decoded is not None
    decode_rows = decoded.shape[0] if has_decode else 0

    def join_pieces(refs, k_all, v_all):
        n = devices - 1
        cached = {1: (refs[0], 0), **{k: (ref, 0) for k, ref in zip(held, refs[1:])}}
        own = {1: (refs[0], 2 * h_rows), **{k: (ref, 0) for k, ref in zip(held, refs[1 + n :])}}
        for k in range(devices):
            for part, dst in ((0, k_all), (1, v_all)):
                for copy in range(2 - part):
                    lanes = slice(copy * HEAD_DIM, (copy + 1) * HEAD_DIM)
                    ref, row = cached[k]
                    row += part * h_rows
                    dst[k * h_rows : (k + 1) * h_rows, lanes] = ref[row : row + h_rows, :]
                    ref, row = own[k]
                    row += part * p_pad
                    dst[h_keys + k * p_pad : h_keys + (k + 1) * p_pad, lanes] = ref[row : row + p_pad, :]
        v_all[:, HEAD_DIM:] = jnp.ones((keys, HEAD_DIM), BF16)

    def body(limits_ref, q, w, *refs):
        if has_decode:
            dec_ref, refs = refs[0], refs[1:]
        if pieces_given:
            parts, refs = refs[: 2 * devices - 1], refs[2 * devices - 1 :]
            k_all, v_all, refs = refs[0], refs[1], refs[2:]
            join_pieces(parts, k_all, v_all)
        else:
            k_all, v_all, refs = refs[0], refs[1], refs[2:]
        targets, att = refs[:-1], refs[-1]
        me = lax.axis_index("tp")
        column = lax.broadcasted_iota(jnp.int32, (1, h_keys), 1)
        place = ((column // h_rows) ^ me) * h_rows + column % h_rows
        history_bias = jnp.where(place < limits_ref[0:1, 0:1], 0.0, MASKED)
        column = lax.broadcasted_iota(jnp.int32, (1, p_keys), 1)
        inner = column % p_pad
        seen_from = jnp.where(inner < p_rows, ((column // p_pad) ^ me) * p_rows + inner, 1 << 20)
        steps = [(i, g) for i in range(len(order)) for g in range(0, local_heads, per)]
        biases = []
        for i, slot in enumerate(order):
            rows = (slot ^ me) * block + first + lax.broadcasted_iota(jnp.int32, (count, 1), 0)
            bias = jnp.where(seen_from <= rows, 0.0, MASKED)
            biases.append(jnp.concatenate([jnp.broadcast_to(history_bias, (count, h_keys)), bias], axis=1))

        def scores_of(i, g):
            row0 = pl.multiple_of((order[i] ^ me) * block + first, 16)
            stacked = jnp.concatenate(
                [q[pl.ds(row0, count), h * HEAD_DIM : (h + 1) * HEAD_DIM] for h in range(g, g + per)], axis=0
            )
            scaled = stacked.astype(F32) * factor
            high = scaled.astype(BF16)
            low = (scaled - high.astype(F32)).astype(BF16)
            stacked = jnp.concatenate([high, low], axis=1)
            scores = lax.dot_general(
                stacked, k_all[...], (((1,), (1,)), ((), ())), preferred_element_type=F32
            )
            return (scores.reshape(per, count, keys) + biases[i][None]).reshape(per * count, keys)

        ahead = scores_of(*steps[0])
        for t, (i, g) in enumerate(steps):
            scores = ahead
            if t + 1 < len(steps):
                ahead = scores_of(*steps[t + 1])
            top = jnp.max(scores, axis=-1, keepdims=True)
            weights = jnp.exp2(scores - top)
            summed = jnp.dot(weights.astype(BF16), v_all[...], preferred_element_type=F32)
            summed = (summed[:, :HEAD_DIM] / summed[:, HEAD_DIM:]).astype(BF16)
            for h in range(per):
                att[i * count : (i + 1) * count, (g + h) * HEAD_DIM : (g + h + 1) * HEAD_DIM] = summed[
                    h * count : (h + 1) * count
                ]
        if has_decode:
            for i, slot in enumerate(order):

                @pl.when(slot ^ me == devices - 1)
                def _():
                    att[(i + 1) * count - decode_rows : (i + 1) * count, :] = dec_ref[...]

        product(att[...], w, 0, columns, targets)

    flops = 2 * len(order) * count * (2 * local_width * keys + local_width * model)
    operands = [limits, queries, weight] + ([decoded] if has_decode else [])
    out_shape = [jax.ShapeDtypeStruct((share, columns), BF16) for share in shares]
    if pieces_given:
        operands += [bundle, *history.values(), *fresh.values()]
        out_shape = [jax.ShapeDtypeStruct((keys, 2 * HEAD_DIM), BF16)] * 2 + out_shape
    else:
        operands += joined
    attended = (len(order) * count, local_width)
    if emit:
        out_shape.append(jax.ShapeDtypeStruct(attended, BF16))
    outs = pl.pallas_call(
        body,
        in_specs=[in_vmem()] * len(operands),
        out_specs=[in_vmem()] * len(out_shape),
        out_shape=out_shape,
        scratch_shapes=[] if emit else [pltpu.VMEM(attended, BF16)],
        compiler_params=params(24),
        cost_estimate=pl.CostEstimate(flops=flops, transcendentals=0, bytes_accessed=weight.size * 2),
    )(*operands)
    if pieces_given:
        joined, outs = list(outs[:2]), outs[2:]
    return outs, joined


def finish(first, begin, residual, own, given, crossed, gain, previous):
    block, model = residual.shape
    count = crossed[0].shape[0]
    tile = 16
    n_cross = len(crossed)
    n_columns = 1 if crossed[0].shape[1] == model else 2

    def body(res_ref, own_ref, given_ref, *refs):
        cross = refs[:n_cross]
        gain_ref = refs[n_cross]
        outs = refs[-5:-3]
        staged, sem = refs[-3:-1], refs[-1]
        copies = []
        for i in range(0, count, tile):
            here, local = slice(first + i, first + i + tile), slice(i, i + tile)
            mine = slice(begin + i, begin + i + tile)
            hidden = res_ref[here, :].astype(F32) + own_ref[mine, :].astype(F32) + given_ref[mine, :].astype(F32)
            for c in range(0, n_cross, n_columns):
                pieces = [piece[local, :].astype(F32) for piece in cross[c : c + n_columns]]
                hidden = hidden + (jnp.concatenate(pieces, axis=1) if n_columns > 1 else pieces[0])
            mean = jnp.mean(hidden * hidden, axis=-1, keepdims=True)
            staged[0][local, :] = hidden.astype(BF16)
            staged[1][local, :] = (hidden * lax.rsqrt(mean + EPS) * gain_ref[...]).astype(BF16)
            for source, target in zip(staged, outs):
                copies.append(pltpu.make_async_copy(source.at[local, :], target.at[here, :], sem.at[len(copies)]))
                copies[-1].start()
        for copy in copies:
            copy.wait()

    n_in = 3 + n_cross + 1
    return pl.pallas_call(
        body,
        in_specs=[in_vmem()] * n_in + [hbm()] * len(previous),
        out_specs=[hbm()] * 2,
        out_shape=[jax.ShapeDtypeStruct((block, model), BF16)] * 2,
        input_output_aliases={n_in + i: i for i in range(len(previous))},
        scratch_shapes=[pltpu.VMEM((count, model), BF16)] * 2 + [pltpu.SemaphoreType.DMA((2 * count // tile,))],
        compiler_params=params(8),
        cost_estimate=busy(2),
    )(residual, own, given, *crossed, gain, *previous)


def step(
    prompt_queries,
    prompt_entries,
    history_cache,
    decode_queries,
    decode_entries,
    decode_cache,
    decode_lengths,
    prompt_start,
    out_weight,
    residual,
    norm_gain,
):
    devices = lax.axis_size("tp")
    local_heads = prompt_queries.shape[1] // HEAD_DIM
    kv_heads = history_cache.shape[2] // HEAD_DIM
    group = devices * local_heads // kv_heads
    block = residual.shape[0]
    h_rows, p_rows = history_cache.shape[1], prompt_entries.shape[1]
    assert group % local_heads == 0 and devices & (devices - 1) == 0
    assert block >= decode_queries.shape[0]

    def swap(value, k):
        return lax.ppermute(value, "tp", [(i, i ^ k) for i in range(devices)])

    def swapped(values):
        return [values[0]] + [swap(values[k], k) for k in range(1, devices)]

    slots = [0] + list(range(2, devices))
    packed, own_query, entries = pack_history(
        history_cache, decode_queries, decode_entries, [1] + slots, local_heads, group
    )
    even_queries = [own_query] + [swap(own_query, k) for k in range(2, devices, 2)]
    history = {k: swap(packed[k], k) if k else packed[k] for k in slots}
    limits = jnp.concatenate([prompt_start, decode_lengths])
    limits = jnp.broadcast_to(limits[:, None], (limits.shape[0], HEAD_DIM))
    bundle, packed = pack_fresh(prompt_entries, packed[1], even_queries, slots, local_heads, group)
    bundle = swap(bundle, 1)
    fresh = {k: swap(packed[k], k) if k else packed[k] for k in slots}
    parts, queries = decode_partials(even_queries, bundle, decode_cache, prompt_queries, limits, local_heads, group)
    parts = swapped(parts)
    decoded = decode_join(parts, own_query, entries, local_heads)

    joined = None

    def attended(order, first, count, decoded, columns, emit=False):
        nonlocal joined
        outs, joined = attend(
            order,
            first,
            count,
            block,
            queries,
            (history, fresh, bundle),
            joined,
            decoded,
            out_weight,
            limits,
            h_rows,
            p_rows,
            columns,
            emit,
        )
        return outs

    def chip_sum(keep, give):
        return keep.astype(F32) + swap(give, 1).astype(F32)

    def cross(pair, count, start, stop):
        return [
            swap(pair[k * count + start : k * count + stop].astype(BF16), 2 * k + 2)
            for k in range(devices // 2 - 1)
        ]

    chunks = [c * block // sum(CHUNKS) for c in CHUNKS]
    if any(c % 16 for c in chunks):
        chunks = [block]
    model = out_weight.shape[1]
    stays, leaves = list(range(2, devices, 2)), list(range(3, devices, 2))
    crossed, first = [], 0
    for count in chunks:
        last = first + count == block
        if last:
            keep, give = attended(stays + leaves, first, count, decoded, model)
            pair = chip_sum(keep, give)
            cut = count - 16 if count > 16 else 0
            for start, stop in [(0, cut), (cut, count)] if cut else [(0, count)]:
                crossed.append((first + start, cross(pair, count, start, stop)))
        else:
            columns = model // 8 * FIRST_EIGHTHS
            give, gone = attended(leaves, first, count, None, columns, emit=True)
            keep, kept = attended(stays, first, count, None, columns, emit=True)
            pieces = [cross(chip_sum(keep, give), count, 0, count)]
            keep, give = project([kept, gone], out_weight, columns)
            pieces.append(cross(chip_sum(keep, give), count, 0, count))
            crossed.append((first, [piece for both in zip(*pieces) for piece in both]))
        first += count
    owned, first = [], 0
    for count in chunks:
        here = decoded if first + count == block else None
        own, give = attended([0, 1], first, count, here, model)
        owned.append((first, own, swap(give, 1)))
        first += count
    gain = norm_gain[None, :]
    outs = []
    for first, pieces in crossed:
        begin, own, given = [o for o in owned if o[0] <= first][-1]
        outs = finish(first, first - begin, residual, own, given, pieces, gain, outs)
    return tuple(outs)


def solution(mesh):
    placed = (
        P("rep", "tp"),
        P("rep", "tp", None),
        P("rep", "tp", None),
        P("rep", "tp"),
        P("rep", None, None),
        P("rep", None, "tp", None),
        P("rep"),
        P("rep"),
        P("tp", None),
        P("tp", "rep"),
        P(),
    )
    return jax.shard_map(
        step,
        mesh=mesh,
        in_specs=placed,
        out_specs=(P("tp", "rep"), P("tp", "rep")),
        check_vma=False,
    )
```

```python
import jax
import jax.numpy as jnp
import numpy as np
from jax import lax
from jax.experimental import pallas as pl
from jax.experimental.pallas import tpu as pltpu
from jax.sharding import PartitionSpec as P


HEAD_DIM = 128
MASKED = -1e30
EPS = 1e-05
CHUNKS = (64, 64)
COLUMNS = 512
FIRST_EIGHTHS = 3
GROUP_ROWS = 256

F32 = jnp.float32
BF16 = jnp.bfloat16


def round_up(value, unit):
    return -(-value // unit) * unit


def hbm():
    return pl.BlockSpec(memory_space=pl.ANY)


def in_hbm():
    return pl.BlockSpec(memory_space=pltpu.HBM)


def in_vmem():
    return pl.BlockSpec(memory_space=pltpu.VMEM)


def to_hbm(value):
    return pltpu.with_memory_space_constraint(value, pltpu.HBM)


def busy(us):
    return pl.CostEstimate(flops=us * 500_000_000, transcendentals=0, bytes_accessed=us * 1_000_000)


def params(mib, **kwargs):
    return pltpu.CompilerParams(vmem_limit_bytes=mib << 20, **kwargs)


def pack_history(history, queries, entries, slots, local_heads, group):
    h_rows = history.shape[1]
    rows = queries.shape[0]
    devices = len(slots)

    def body(h_hbm, q_hbm, e_hbm, *refs):
        o_refs, (q_ref, e_ref, sem) = refs[:devices], refs[devices:]
        me = lax.axis_index("tp")
        lane = pl.multiple_of(me * local_heads // group * HEAD_DIM, HEAD_DIM)
        copies = [pltpu.make_async_copy(e_hbm.at[:, :, pl.ds(lane, HEAD_DIM)], e_ref, sem.at[0])]
        for i, k in enumerate(slots):
            lane = pl.multiple_of((me ^ k) * local_heads // group * HEAD_DIM, HEAD_DIM)
            for part in range(2):
                copies.append(
                    pltpu.make_async_copy(
                        h_hbm.at[part, :, pl.ds(lane, HEAD_DIM)],
                        o_refs[i].at[part * h_rows : (part + 1) * h_rows, :],
                        sem.at[len(copies)],
                    )
                )
        for h in range(local_heads):
            copies.append(
                pltpu.make_async_copy(
                    q_hbm.at[:, h * HEAD_DIM : (h + 1) * HEAD_DIM],
                    q_ref.at[h * rows : (h + 1) * rows, :],
                    sem.at[len(copies)],
                )
            )
        for copy in copies:
            copy.start()
        for copy in copies:
            copy.wait()
        for o_ref, size in zip(o_refs, sizes):
            if size > 2 * h_rows:
                o_ref[2 * h_rows :, :] = q_ref[...]

    sizes = [2 * h_rows + (rows * local_heads if k and k % 2 == 0 else 0) for k in slots]
    outs = pl.pallas_call(
        body,
        in_specs=[in_hbm()] * 3,
        out_specs=[in_vmem()] * (devices + 2),
        out_shape=[jax.ShapeDtypeStruct((size, HEAD_DIM), BF16) for size in sizes]
        + [
            jax.ShapeDtypeStruct((rows * local_heads, HEAD_DIM), BF16),
            pltpu.VMEM((2, rows, HEAD_DIM), BF16),
        ],
        scratch_shapes=[pltpu.SemaphoreType.DMA((1 + 2 * devices + local_heads,))],
        compiler_params=params(2),
        cost_estimate=busy(6),
        name="pack_history",
    )(to_hbm(history), to_hbm(queries), to_hbm(entries))
    return dict(zip(slots, outs)), outs[devices], outs[devices + 1]


def pack_fresh(prompt, history, queries, slots, local_heads, group):
    h_rows, p_rows = history.shape[0] // 2, prompt.shape[1]
    p_pad = round_up(p_rows, 16)
    q_rows = queries[0].shape[0]
    every = [1] + slots
    n = len(every)

    def body(p_ref, h_ref, *refs):
        q_refs, o_refs = refs[: len(queries)], refs[len(queries) :]
        me = lax.axis_index("tp")
        o_refs[0][0 : 2 * h_rows, :] = h_ref[...]
        for i, k in enumerate(every):
            lane = pl.multiple_of((me ^ k) * local_heads // group * HEAD_DIM, HEAD_DIM)
            row = 2 * h_rows if i == 0 else 0
            for part in range(2):
                fresh = p_ref[part, :, pl.ds(lane, HEAD_DIM)]
                if p_pad > p_rows:
                    fresh = jnp.concatenate(
                        [fresh.astype(F32), jnp.zeros((p_pad - p_rows, HEAD_DIM), F32)], axis=0
                    ).astype(BF16)
                o_refs[i][row + part * p_pad : row + (part + 1) * p_pad, :] = fresh
        row = 2 * (h_rows + p_pad)
        for i, q_ref in enumerate(q_refs):
            last = q_ref.shape[0]
            o_refs[0][row + i * q_rows : row + (i + 1) * q_rows, :] = q_ref[last - q_rows : last, :]

    sizes = [2 * (h_rows + p_pad) + len(queries) * q_rows] + [2 * p_pad] * len(slots)
    outs = pl.pallas_call(
        body,
        in_specs=[in_vmem()] * (2 + len(queries)),
        out_specs=[in_vmem()] * n,
        out_shape=[jax.ShapeDtypeStruct((size, HEAD_DIM), BF16) for size in sizes],
        compiler_params=params(8),
        cost_estimate=busy(12),
        name="pack_fresh",
    )(prompt, history, *queries)
    return outs[0], dict(zip(slots, outs[1:]))


def split(value):
    terms = []
    for _ in range(3):
        terms.append(value.astype(BF16))
        value = value - terms[-1].astype(F32)
    return terms


def decode_partials(queries, bundle, cache, prompt_queries, limits, local_heads, group):
    devices = 2 * len(queries)
    rows, span, width = cache.shape[1], cache.shape[2], cache.shape[3]
    kv_heads = width // HEAD_DIM
    heads = devices * local_heads
    factor = HEAD_DIM ** (-0.5) * float(np.log2(np.e))
    part_rows = rows * local_heads
    stat_rows = round_up(local_heads, 8)
    prompt_rows, local_width = prompt_queries.shape

    def body(limits_ref, *refs):
        q_refs, refs = refs[: devices // 2], refs[devices // 2 :]
        bundle_ref, cache_ref, pq_ref = refs[:3]
        o_refs, refs = refs[3 : 3 + devices], refs[3 + devices :]
        q_ref, q_all, sums = refs
        me = lax.axis_index("tp")
        q_ref[0:prompt_rows, :] = pq_ref[...]
        q_ref[prompt_rows:, :] = jnp.zeros((rows, local_width), BF16)
        for k in range(devices):
            q_ref_k = bundle_ref if k % 2 else q_refs[k // 2]
            base = q_ref_k.shape[0] - ((devices // 2 - k // 2) if k % 2 else 1) * part_rows
            for h in range(local_heads):
                row = base + h * rows
                q_all[k, pl.ds(h, rows, stride=local_heads), :] = q_ref_k[row : row + rows, :].astype(F32)

        slot = lax.broadcasted_iota(jnp.int32, (heads, 1), 0) // local_heads
        reads = ((slot ^ me) * local_heads) // group
        lane = lax.broadcasted_iota(jnp.int32, (heads, HEAD_DIM), 1)
        place = me * span + lax.broadcasted_iota(jnp.int32, (1, span), 1)
        scores = []
        for b in range(rows):
            here = slice(b * local_heads, (b + 1) * local_heads)
            q = jnp.concatenate([q_all[k, here, :] for k in range(devices)], axis=0)
            spread = jnp.concatenate(
                [jnp.where(reads == g, q, 0.0) for g in range(kv_heads)], axis=1
            ).astype(BF16)
            score = lax.dot_general(
                spread, cache_ref[0, b], (((1,), (1,)), ((), ())), preferred_element_type=F32
            )
            scores.append(jnp.where(place < limits_ref[1 + b : 2 + b, 0:1], score, MASKED))
        scores = jnp.concatenate(scores, axis=0)
        top = jnp.max(scores, axis=-1, keepdims=True)
        weights = jnp.where(scores > 0.5 * MASKED, jnp.exp2((scores - top) * factor), 0.0)
        total = jnp.sum(weights, axis=-1, keepdims=True)
        weights = weights.astype(BF16)
        stats = jnp.zeros((heads, HEAD_DIM), F32)
        for b in range(rows):
            these = slice(b * heads, (b + 1) * heads)
            summed = jnp.dot(weights[these], cache_ref[1, b], preferred_element_type=F32)
            own = jnp.zeros((heads, HEAD_DIM), F32)
            for g in range(kv_heads):
                own = own + jnp.where(reads == g, summed[:, g * HEAD_DIM : (g + 1) * HEAD_DIM], 0.0)
            for k in range(devices):
                sums[k, b * local_heads : (b + 1) * local_heads, :] = own[k * local_heads : (k + 1) * local_heads]
            stats = jnp.where(lane == b, top[these], jnp.where(lane == rows + b, total[these], stats))
        terms = split(stats)
        for k in range(devices):
            o_refs[k][0:part_rows, :] = sums[k].astype(BF16)
            for i, term in enumerate(terms):
                row = part_rows + i * stat_rows
                o_refs[k][row : row + local_heads, :] = term[k * local_heads : (k + 1) * local_heads, :]

    outs = pl.pallas_call(
        body,
        in_specs=[in_vmem()] * (devices // 2 + 4),
        out_specs=[in_vmem()] * (devices + 1),
        scratch_shapes=[pltpu.VMEM((devices, part_rows, HEAD_DIM), F32)] * 2,
        out_shape=[jax.ShapeDtypeStruct((part_rows + 3 * stat_rows, HEAD_DIM), BF16)] * devices
        + [pltpu.VMEM((prompt_rows + rows, local_width), BF16)],
        compiler_params=params(12),
        cost_estimate=busy(12),
        name="decode",
    )(limits, *queries, bundle, cache, prompt_queries)
    return outs[:devices], outs[devices]


def decode_join(parts, queries, entries, local_heads):
    devices = len(parts)
    rows = entries.shape[1]
    factor = HEAD_DIM ** (-0.5) * float(np.log2(np.e))
    part_rows = rows * local_heads
    stat_rows = round_up(local_heads, 8)

    def body(*refs):
        p_refs = refs[:devices]
        q_ref, e_ref, o_ref, q_all, out = refs[devices:]
        for h in range(local_heads):
            q_all[pl.ds(h, rows, stride=local_heads), :] = q_ref[h * rows : (h + 1) * rows, :].astype(F32)
        stats = []
        for p in p_refs:
            starts = [part_rows + i * stat_rows for i in range(3)]
            high, middle, low = [p[row : row + local_heads, :].astype(F32) for row in starts]
            stats.append(high + middle + low)
        keys, values = e_ref[0].astype(F32), e_ref[1].astype(F32)
        sums = [p[0:part_rows, :].astype(F32) for p in p_refs]
        for b in range(rows):
            here = slice(b * local_heads, (b + 1) * local_heads)
            own = jnp.sum(q_all[here, :] * keys[b : b + 1, :], axis=-1, keepdims=True)
            tops = [s[:, b : b + 1] for s in stats]
            top = own
            for t in tops:
                top = jnp.maximum(top, t)
            weight = jnp.exp2((own - top) * factor)
            total = weight
            summed = weight.astype(BF16).astype(F32) * values[b : b + 1, :]
            for s, t, p in zip(stats, tops, sums):
                share = jnp.exp2((t - top) * factor)
                total = total + share * s[:, rows + b : rows + b + 1]
                summed = summed + share * p[here, :]
            out[here, :] = summed / total
        for h in range(local_heads):
            o_ref[:, h * HEAD_DIM : (h + 1) * HEAD_DIM] = out[pl.ds(h, rows, stride=local_heads), :].astype(BF16)

    return pl.pallas_call(
        body,
        in_specs=[in_vmem()] * (devices + 2),
        out_specs=in_vmem(),
        scratch_shapes=[pltpu.VMEM((part_rows, HEAD_DIM), F32)] * 2,
        out_shape=jax.ShapeDtypeStruct((rows, local_heads * HEAD_DIM), BF16),
        compiler_params=params(4),
        cost_estimate=busy(1),
        name="join",
    )(*parts, queries, entries)


def product(att, w, start, stop, targets):
    for c in range(start, stop, COLUMNS):
        width = min(COLUMNS, stop - c)
        out = jnp.dot(att, w[:, c : c + width], preferred_element_type=F32).astype(BF16)
        row = 0
        for target in targets:
            target[:, c - start : c - start + width] = out[row : row + target.shape[0]]
            row += target.shape[0]


def project(atts, weight, start):
    model = weight.shape[1]
    n = len(atts)

    def body(*refs):
        att = jnp.concatenate([ref[...] for ref in refs[:n]], axis=0)
        product(att, refs[n], start, model, refs[n + 1 :])

    return pl.pallas_call(
        body,
        in_specs=[in_vmem()] * (n + 1),
        out_specs=[in_vmem()] * n,
        out_shape=[jax.ShapeDtypeStruct((att.shape[0], model - start), BF16) for att in atts],
        compiler_params=params(8),
        cost_estimate=busy(2),
        name="project",
    )(*atts, weight)


def attend(order, first, count, block, queries, pieces, joined, decoded, weight, limits, h_rows, p_rows, columns, emit):
    history, fresh, bundle = pieces
    devices = len(history) + 1
    held = list(history)
    p_pad = fresh[0].shape[0] // 2
    local_width = queries.shape[1]
    local_heads = local_width // HEAD_DIM
    model = weight.shape[1]
    h_keys, p_keys = devices * h_rows, devices * p_pad
    keys = h_keys + p_keys
    pieces_given = joined is None
    shares = [sum(count for s in order if s % 2 == parity) for parity in (0, 1)]
    shares = [share for share in shares if share]
    factor = HEAD_DIM ** (-0.5) * float(np.log2(np.e))
    per = max(1, min(local_heads, GROUP_ROWS // count))
    has_decode = decoded is not None
    decode_rows = decoded.shape[0] if has_decode else 0

    def join_pieces(refs, k_all, v_all):
        n = devices - 1
        cached = {1: (refs[0], 0), **{k: (ref, 0) for k, ref in zip(held, refs[1:])}}
        own = {1: (refs[0], 2 * h_rows), **{k: (ref, 0) for k, ref in zip(held, refs[1 + n :])}}
        for k in range(devices):
            for part, dst in ((0, k_all), (1, v_all)):
                for copy in range(2 - part):
                    lanes = slice(copy * HEAD_DIM, (copy + 1) * HEAD_DIM)
                    ref, row = cached[k]
                    row += part * h_rows
                    dst[k * h_rows : (k + 1) * h_rows, lanes] = ref[row : row + h_rows, :]
                    ref, row = own[k]
                    row += part * p_pad
                    dst[h_keys + k * p_pad : h_keys + (k + 1) * p_pad, lanes] = ref[row : row + p_pad, :]
        v_all[:, HEAD_DIM:] = jnp.ones((keys, HEAD_DIM), BF16)

    def body(limits_ref, q, w, *refs):
        if has_decode:
            dec_ref, refs = refs[0], refs[1:]
        if pieces_given:
            parts, refs = refs[: 2 * devices - 1], refs[2 * devices - 1 :]
            k_all, v_all, refs = refs[0], refs[1], refs[2:]
            join_pieces(parts, k_all, v_all)
        else:
            k_all, v_all, refs = refs[0], refs[1], refs[2:]
        targets, att = refs[:-1], refs[-1]
        me = lax.axis_index("tp")
        column = lax.broadcasted_iota(jnp.int32, (1, h_keys), 1)
        place = ((column // h_rows) ^ me) * h_rows + column % h_rows
        history_bias = jnp.where(place < limits_ref[0:1, 0:1], 0.0, MASKED)
        column = lax.broadcasted_iota(jnp.int32, (1, p_keys), 1)
        inner = column % p_pad
        seen_from = jnp.where(inner < p_rows, ((column // p_pad) ^ me) * p_rows + inner, 1 << 20)
        steps = [(i, g) for i in range(len(order)) for g in range(0, local_heads, per)]
        biases = []
        for i, slot in enumerate(order):
            rows = (slot ^ me) * block + first + lax.broadcasted_iota(jnp.int32, (count, 1), 0)
            bias = jnp.where(seen_from <= rows, 0.0, MASKED)
            biases.append(jnp.concatenate([jnp.broadcast_to(history_bias, (count, h_keys)), bias], axis=1))

        def scores_of(i, g):
            row0 = pl.multiple_of((order[i] ^ me) * block + first, 16)
            stacked = jnp.concatenate(
                [q[pl.ds(row0, count), h * HEAD_DIM : (h + 1) * HEAD_DIM] for h in range(g, g + per)], axis=0
            )
            scaled = stacked.astype(F32) * factor
            high = scaled.astype(BF16)
            low = (scaled - high.astype(F32)).astype(BF16)
            stacked = jnp.concatenate([high, low], axis=1)
            scores = lax.dot_general(
                stacked, k_all[...], (((1,), (1,)), ((), ())), preferred_element_type=F32
            )
            return (scores.reshape(per, count, keys) + biases[i][None]).reshape(per * count, keys)

        ahead = scores_of(*steps[0])
        for t, (i, g) in enumerate(steps):
            scores = ahead
            if t + 1 < len(steps):
                ahead = scores_of(*steps[t + 1])
            top = jnp.max(scores, axis=-1, keepdims=True)
            weights = jnp.exp2(scores - top)
            summed = jnp.dot(weights.astype(BF16), v_all[...], preferred_element_type=F32)
            summed = (summed[:, :HEAD_DIM] / summed[:, HEAD_DIM:]).astype(BF16)
            for h in range(per):
                att[i * count : (i + 1) * count, (g + h) * HEAD_DIM : (g + h + 1) * HEAD_DIM] = summed[
                    h * count : (h + 1) * count
                ]
        if has_decode:
            for i, slot in enumerate(order):

                @pl.when(slot ^ me == devices - 1)
                def _():
                    att[(i + 1) * count - decode_rows : (i + 1) * count, :] = dec_ref[...]

        product(att[...], w, 0, columns, targets)

    flops = 2 * len(order) * count * (2 * local_width * keys + local_width * model)
    operands = [limits, queries, weight] + ([decoded] if has_decode else [])
    out_shape = [jax.ShapeDtypeStruct((share, columns), BF16) for share in shares]
    if pieces_given:
        operands += [bundle, *history.values(), *fresh.values()]
        out_shape = [jax.ShapeDtypeStruct((keys, 2 * HEAD_DIM), BF16)] * 2 + out_shape
    else:
        operands += joined
    attended = (len(order) * count, local_width)
    if emit:
        out_shape.append(jax.ShapeDtypeStruct(attended, BF16))
    outs = pl.pallas_call(
        body,
        in_specs=[in_vmem()] * len(operands),
        out_specs=[in_vmem()] * len(out_shape),
        out_shape=out_shape,
        scratch_shapes=[] if emit else [pltpu.VMEM(attended, BF16)],
        compiler_params=params(24),
        cost_estimate=pl.CostEstimate(flops=flops, transcendentals=0, bytes_accessed=weight.size * 2),
    )(*operands)
    if pieces_given:
        joined, outs = list(outs[:2]), outs[2:]
    return outs, joined


def finish(first, begin, residual, own, given, crossed, gain, previous):
    block, model = residual.shape
    count = crossed[0].shape[0]
    tile = 16
    n_cross = len(crossed)
    n_columns = 1 if crossed[0].shape[1] == model else 2

    def body(res_ref, own_ref, given_ref, *refs):
        cross = refs[:n_cross]
        gain_ref = refs[n_cross]
        outs = refs[-5:-3]
        staged, sem = refs[-3:-1], refs[-1]
        copies = []
        for i in range(0, count, tile):
            here, local = slice(first + i, first + i + tile), slice(i, i + tile)
            mine = slice(begin + i, begin + i + tile)
            hidden = res_ref[here, :].astype(F32) + own_ref[mine, :].astype(F32) + given_ref[mine, :].astype(F32)
            for c in range(0, n_cross, n_columns):
                pieces = [piece[local, :].astype(F32) for piece in cross[c : c + n_columns]]
                hidden = hidden + (jnp.concatenate(pieces, axis=1) if n_columns > 1 else pieces[0])
            mean = jnp.mean(hidden * hidden, axis=-1, keepdims=True)
            staged[0][local, :] = hidden.astype(BF16)
            staged[1][local, :] = (hidden * lax.rsqrt(mean + EPS) * gain_ref[...]).astype(BF16)
            for source, target in zip(staged, outs):
                copies.append(pltpu.make_async_copy(source.at[local, :], target.at[here, :], sem.at[len(copies)]))
                copies[-1].start()
        for copy in copies:
            copy.wait()

    n_in = 3 + n_cross + 1
    return pl.pallas_call(
        body,
        in_specs=[in_vmem()] * n_in + [hbm()] * len(previous),
        out_specs=[hbm()] * 2,
        out_shape=[jax.ShapeDtypeStruct((block, model), BF16)] * 2,
        input_output_aliases={n_in + i: i for i in range(len(previous))},
        scratch_shapes=[pltpu.VMEM((count, model), BF16)] * 2 + [pltpu.SemaphoreType.DMA((2 * count // tile,))],
        compiler_params=params(8),
        cost_estimate=busy(2),
    )(residual, own, given, *crossed, gain, *previous)


def step(
    prompt_queries,
    prompt_entries,
    history_cache,
    decode_queries,
    decode_entries,
    decode_cache,
    decode_lengths,
    prompt_start,
    out_weight,
    residual,
    norm_gain,
):
    devices = lax.axis_size("tp")
    local_heads = prompt_queries.shape[1] // HEAD_DIM
    kv_heads = history_cache.shape[2] // HEAD_DIM
    group = devices * local_heads // kv_heads
    block = residual.shape[0]
    h_rows, p_rows = history_cache.shape[1], prompt_entries.shape[1]
    assert group % local_heads == 0 and devices & (devices - 1) == 0
    assert block >= decode_queries.shape[0]

    def swap(value, k):
        return lax.ppermute(value, "tp", [(i, i ^ k) for i in range(devices)])

    def swapped(values):
        return [values[0]] + [swap(values[k], k) for k in range(1, devices)]

    slots = [0] + list(range(2, devices))
    packed, own_query, entries = pack_history(
        history_cache, decode_queries, decode_entries, [1] + slots, local_heads, group
    )
    history = {k: swap(packed[k], k) if k else packed[k] for k in slots}
    even_queries = [own_query] + [history[k] for k in range(2, devices, 2)]
    limits = jnp.concatenate([prompt_start, decode_lengths])
    limits = jnp.broadcast_to(limits[:, None], (limits.shape[0], HEAD_DIM))
    bundle, packed = pack_fresh(prompt_entries, packed[1], even_queries, slots, local_heads, group)
    bundle = swap(bundle, 1)
    fresh = {k: swap(packed[k], k) if k else packed[k] for k in slots}
    parts, queries = decode_partials(even_queries, bundle, decode_cache, prompt_queries, limits, local_heads, group)
    parts = swapped(parts)
    decoded = decode_join(parts, own_query, entries, local_heads)

    joined = None

    def attended(order, first, count, decoded, columns, emit=False):
        nonlocal joined
        outs, joined = attend(
            order,
            first,
            count,
            block,
            queries,
            (history, fresh, bundle),
            joined,
            decoded,
            out_weight,
            limits,
            h_rows,
            p_rows,
            columns,
            emit,
        )
        return outs

    def chip_sum(keep, give):
        return keep.astype(F32) + swap(give, 1).astype(F32)

    def cross(pair, count, start, stop):
        return [
            swap(pair[k * count + start : k * count + stop].astype(BF16), 2 * k + 2)
            for k in range(devices // 2 - 1)
        ]

    chunks = [c * block // sum(CHUNKS) for c in CHUNKS]
    if any(c % 16 for c in chunks):
        chunks = [block]
    model = out_weight.shape[1]
    stays, leaves = list(range(2, devices, 2)), list(range(3, devices, 2))
    crossed, first = [], 0
    for count in chunks:
        last = first + count == block
        if last:
            keep, give = attended(stays + leaves, first, count, decoded, model)
            pair = chip_sum(keep, give)
            cut = count - 16 if count > 16 else 0
            for start, stop in [(0, cut), (cut, count)] if cut else [(0, count)]:
                crossed.append((first + start, cross(pair, count, start, stop)))
        else:
            columns = model // 8 * FIRST_EIGHTHS
            give, gone = attended(leaves, first, count, None, columns, emit=True)
            keep, kept = attended(stays, first, count, None, columns, emit=True)
            pieces = [cross(chip_sum(keep, give), count, 0, count)]
            keep, give = project([kept, gone], out_weight, columns)
            pieces.append(cross(chip_sum(keep, give), count, 0, count))
            crossed.append((first, [piece for both in zip(*pieces) for piece in both]))
        first += count
    owned, first = [], 0
    for count in chunks:
        here = decoded if first + count == block else None
        own, give = attended([0, 1], first, count, here, model)
        owned.append((first, own, swap(give, 1)))
        first += count
    gain = norm_gain[None, :]
    outs = []
    for first, pieces in crossed:
        begin, own, given = [o for o in owned if o[0] <= first][-1]
        outs = finish(first, first - begin, residual, own, given, pieces, gain, outs)
    return tuple(outs)


def solution(mesh):
    placed = (
        P("rep", "tp"),
        P("rep", "tp", None),
        P("rep", "tp", None),
        P("rep", "tp"),
        P("rep", None, None),
        P("rep", None, "tp", None),
        P("rep"),
        P("rep"),
        P("tp", None),
        P("tp", "rep"),
        P(),
    )
    return jax.shard_map(
        step,
        mesh=mesh,
        in_specs=placed,
        out_specs=(P("tp", "rep"), P("tp", "rep")),
        check_vma=False,
    )
```
